32 devices in a mesh: seq: 8 (over z, core), mp: 4 (over y, x).
Axes of the slice: x: 2, y: 2, z: 4, core: 2. Of those that a mesh axis runs over, the one named last changes fastest.
Arguments:
- hidden_in: bfloat16 [4096, 4096], P('seq', 'mp'), may hold values from -30 to 30
- norm_gain: float32 [4096], replicated, may hold values from 0.1 to 1.9
- w_z: bfloat16 [4096, 8192], P('seq', 'mp'), may hold values from -0.09375 to 0.09375
- w_x: bfloat16 [4096, 8192], P('seq', 'mp'), may hold values from -0.09375 to 0.09375
- w_b: bfloat16 [4096, 1024], P('seq', 'mp'), may hold values from -0.09375 to 0.09375
- w_c: bfloat16 [4096, 1024], P('seq', 'mp'), may hold values from -0.09375 to 0.09375
- w_dt: bfloat16 [4096, 128], P('seq', 'mp'), may hold values from -0.0625 to 0.0625
- conv_x: float32 [4, 8192], P(None, 'mp'), may hold values from -3 to 3
- conv_b: float32 [4, 1024], P(None, 'mp'), may hold values from -3 to 3
- conv_c: float32 [4, 1024], P(None, 'mp'), may hold values from -3 to 3
- dt_bias: float32 [128], P('mp'), may hold values from -9 to -5
- a_rate: float32 [128], P('mp'), may hold values from 0.5 to 16
- skip_gain: float32 [128], P('mp'), may hold values from -3 to 3
- group_gain: float32 [8192], P('mp'), may hold values from 0.1 to 1.9
- w_out: bfloat16 [8192, 4096], P('mp', 'seq'), may hold values from -0.0625 to 0.0625
- attn_gain: float32 [4096], replicated, may hold values from 0.1 to 1.9
- w_q: bfloat16 [4096, 4096], P(None, 'mp'), may hold values from -0.125 to 0.125
- w_k: bfloat16 [4096, 1024], P(None, 'mp'), may hold values from -0.125 to 0.125
- w_v: bfloat16 [4096, 1024], P(None, 'mp'), may hold values from -0.09375 to 0.09375
Outputs:
- mixed: float32 [4096, 4096], P('seq', 'mp')
- context: float32 [4096, 4096], P('seq', 'mp')
The draws below stay inside these ranges and needn't reach their ends.
All inputs are finite; a program needn't handle non-finite values.
Results may differ from the reference program's by a relative error of at most 0.017.
Values may be sent and summed in bfloat16 or wider, within the bound.
A program may use at most 192 MiB of HBM per device.

```python
import math
import jax
import jax.numpy as jnp
from jax import lax

D = 4096
DI = 8192
H = 128
P_SIZE = 64
N = 128
G = 8
KW = 4
HQ = 32
HK = 8
HD = 128
WINDOW = 4096
QB = 128
TOK_DEV = 512
TOKENS = 4096
N_SEQ = 8
N_MP = 4


def contiguous_spans(key):
    forward_sense = jnp.clip(jax.random.normal(jax.random.fold_in(key, 101), (D,), jnp.float32), -4.0, 4.0)
    processor_slots = jax.random.randint(jax.random.fold_in(key, 102), (TOKENS // TOK_DEV * 2,), 0, TOKENS)
    input_magnitude = jax.random.uniform(jax.random.fold_in(key, 103), (TOKENS // TOK_DEV * 2,), jnp.float32, 0.6, 1.0)
    return (forward_sense, processor_slots, input_magnitude)


def draw_hidden_in(key, part):
    forward_sense, processor_slots, input_magnitude = contiguous_spans(key)
    base = jnp.clip(jax.random.normal(jax.random.fold_in(key, 1), (TOKENS, D), jnp.float32), -6.0, 6.0)
    mixing = jnp.zeros((TOKENS,), jnp.float32).at[processor_slots].set(input_magnitude)
    values = base * (1.0 - mixing)[:, None] + forward_sense[None, :] * (4.0 * mixing)[:, None]
    return jnp.clip(values, -30.0, 30.0).astype(jnp.bfloat16)


def draw_w_dt(key, part):
    forward_sense, processor_slots, input_magnitude = contiguous_spans(key)
    noise = 0.3 * jnp.clip(jax.random.normal(jax.random.fold_in(key, 3), (D, H), jnp.float32), -6.0, 6.0) / math.sqrt(D)
    lifted = jax.random.uniform(jax.random.fold_in(key, 4), (H,), jnp.float32, 6.0, 10.0)
    limit = 4.0 / math.sqrt(D)
    return jnp.clip(noise + forward_sense[:, None] * lifted[None, :] / D, -limit, limit).astype(jnp.bfloat16)


def draw_w_q(key, part):
    base = jnp.clip(jax.random.normal(jax.random.fold_in(key, 5), (D, HQ * HD), jnp.float32), -6.0, 6.0) / math.sqrt(D)
    limit = 8.0 / math.sqrt(D)
    return jnp.clip(base, -limit, limit).astype(jnp.bfloat16)


def draw_w_k(key, part):
    base = jnp.clip(jax.random.normal(jax.random.fold_in(key, 6), (D, HK * HD), jnp.float32), -6.0, 6.0) / math.sqrt(D)
    limit = 8.0 / math.sqrt(D)
    return jnp.clip(base, -limit, limit).astype(jnp.bfloat16)


def block_levels(own_key, dims, split, smallest, largest):
    factor_of, own = 1.0, jax.random.fold_in(own_key, 6)
    for position, blocks in split:
        draws = jnp.exp(jax.random.uniform(jax.random.fold_in(own, position), (blocks,), jnp.float32, smallest / len(split), largest / len(split)))
        factor_of = factor_of * jnp.repeat(draws, dims[position] // blocks).reshape([-1 if axis == position else 1 for axis in range(len(dims))])
    return factor_of


def scatter_about(own_key, dims, scale, bound, split=(), kind=jnp.bfloat16):
    result = scale * jax.random.normal(own_key, dims, jnp.float32)
    if split:
        result = result * block_levels(own_key, dims, split, -0.22, 0.18)
    return jnp.clip(result, -bound, bound).astype(kind)


def setup_inputs(seed: int = 0) -> dict:
    key_list = jax.random.split(jax.random.key(seed), 20)
    return {
        "hidden_in": draw_hidden_in(jax.random.fold_in(key_list[19], 71), 0),
        "norm_gain": jnp.clip(1.0 + 0.18 * jax.random.normal(key_list[1], (D,), jnp.float32), 0.1, 1.9),
        "w_z": scatter_about(key_list[2], (D, DI), D ** -0.5, 0.09375, ((0, 8), (1, 4))),
        "w_x": scatter_about(key_list[3], (D, DI), D ** -0.5, 0.09375, ((0, 8), (1, 4))),
        "w_b": scatter_about(key_list[4], (D, G * N), D ** -0.5, 0.09375, ((0, 8), (1, 4))),
        "w_c": scatter_about(key_list[5], (D, G * N), D ** -0.5, 0.09375, ((0, 8), (1, 4))),
        "w_dt": draw_w_dt(jax.random.fold_in(key_list[19], 71), 0),
        "conv_x": scatter_about(key_list[7], (KW, DI), 0.5, 3.0, ((1, 4),), jnp.float32),
        "conv_b": scatter_about(key_list[8], (KW, G * N), 0.5, 3.0, ((1, 4),), jnp.float32),
        "conv_c": scatter_about(key_list[9], (KW, G * N), 0.5, 3.0, ((1, 4),), jnp.float32),
        "dt_bias": jnp.clip(-9.0 + 4.0 * jax.random.uniform(key_list[10], (H,), jnp.float32) ** block_levels(key_list[10], (H,), ((0, 4),), -0.2, 0.2), -9.0, -5.0),
        "a_rate": jnp.clip(jnp.exp(math.log(16.0) - 3.465736 * jax.random.uniform(key_list[11], (H,), jnp.float32) ** block_levels(key_list[11], (H,), ((0, 4),), -0.2, 0.2)), 0.5, 16.0),
        "skip_gain": scatter_about(key_list[12], (H,), 1.0, 3.0, ((0, 4),), jnp.float32),
        "group_gain": jnp.clip(1.0 + 0.18 * jax.random.normal(key_list[13], (DI,), jnp.float32), 0.1, 1.9),
        "w_out": scatter_about(key_list[14], (DI, D), DI ** -0.5, 0.0625, ((0, 4), (1, 8))),
        "attn_gain": jnp.clip(1.0 + 0.18 * jax.random.normal(key_list[15], (D,), jnp.float32), 0.1, 1.9),
        "w_q": draw_w_q(jax.random.fold_in(key_list[19], 71), 0),
        "w_k": draw_w_k(jax.random.fold_in(key_list[19], 71), 0),
        "w_v": scatter_about(key_list[18], (D, HK * HD), D ** -0.5, 0.09375, ((1, 4),)),
    }


HIGH = lax.Precision.HIGHEST

def rms_norm(values, gain):
    return values * lax.rsqrt(lax.optimization_barrier(jnp.mean(values * values, axis=-1, keepdims=True)) + 1e-05) * gain

def causal_conv(values, rim, device_routine):
    padded = jnp.concatenate([rim, values], axis=0)
    length = values.shape[0]
    summed = jnp.zeros(values.shape, jnp.float32)
    for offset in range(device_routine.shape[0]):
        summed = summed + device_routine[offset][None, :] * padded[offset:offset + length]
    return jax.nn.silu(summed)

def ssd_block(carry_state, pieces):
    inputs, step_sizes, decays, keys_b, reads_c = pieces
    per_group = inputs.shape[1] // keys_b.shape[1]
    b_heads = jnp.repeat(keys_b, per_group, axis=1)
    c_heads = jnp.repeat(reads_c, per_group, axis=1)
    cumulative = jnp.cumsum(decays, axis=0)
    length = inputs.shape[0]
    causal_mask = jnp.arange(length)[:, None] >= jnp.arange(length)[None, :]
    spread = cumulative[:, None, :] - cumulative[None, :, :]
    within = jnp.exp(jnp.where(causal_mask[:, :, None], spread, -jnp.inf))
    affinity = jnp.einsum('tgn,sgn->gts', reads_c, keys_b, precision=HIGH)
    affinity = jnp.repeat(affinity, per_group, axis=0)
    mixing = affinity * jnp.transpose(within, (2, 0, 1)) * jnp.transpose(step_sizes)[:, None, :]
    inside = jnp.einsum('hts,shp->thp', mixing, inputs, precision=HIGH)
    carried = jnp.exp(cumulative)[:, :, None] * jnp.einsum('thn,hpn->thp', c_heads, carry_state, precision=HIGH)
    tail_weight = jnp.exp(cumulative[-1][None, :] - cumulative) * step_sizes
    fresh_state = jnp.einsum('sh,shp,shn->hpn', tail_weight, inputs, b_heads, precision=HIGH)
    updated = jnp.exp(cumulative[-1])[:, None, None] * carry_state + fresh_state
    return (updated, inside + carried)

def run_ssd(inputs, step_sizes, decays, keys_b, reads_c, block, carry_state):
    total_rows = inputs.shape[0]
    block_count = total_rows // block

    def blocked(values):
        return values.reshape((block_count, block) + values.shape[1:])
    final_state, outputs = lax.scan(ssd_block, carry_state, (blocked(inputs), blocked(step_sizes), blocked(decays), blocked(keys_b), blocked(reads_c)))
    return (final_state, outputs.reshape((total_rows,) + outputs.shape[2:]))

def window_attention(asking_vectors, keys, values, shift_rows, first_key):
    per_kv = asking_vectors.shape[1] // keys.shape[1]
    keys_all = jnp.repeat(keys, per_kv, axis=1)
    values_all = jnp.repeat(values, per_kv, axis=1)
    query_rows = asking_vectors.shape[0]
    key_count = keys.shape[0]
    scale = asking_vectors.shape[2] ** (-0.5)
    index_offsets = jnp.arange(key_count)[None, :] - shift_rows - jnp.arange(query_rows)[:, None]
    allowed = (index_offsets <= 0) & (index_offsets > -WINDOW) & (first_key + jnp.arange(key_count) >= 0)[None, :]

    def one_head(operands):
        query_h, key_h, value_h = operands
        scores = lax.dot_general(query_h, key_h, (((1,), (1,)), ((), ())), preferred_element_type=jnp.float32) * scale
        scores = jnp.where(allowed, scores, -jnp.inf)
        row_peak = lax.optimization_barrier(jnp.max(scores, axis=1, keepdims=True))
        exp_scores = jnp.exp(scores - row_peak)
        weights = (exp_scores / lax.optimization_barrier(jnp.sum(exp_scores, axis=1, keepdims=True))).astype(jnp.bfloat16)
        return jnp.dot(weights, value_h, preferred_element_type=jnp.float32)
    outputs = lax.map(one_head, (jnp.transpose(asking_vectors, (1, 0, 2)), jnp.transpose(keys_all, (1, 0, 2)), jnp.transpose(values_all, (1, 0, 2))))
    return jnp.transpose(outputs, (1, 0, 2)).reshape(query_rows, -1)

def reference(hidden_in, norm_gain, w_z, w_x, w_b, w_c, w_dt, conv_x, conv_b, conv_c, dt_bias, a_rate, skip_gain, group_gain, w_out, attn_gain, w_q, w_k, w_v):
    stream = hidden_in.astype(jnp.float32)
    normed = rms_norm(stream, norm_gain).astype(jnp.bfloat16)
    gate_proj = jnp.dot(normed, w_z, preferred_element_type=jnp.float32)
    input_mapped = jnp.dot(normed, w_x, preferred_element_type=jnp.float32)
    b_proj = jnp.dot(normed, w_b, preferred_element_type=jnp.float32)
    c_proj = jnp.dot(normed, w_c, preferred_element_type=jnp.float32)
    delta_time_unscaled = jnp.dot(normed, w_dt, preferred_element_type=jnp.float32)
    conv_in = causal_conv(input_mapped, jnp.zeros((KW - 1, DI), jnp.float32), conv_x)
    conv_bv = causal_conv(b_proj, jnp.zeros((KW - 1, G * N), jnp.float32), conv_b)
    conv_cv = causal_conv(c_proj, jnp.zeros((KW - 1, G * N), jnp.float32), conv_c)
    step_sizes = jax.nn.softplus(delta_time_unscaled + dt_bias[None, :])
    decays = -a_rate[None, :] * step_sizes
    inputs = conv_in.reshape(TOKENS, H, P_SIZE)
    final_state, ssd_out = run_ssd(inputs, step_sizes, decays, conv_bv.reshape(TOKENS, G, N), conv_cv.reshape(TOKENS, G, N), QB, jnp.zeros((H, P_SIZE, N), jnp.float32))
    full = ssd_out + skip_gain[None, :, None] * inputs
    gated = full.reshape(TOKENS, DI) * jax.nn.silu(gate_proj)
    grouped = gated.reshape(TOKENS, G, DI // G)
    y_normed = rms_norm(grouped, group_gain.reshape(G, DI // G)).reshape(TOKENS, DI).astype(jnp.bfloat16)
    width = DI // N_MP
    summed = jnp.zeros((TOKENS, D), jnp.float32)
    for member in range(N_MP):
        term = jnp.dot(y_normed[:, member * width:(member + 1) * width], w_out[member * width:(member + 1) * width], preferred_element_type=jnp.float32)
        summed = summed + lax.optimization_barrier(term.astype(jnp.bfloat16)).astype(jnp.float32)
    mixed = stream + summed
    mixed_low = lax.optimization_barrier(mixed.astype(jnp.bfloat16)).astype(jnp.float32)
    normed_two = rms_norm(mixed_low, attn_gain).astype(jnp.bfloat16)
    asking_vectors = jnp.dot(normed_two, w_q, preferred_element_type=jnp.float32).astype(jnp.bfloat16).reshape(TOKENS, HQ, HD)
    keys = jnp.dot(normed_two, w_k, preferred_element_type=jnp.float32).astype(jnp.bfloat16).reshape(TOKENS, HK, HD)
    values = jnp.dot(normed_two, w_v, preferred_element_type=jnp.float32).astype(jnp.bfloat16).reshape(TOKENS, HK, HD)
    keys_pad = jnp.concatenate([jnp.zeros((WINDOW, HK, HD), jnp.bfloat16), keys], axis=0)
    values_pad = jnp.concatenate([jnp.zeros((WINDOW, HK, HD), jnp.bfloat16), values], axis=0)

    def one_block(block_index):
        start = (block_index * TOK_DEV).astype(jnp.int32)
        asking_tile = lax.dynamic_slice_in_dim(asking_vectors, start, TOK_DEV, 0)
        key_blk = lax.dynamic_slice_in_dim(keys_pad, start, WINDOW + TOK_DEV, 0)
        value_blk = lax.dynamic_slice_in_dim(values_pad, start, WINDOW + TOK_DEV, 0)
        return window_attention(asking_tile, key_blk, value_blk, WINDOW, start - WINDOW)
    blocks = lax.map(one_block, jnp.arange(N_SEQ, dtype=jnp.int32))
    context = blocks.reshape(TOKENS, HQ * HD)
    return (mixed, context)
```

```python
import functools
import math

import jax
import jax.numpy as jnp
from jax import lax
from jax.experimental import pallas as pl
from jax.experimental.pallas import tpu as pltpu
from jax.sharding import PartitionSpec as P

P_SIZE = 64
N = 128
HD = 128
WINDOW = 4096
QB = 128
LANES = 128
VMEM_LIMIT = 62 * 1024 * 1024

HIGH = lax.Precision.HIGHEST
F32 = jnp.float32
BF16 = jnp.bfloat16


def from_behind(block, axis, distance):
    devices = range(lax.axis_size(axis))
    route = [(i - distance, i) for i in devices if i - distance in devices]
    return lax.ppermute(block, axis, route)


def rms_norm(values, gain):
    return values * lax.rsqrt(jnp.mean(values * values, axis=-1, keepdims=True) + 1e-05) * gain


def signal_seq(sem, index):
    pl.semaphore_signal(
        sem, inc=1, device_id={"seq": index}, device_id_type=pl.DeviceIdType.MESH
    )


def signal_mp(sem, index):
    pl.semaphore_signal(
        sem, inc=1, device_id={"mp": index}, device_id_type=pl.DeviceIdType.MESH
    )


def norm_rows(source, gain_ref, target):
    rows = source.shape[0]
    tile = min(64, rows)

    def body(i, carry_none):
        here = pl.ds(pl.multiple_of(i * tile, tile), tile)
        target[here, :] = rms_norm(source[here, :].astype(F32), gain_ref[...]).astype(BF16)
        return carry_none

    lax.fori_loop(0, rows // tile, body, 0)


def share_features(m, source, whole, send_sem, recv_sem):
    member = lax.axis_index("mp")
    wide = source.shape[1]
    own = pl.ds(pl.multiple_of(member * wide, wide), wide)
    copies = [
        pltpu.make_async_remote_copy(
            src_ref=source,
            dst_ref=whole.at[:, own],
            send_sem=send_sem.at[d - 1],
            recv_sem=recv_sem.at[d - 1],
            device_id={"mp": lax.rem(member + d, m)},
            device_id_type=pl.DeviceIdType.MESH,
        )
        for d in range(1, m)
    ]
    for copy in copies:
        copy.start()
    return copies, own


def features_arrived(m, whole, wide, recv_sem):
    member = lax.axis_index("mp")
    for d in range(1, m):
        sender = lax.rem(member - d + m, m)
        there = whole.at[:, pl.ds(pl.multiple_of(sender * wide, wide), wide)]
        pltpu.make_async_copy(there, there, recv_sem.at[d - 1]).wait()


def gather_dot_kernel(
    n,
    m,
    hidden_ref,
    gain_ref,
    w_ref,
    out_ref,
    slots,
    normed_ref,
    local_sem,
    send_sem,
    recv_sem,
    own_sem,
    mp_send_sem,
    mp_recv_sem,
):
    me = lax.axis_index("seq")
    member = lax.axis_index("mp")
    ring = n // 2
    half = ring // 2
    chip, core = me // 2, lax.rem(me, 2)
    up = lax.rem(chip + 1, ring) * 2 + core
    down = lax.rem(chip + ring - 1, ring) * 2 + core
    partner = chip * 2 + 1 - core
    depth, cols = w_ref.shape
    mid = depth // 2

    barrier = pltpu.get_barrier_semaphore()
    for other in (up, down, partner):
        signal_seq(barrier, other)
    for d in range(1, m):
        signal_mp(barrier, lax.rem(member + d, m))
    pl.semaphore_wait(barrier, 3 + m - 1)

    shared, own = share_features(m, hidden_ref, normed_ref, mp_send_sem, mp_recv_sem)
    own_copy = pltpu.make_async_copy(hidden_ref, normed_ref.at[:, own], own_sem)
    own_copy.start()
    local = pltpu.make_async_copy(w_ref, slots.at[0], local_sem)
    local.start()
    started = []

    def send(source, slot, rows, part, target):
        copy = pltpu.make_async_remote_copy(
            src_ref=source,
            dst_ref=slots.at[slot, rows],
            send_sem=send_sem.at[len(started)],
            recv_sem=recv_sem.at[2 * slot + part],
            device_id={"seq": target},
            device_id_type=pl.DeviceIdType.MESH,
        )
        copy.start()
        started.append(copy)

    def arrived(slot, rows, part):
        pltpu.make_async_copy(
            slots.at[slot, rows], slots.at[slot, rows], recv_sem.at[2 * slot + part]
        ).wait()

    whole, upper, lower = pl.ds(0, depth), pl.ds(0, mid), pl.ds(mid, mid)
    send(w_ref, 2 * 1, whole, 0, up)
    send(w_ref, 2 * (ring - 1), whole, 0, down)
    send(w_ref, 1, whole, 0, partner)

    def multiply(slot, first=False):
        step, lane = slot // 2, slot % 2
        origin = lax.rem(chip - step + ring, ring) * 2
        owner = origin + (core if lane == 0 else 1 - core)
        features = pl.ds(pl.multiple_of(owner * depth, depth), depth)

        def tile(start, width):
            where = pl.ds(start, width)
            product = jnp.dot(
                normed_ref[:, features], slots[slot, :, where], preferred_element_type=F32
            )
            if first:
                out_ref[:, where] = product
            else:
                out_ref[:, where] += product

        width = 512
        full = cols // width

        def body(i, carry):
            tile(pl.multiple_of(i * width, width), width)
            return carry

        lax.fori_loop(0, full, body, 0)
        if cols % width:
            tile(full * width, cols % width)

    own_copy.wait()
    features_arrived(m, normed_ref, hidden_ref.shape[1], mp_recv_sem)
    norm_rows(normed_ref, gain_ref, normed_ref)
    local.wait()
    multiply(0, True)
    arrived(1, whole, 0)
    multiply(1)
    for d in range(1, half):
        s_up, s_down = 2 * d, 2 * (ring - d)
        last = d + 1 == half
        arrived(s_up, whole, 0)
        rows = upper if last else whole
        send(slots.at[s_up, rows], 2 * (d + 1), rows, 0, up)
        arrived(s_down, whole, 0)
        rows = lower if last else whole
        send(slots.at[s_down, rows], 2 * (ring - d - 1), rows, 1 if last else 0, down)
        send(slots.at[s_up, whole], s_up + 1, whole, 0, partner)
        send(slots.at[s_down, whole], s_down + 1, whole, 0, partner)
        multiply(s_up)
        multiply(s_down)
        arrived(s_up + 1, whole, 0)
        multiply(s_up + 1)
        arrived(s_down + 1, whole, 0)
        multiply(s_down + 1)
    far = 2 * half
    arrived(far, upper, 0)
    send(slots.at[far, upper], far + 1, upper, 0, partner)
    arrived(far, lower, 1)
    send(slots.at[far, lower], far + 1, lower, 1, partner)
    multiply(far)
    arrived(far + 1, upper, 0)
    arrived(far + 1, lower, 1)
    multiply(far + 1)
    for copy in started + shared:
        copy.wait_send()


def gather_dot(hidden, gain, weights):
    n, m = lax.axis_size("seq"), lax.axis_size("mp")
    depth, cols = weights.shape
    rows, features = hidden.shape[0], hidden.shape[1] * m
    ring = n // 2
    sends = 3 + 4 * (ring // 2 - 1) + 2
    return pl.pallas_call(
        functools.partial(gather_dot_kernel, n, m),
        out_shape=jax.ShapeDtypeStruct((rows, cols), F32),
        in_specs=[
            pl.BlockSpec(memory_space=pl.ANY),
            pl.BlockSpec(memory_space=pltpu.VMEM),
            pl.BlockSpec(memory_space=pl.ANY),
        ],
        out_specs=pl.BlockSpec(memory_space=pltpu.VMEM),
        scratch_shapes=[
            pltpu.VMEM((n, depth, cols), BF16),
            pltpu.VMEM((rows, features), BF16),
            pltpu.SemaphoreType.DMA,
            pltpu.SemaphoreType.DMA((sends,)),
            pltpu.SemaphoreType.DMA((2 * n,)),
            pltpu.SemaphoreType.DMA,
            pltpu.SemaphoreType.DMA((m - 1,)),
            pltpu.SemaphoreType.DMA((m - 1,)),
        ],
        compiler_params=pltpu.CompilerParams(
            collective_id=0, has_side_effects=True, vmem_limit_bytes=VMEM_LIMIT
        ),
        cost_estimate=pl.CostEstimate(
            flops=2 * rows * features * cols,
            bytes_accessed=160_000_000,
            transcendentals=0,
        ),
    )(hidden, gain, weights)


def silu(v):
    return v / (1.0 + jnp.exp(-v))


def spread_heads(values, expand):
    high = values.astype(BF16)
    low = (values - high.astype(F32)).astype(BF16)
    return jnp.dot(high, expand, preferred_element_type=F32) + jnp.dot(
        low, expand, preferred_element_type=F32
    )


def mixer_kernel(
    n,
    heads,
    groups,
    proj_ref,
    rim_ref,
    taps_ref,
    bias_ref,
    rate_ref,
    skip_ref,
    gain_ref,
    expand_ref,
    y_ref,
    window,
    conv,
    ssd,
    reads,
    logs,
    state,
    carry,
    state_out,
    state_in,
    send_sem,
    recv_sem,
):
    me = lax.axis_index("seq")
    rows = proj_ref.shape[0]
    inner = heads * P_SIZE
    width = inner + 2 * groups * N
    gate_at = width + LANES
    per_group = inner // groups
    blocks = rows // QB
    kw = taps_ref.shape[0]

    barrier = pltpu.get_barrier_semaphore()
    signal_seq(barrier, lax.rem(me + 1, n))
    signal_seq(barrier, lax.rem(me + n - 1, n))
    pl.semaphore_wait(barrier, 2)

    expand = expand_ref[...]
    window[0:8, :] = rim_ref[...]
    state[...] = jnp.zeros_like(state)
    carry[...] = jnp.zeros_like(carry)
    row_id = lax.broadcasted_iota(jnp.int32, (QB, QB), 0)
    col_id = lax.broadcasted_iota(jnp.int32, (QB, QB), 1)
    causal = row_id >= col_id
    low_lanes = col_id < P_SIZE
    tri = jnp.where(causal, 1.0, 0.0).astype(F32)

    def block(i, carry_none):
        base = pl.multiple_of(i * QB, QB)
        here = pl.ds(base, QB)
        window[8 : 8 + QB, :] = proj_ref[here, 0:width]
        step_cols = 256 if width % 256 == 0 else 128
        for at in range(0, width, step_cols):
            cs = slice(at, at + step_cols)
            total = None
            for j in range(kw):
                term = taps_ref[j : j + 1, cs] * window[8 - kw + 1 + j : 8 - kw + 1 + j + QB, cs]
                total = term if total is None else total + term
            conv[:, cs] = silu(total)
        window[0:8, :] = window[QB : QB + 8, :]

        raw = proj_ref[here, width : width + LANES] + bias_ref[...]
        steps = jnp.maximum(raw, 0.0) + jnp.log1p(jnp.exp(-jnp.abs(raw)))
        decays = -rate_ref[...] * steps
        cum = jnp.dot(tri, decays, precision=HIGH, preferred_element_type=F32)
        cum_t = jnp.transpose(cum)
        logs[here, :] = cum + carry[0:1, :]
        carry[...] = carry[...] + cum[QB - 1 : QB, :]
        grown = jnp.exp(cum)
        tail = jnp.exp(cum[QB - 1 : QB, :] - cum)

        for g in range(groups):
            lanes = slice(g * per_group, (g + 1) * per_group)
            expand_g = expand[:, lanes]
            x = conv[:, lanes]
            b = conv[:, inner + g * N : inner + (g + 1) * N].astype(BF16)
            c = conv[:, inner + (groups + g) * N : inner + (groups + g + 1) * N].astype(BF16)
            reads[here, g * N : (g + 1) * N] = c
            scaled = x * spread_heads(steps, expand_g)
            grown_e = spread_heads(grown, expand_g)
            tailed = (scaled * spread_heads(tail, expand_g)).astype(BF16)
            scaled_low = scaled.astype(BF16)
            held = state[:, lanes]
            carried = grown_e * jnp.dot(c, held.astype(BF16), preferred_element_type=F32)
            ssd[here, lanes] = carried + skip_ref[:, lanes] * x
            fresh = lax.dot_general(
                b, tailed, (((0,), (0,)), ((), ())), preferred_element_type=F32
            )
            state[:, lanes] = grown_e[QB - 1 : QB, :] * held + fresh
            affinity = lax.dot_general(
                c, b, (((1,), (1,)), ((), ())), preferred_element_type=F32
            )
            affinity = jnp.where(causal, affinity, 0.0)
            for pair in range(per_group // LANES):
                at = pair * LANES
                inputs = scaled_low[:, at : at + LANES]
                outs = []
                for k in range(2):
                    h = (g * per_group + at) // P_SIZE + k
                    spread = jnp.minimum(cum[:, h : h + 1] - cum_t[h : h + 1, :], 0.0)
                    mixing = (affinity * jnp.exp(spread)).astype(BF16)
                    outs.append(jnp.dot(mixing, inputs, preferred_element_type=F32))
                where = slice(g * per_group + at, g * per_group + at + LANES)
                ssd[here, where] += jnp.where(low_lanes, outs[0], outs[1])
        return carry_none

    lax.fori_loop(0, blocks, block, 0)

    parts = 4
    piece = inner // parts
    decay = jnp.exp(carry[...])

    def hand_on(k):
        lanes = slice(k * piece, (k + 1) * piece)
        return pltpu.make_async_remote_copy(
            src_ref=state_out.at[:, lanes],
            dst_ref=state_in.at[:, lanes],
            send_sem=send_sem.at[k],
            recv_sem=recv_sem.at[k],
            device_id={"seq": jnp.minimum(me + 1, n - 1)},
            device_id_type=pl.DeviceIdType.MESH,
        )

    for k in range(parts):
        lanes = slice(k * piece, (k + 1) * piece)
        weight = spread_heads(decay, expand[:, lanes])[0:1, :]

        @pl.when(me > 0)
        def _():
            hand_on(k).wait_recv()
            before = state_in[:, lanes].astype(F32)
            state_out[:, lanes] = (weight * before + state[:, lanes]).astype(BF16)

        @pl.when(me == 0)
        def _():
            state_out[:, lanes] = state[:, lanes].astype(BF16)
            state_in[:, lanes] = jnp.zeros((N, piece), BF16)

        @pl.when(me < n - 1)
        def _():
            hand_on(k).start()

    def finish(i, carry_none):
        here = pl.ds(pl.multiple_of(i * QB, QB), QB)
        grown = jnp.exp(logs[here, :])
        for g in range(groups):
            lanes = slice(g * per_group, (g + 1) * per_group)
            late = jnp.dot(
                reads[here, g * N : (g + 1) * N],
                state_in[:, lanes],
                preferred_element_type=F32,
            )
            full = ssd[here, lanes] + spread_heads(grown, expand[:, lanes]) * late
            gate = proj_ref[here, gate_at + g * per_group : gate_at + (g + 1) * per_group]
            gated = full * silu(gate)
            power = jnp.mean(gated * gated, axis=-1, keepdims=True)
            y_ref[here, lanes] = (gated * lax.rsqrt(power + 1e-05) * gain_ref[:, lanes]).astype(BF16)
        return carry_none

    lax.fori_loop(0, blocks, finish, 0)

    @pl.when(me < n - 1)
    def _():
        for k in range(parts):
            hand_on(k).wait_send()


def mixer(proj, rim, taps, bias, rate, skip, gain, heads, groups):
    n = lax.axis_size("seq")
    rows = proj.shape[0]
    inner = heads * P_SIZE
    width = inner + 2 * groups * N
    expand = (
        jnp.arange(LANES)[:, None] == (jnp.arange(inner) // P_SIZE)[None, :]
    ).astype(BF16)
    vmem = pl.BlockSpec(memory_space=pltpu.VMEM)
    return pl.pallas_call(
        functools.partial(mixer_kernel, n, heads, groups),
        out_shape=jax.ShapeDtypeStruct((rows, inner), BF16),
        in_specs=[vmem] * 8,
        out_specs=vmem,
        scratch_shapes=[
            pltpu.VMEM((8 + QB, width), F32),
            pltpu.VMEM((QB, width), F32),
            pltpu.VMEM((rows, inner), F32),
            pltpu.VMEM((rows, groups * N), BF16),
            pltpu.VMEM((rows, LANES), F32),
            pltpu.VMEM((N, inner), F32),
            pltpu.VMEM((8, LANES), F32),
            pltpu.VMEM((N, inner), BF16),
            pltpu.VMEM((N, inner), BF16),
            pltpu.SemaphoreType.DMA((4,)),
            pltpu.SemaphoreType.DMA((4,)),
        ],
        compiler_params=pltpu.CompilerParams(
            collective_id=1, has_side_effects=True, vmem_limit_bytes=48 * 1024 * 1024
        ),
        cost_estimate=pl.CostEstimate(
            flops=8_000_000_000, bytes_accessed=100_000_000, transcendentals=8_000_000
        ),
    )(proj, rim, taps, bias, rate, skip, gain, expand)


def output_kernel(
    m,
    y_ref,
    w_ref,
    hidden_ref,
    gain_ref,
    mixed_ref,
    normed_ref,
    outgoing,
    incoming,
    low,
    part_send,
    part_recv,
    own_sem,
    mp_send,
    mp_recv,
):
    member = lax.axis_index("mp")
    wide = hidden_ref.shape[1]
    barrier = pltpu.get_barrier_semaphore()
    for d in range(1, m):
        signal_mp(barrier, lax.rem(member + d, m))
    pl.semaphore_wait(barrier, m - 1)
    tile = min(512, wide)

    def part(target, store):
        for at in range(0, wide, tile):
            where = pl.ds(pl.multiple_of(target * wide + at, tile), tile)
            term = jnp.dot(y_ref[...], w_ref[:, where], preferred_element_type=F32)
            store(slice(at, at + tile), term.astype(BF16))

    copies = []
    for d in range(1, m):
        target = lax.rem(member + d, m)

        def keep(where, term):
            outgoing[d - 1, :, where] = term

        part(target, keep)
        copy = pltpu.make_async_remote_copy(
            src_ref=outgoing.at[d - 1],
            dst_ref=incoming.at[d - 1],
            send_sem=part_send.at[d - 1],
            recv_sem=part_recv.at[d - 1],
            device_id={"mp": target},
            device_id_type=pl.DeviceIdType.MESH,
        )
        copy.start()
        copies.append(copy)

    def begin(where, term):
        mixed_ref[:, where] = hidden_ref[:, where].astype(F32) + term.astype(F32)

    part(member, begin)
    for d in range(1, m):
        copies[d - 1].wait_recv()
        if d < m - 1:
            mixed_ref[...] += incoming[d - 1].astype(F32)
        else:
            total = mixed_ref[...] + incoming[d - 1].astype(F32)
            mixed_ref[...] = total
            low[...] = total.astype(BF16)
    shared, own = share_features(m, low, normed_ref, mp_send, mp_recv)
    own_copy = pltpu.make_async_copy(low, normed_ref.at[:, own], own_sem)
    own_copy.start()
    own_copy.wait()
    features_arrived(m, normed_ref, wide, mp_recv)
    norm_rows(normed_ref, gain_ref, normed_ref)
    for copy in copies + shared:
        copy.wait_send()


def output_stage(y, weights, hidden, gain):
    m = lax.axis_size("mp")
    rows, wide = hidden.shape
    vmem = pl.BlockSpec(memory_space=pltpu.VMEM)
    return pl.pallas_call(
        functools.partial(output_kernel, m),
        out_shape=(
            jax.ShapeDtypeStruct((rows, wide), F32),
            jax.ShapeDtypeStruct((rows, wide * m), BF16),
        ),
        in_specs=[vmem] * 4,
        out_specs=(vmem, vmem),
        scratch_shapes=[
            pltpu.VMEM((m - 1, rows, wide), BF16),
            pltpu.VMEM((m - 1, rows, wide), BF16),
            pltpu.VMEM((rows, wide), BF16),
            pltpu.SemaphoreType.DMA((m - 1,)),
            pltpu.SemaphoreType.DMA((m - 1,)),
            pltpu.SemaphoreType.DMA,
            pltpu.SemaphoreType.DMA((m - 1,)),
            pltpu.SemaphoreType.DMA((m - 1,)),
        ],
        compiler_params=pltpu.CompilerParams(
            collective_id=2, has_side_effects=True, vmem_limit_bytes=56 * 1024 * 1024
        ),
        cost_estimate=pl.CostEstimate(
            flops=2 * rows * y.shape[1] * wide * m, bytes_accessed=60_000_000, transcendentals=0
        ),
    )(y, weights, hidden, gain)


def attention_kernel(n, rows, q_ref, k_ref, v_ref, o_ref, peak, total, acc):
    me = lax.axis_index("seq")
    reach = WINDOW // rows
    factor = HD ** (-0.5) * math.log2(math.e)
    query = q_ref[...]
    row_id = lax.broadcasted_iota(jnp.int32, (rows, rows), 0)
    col_id = lax.broadcasted_iota(jnp.int32, (rows, rows), 1)

    def visit(block, allowed, first, count=1):
        here = pl.ds(pl.multiple_of(block * rows, rows), count * rows)
        scores = lax.dot_general(
            query, k_ref[here, :], (((1,), (1,)), ((), ())), preferred_element_type=F32
        )
        if allowed is not None:
            scores = jnp.where(allowed, scores, -1e30)
        top = jnp.max(scores, axis=1, keepdims=True)
        if not first:
            before = peak[...]
            top = jnp.maximum(before, top)
        weights = jnp.exp2((scores - top) * factor)
        added = jnp.sum(weights, axis=1, keepdims=True)
        product = jnp.dot(weights.astype(BF16), v_ref[here, :], preferred_element_type=F32)
        if first:
            total[...] = added
            acc[...] = product
        else:
            shrink = jnp.exp2((before - top) * factor)
            total[...] = total[...] * shrink + added
            acc[...] = acc[...] * shrink + product
        peak[...] = top

    visit(me, row_id >= col_id, True)
    lowest = jnp.maximum(me - reach + 1, 0)

    twos = (me - lowest) // 2

    def body(i, carry_none):
        visit(lowest + 2 * i, None, False, 2)
        return carry_none

    lax.fori_loop(0, twos, body, 0)

    @pl.when(lowest + 2 * twos < me)
    def _():
        visit(me - 1, None, False)

    if n > reach:

        @pl.when(me >= reach)
        def _():
            visit(me - reach, col_id > row_id, False)

    o_ref[...] = acc[...] / total[...]


def attention(queries, pairs, kv_heads):
    n = lax.axis_size("seq")
    rows = queries.shape[0]
    keys = pairs.shape[0]
    per_kv = queries.shape[1] // HD // kv_heads
    return pl.pallas_call(
        functools.partial(attention_kernel, n, rows),
        grid=(kv_heads, per_kv),
        out_shape=jax.ShapeDtypeStruct(queries.shape, F32),
        in_specs=[
            pl.BlockSpec((rows, HD), lambda i, j: (0, i * per_kv + j)),
            pl.BlockSpec((keys, HD), lambda i, j: (0, i)),
            pl.BlockSpec((keys, HD), lambda i, j: (0, kv_heads + i)),
        ],
        out_specs=pl.BlockSpec((rows, HD), lambda i, j: (0, i * per_kv + j)),
        scratch_shapes=[
            pltpu.VMEM((rows, 1), F32),
            pltpu.VMEM((rows, 1), F32),
            pltpu.VMEM((rows, HD), F32),
        ],
        compiler_params=pltpu.CompilerParams(
            dimension_semantics=("arbitrary", "arbitrary"), vmem_limit_bytes=40 * 1024 * 1024
        ),
        cost_estimate=pl.CostEstimate(
            flops=9_000_000_000, bytes_accessed=20_000_000, transcendentals=17_000_000
        ),
    )(queries, pairs, pairs)


def pad_lanes(values):
    return jnp.pad(values, ((0, 0), (0, LANES - values.shape[1])))


def spread_kernel(
    n,
    groups,
    hidden_ref,
    gain_ref,
    wx_ref,
    wz_ref,
    wbc_ref,
    wdt_ref,
    all_ref,
    w_ref,
    dt_ref,
    own,
    cols,
    sums,
    local_sem,
    send_sem,
    recv_sem,
):
    me = lax.axis_index("seq")
    member = lax.axis_index("mp")
    chips = n // 2
    z, c = me // 2, lax.rem(me, 2)
    partner = 2 * z + 1 - c
    across = member + 1 - 2 * lax.rem(member, 2)
    along = lax.rem(member + 2, 4)
    far = 3 - member
    rows, wide = own.shape
    depth = wx_ref.shape[0]
    piece = wx_ref.shape[1] // n
    pair = wbc_ref.shape[1] // groups

    names, started = {}, []

    def sem_of(key):
        return recv_sem.at[names.setdefault(key, len(names))]

    def guarded(cond, body):
        if cond is True:
            body()
        else:
            pl.when(cond)(body)

    def send(cond, make_refs, key, **target):
        index = len(started)

        def make():
            source, place = make_refs()
            return pltpu.make_async_remote_copy(
                src_ref=source,
                dst_ref=place,
                send_sem=send_sem.at[index],
                recv_sem=sem_of(key),
                device_id=target,
                device_id_type=pl.DeviceIdType.MESH,
            )

        started.append((cond, make))
        guarded(cond, lambda: make().start())

    def arrived(cond, make_ref, key):
        def body():
            place = make_ref()
            pltpu.make_async_copy(place, place, sem_of(key)).wait()

        guarded(cond, body)

    def both(first, second):
        return second if first is True else jnp.logical_and(first, second)

    barrier = pltpu.get_barrier_semaphore()
    for d in range(1, n):
        signal_seq(barrier, lax.rem(me + d, n))
    for other in (across, along, far):
        signal_mp(barrier, other)
    pl.semaphore_wait(barrier, n - 1 + 3)

    def rows_of(chip, core):
        return pl.ds(pl.multiple_of((2 * chip + core) * depth, depth), depth)

    def send_weights(way, d, same, cond, chip):
        core = c if same else 1 - c
        target = 2 * chip + core
        here = pl.ds(pl.multiple_of(me * depth, depth), depth)
        take = pl.ds(pl.multiple_of(target * piece, piece), piece)
        group = target * groups // n
        key = ("w", way, d, same)
        send(cond, lambda: (wx_ref.at[:, take], w_ref.at[here, 0:piece]), key, seq=target)
        send(cond, lambda: (wz_ref.at[:, take], w_ref.at[here, piece : 2 * piece]), key, seq=target)
        if same or d == 0:
            send(
                cond,
                lambda: (
                    wbc_ref.at[:, pl.ds(pl.multiple_of(group * pair, pair), pair)],
                    w_ref.at[here, 2 * piece : 2 * piece + pair],
                ),
                key,
                seq=target,
            )
        send(cond, lambda: (wdt_ref, dt_ref.at[:, here]), ("dt", way, d, same), seq=target)

    def weights_at(d):
        for way in (1, -1):
            chip = z + way * d
            cond = chip <= chips - 1 if way == 1 else chip >= 0
            for same in (True, False):
                send_weights(way, d, same, cond, chip)

    send_weights(0, 0, False, True, z)
    here = pl.ds(pl.multiple_of(me * depth, depth), depth)
    take = pl.ds(pl.multiple_of(me * piece, piece), piece)
    group = pl.ds(pl.multiple_of(me * groups // n * pair, pair), pair)
    locals_ = [
        pltpu.make_async_copy(wx_ref.at[:, take], w_ref.at[here, 0:piece], local_sem.at[0]),
        pltpu.make_async_copy(wz_ref.at[:, take], w_ref.at[here, piece : 2 * piece], local_sem.at[1]),
        pltpu.make_async_copy(
            wbc_ref.at[:, group], w_ref.at[here, 2 * piece : 2 * piece + pair], local_sem.at[2]
        ),
        pltpu.make_async_copy(wdt_ref, dt_ref.at[:, here], local_sem.at[3]),
    ]
    for copy in locals_:
        copy.start()

    tile = min(64, rows)

    def square(i, carry):
        at = pl.ds(pl.multiple_of(i * tile, tile), tile)
        v = hidden_ref[at, :].astype(F32)
        cols[at, :] = jnp.broadcast_to(jnp.sum(v * v, axis=-1, keepdims=True), (tile, LANES))
        return carry

    lax.fori_loop(0, rows // tile, square, 0)
    sums[0] = jnp.transpose(cols[...])[0:8, :]
    for i, other in enumerate((across, along, far)):
        send(True, lambda i=i: (sums.at[0], sums.at[i + 1]), ("sum", i), mp=other)
    for i in range(3):
        arrived(True, lambda i=i: sums.at[i + 1], ("sum", i))
    power = sums[0] + sums[1] + sums[2] + sums[3]
    cols[...] = jnp.transpose(jnp.broadcast_to(power[0:1, :], (LANES, rows)))

    def normalise(i, carry):
        at = pl.ds(pl.multiple_of(i * tile, tile), tile)
        scale = lax.rsqrt(cols[at, 0:1] / (4 * wide) + 1e-05)
        own[at, :] = (hidden_ref[at, :].astype(F32) * scale * gain_ref[...]).astype(BF16)
        return carry

    lax.fori_loop(0, rows // tile, normalise, 0)

    def valid(slot):
        kind, d = slot
        return True if d == 0 else z >= d if kind == "b" else z + d <= chips - 1

    def region(slot, owner, half=None, core=None):
        kind, d = slot
        origin = z - d if kind == "b" else z + d
        core = c if core is None else core
        start = (2 * origin + core) * rows
        size = rows
        if half is not None:
            size = rows // 2
            start = start + half * size
        return all_ref.at[
            pl.ds(pl.multiple_of(start, size), size),
            pl.ds(pl.multiple_of(owner * wide, wide), wide),
        ]

    def stage_a(slot):
        kind, d = slot
        ok = valid(slot)
        if d:
            arrived(ok, lambda: region(slot, member), ("col", slot))

        def source():
            return region(slot, member) if d else own

        if d < chips - 1:
            if kind in "ob":
                up = both(ok, z + 1 <= chips - 1)
                send(up, lambda: (source(), region(slot, member)), ("col", ("b", d + 1)), seq=me + 2)
            if kind in "oa":
                down = both(ok, z >= 1)
                send(down, lambda: (source(), region(slot, member)), ("col", ("a", d + 1)), seq=me - 2)
        send(ok, lambda: (source(), region(slot, member)), ("px", slot), mp=across)
        send(ok, lambda: (source(), region(slot, member)), ("py", slot), mp=along)
        send(ok, lambda: (source(), region(slot, member)), ("d", "col", slot), seq=partner)

    def stage_b(slot):
        ok = valid(slot)
        for q, owner, half, nxt in (("px", across, 0, along), ("py", along, 1, across)):
            arrived(ok, lambda: region(slot, owner), (q, slot))
            send(
                ok,
                lambda owner=owner, half=half: (region(slot, owner, half), region(slot, owner, half)),
                ("half", half, slot),
                mp=nxt,
            )
            send(
                ok,
                lambda owner=owner: (region(slot, owner), region(slot, owner)),
                ("d", q, slot),
                seq=partner,
            )

    def stage_c(slot):
        ok = valid(slot)
        for half in range(2):
            arrived(ok, lambda: region(slot, far, half), ("half", half, slot))
        send(ok, lambda: (region(slot, far), region(slot, far)), ("d", "far", slot), seq=partner)

    own_copy = pltpu.make_async_copy(own, region(("o", 0), member), local_sem.at[4])
    own_copy.start()
    locals_.append(own_copy)

    def step(stage, d):
        for slot in ((("o", 0),) if d == 0 else (("b", d), ("a", d))):
            stage(slot)

    last = chips - 1
    for t in range(chips + 2):
        if t <= last:
            step(stage_a, t)
            if last - t >= 1:
                weights_at(last - t)
        if 0 <= t - 1 <= last:
            step(stage_b, t - 1)
        if 0 <= t - 2 <= last:
            step(stage_c, t - 2)

    ways = [(way, d) for d in range(1, chips) for way in (1, -1)]

    def origin_of(way, d):
        chip = z - way * d
        return chip, (chip >= 0 if way == 1 else chip <= chips - 1)

    for way, d in ways:
        chip, ok = origin_of(way, d)
        arrived(ok, lambda: w_ref.at[rows_of(chip, c), :], ("w", way, d, True))

        def shared(chip=chip):
            place = w_ref.at[rows_of(chip, c), 2 * piece : 2 * piece + pair]
            return place, place

        send(ok, shared, ("wd", way, d), seq=partner)
    for way, d in ways:
        chip, ok = origin_of(way, d)
        arrived(ok, lambda: w_ref.at[rows_of(chip, 1 - c), 0 : 2 * piece], ("w", way, d, False))
        arrived(
            ok,
            lambda: w_ref.at[rows_of(chip, 1 - c), 2 * piece : 2 * piece + pair],
            ("wd", way, d),
        )
        for same in (True, False):
            core = c if same else 1 - c
            arrived(ok, lambda: dt_ref.at[:, rows_of(chip, core)], ("dt", way, d, same))
    arrived(True, lambda: w_ref.at[rows_of(z, 1 - c), :], ("w", 0, 0, False))
    arrived(True, lambda: dt_ref.at[:, rows_of(z, 1 - c)], ("dt", 0, 0, False))
    for d in range(chips):
        for slot in ((("o", 0),) if d == 0 else (("b", d), ("a", d))):
            for q, owner in (("col", member), ("px", across), ("py", along), ("far", far)):
                arrived(valid(slot), lambda: region(slot, owner, None, 1 - c), ("d", q, slot))
    for copy in locals_:
        copy.wait()
    for cond, make in started:
        guarded(cond, lambda: make().wait_send())


def spread(hidden, gain, w_x, w_z, w_bc, w_dt, groups):
    n = lax.axis_size("seq")
    rows, wide = hidden.shape
    depth = w_x.shape[0]
    cols = 2 * (w_x.shape[1] // n) + w_bc.shape[1] // groups
    anywhere = pl.BlockSpec(memory_space=pl.ANY)
    vmem = pl.BlockSpec(memory_space=pltpu.VMEM)
    return pl.pallas_call(
        functools.partial(spread_kernel, n, groups),
        out_shape=(
            jax.ShapeDtypeStruct((n * rows, 4 * wide), BF16),
            jax.ShapeDtypeStruct((n * depth, cols), BF16),
            jax.ShapeDtypeStruct((w_dt.shape[0], n * depth), BF16),
        ),
        in_specs=[vmem, vmem] + [anywhere] * 4,
        out_specs=(anywhere,) * 3,
        scratch_shapes=[
            pltpu.VMEM((rows, wide), BF16),
            pltpu.VMEM((rows, LANES), F32),
            pltpu.VMEM((4, 8, rows), F32),
            pltpu.SemaphoreType.DMA((5,)),
            pltpu.SemaphoreType.DMA((45 * n // 2,)),
            pltpu.SemaphoreType.DMA((30 * n // 2,)),
        ],
        compiler_params=pltpu.CompilerParams(
            collective_id=3, has_side_effects=True, vmem_limit_bytes=24 * 1024 * 1024
        ),
        cost_estimate=pl.CostEstimate(
            flops=20_000_000_000, bytes_accessed=100_000_000, transcendentals=0
        ),
    )(hidden, gain, w_x, w_z, w_bc, w_dt)


def heads_kernel(
    n,
    groups,
    hidden_ref,
    w_ref,
    wdt_ref,
    taps_ref,
    bias_ref,
    rate_ref,
    skip_ref,
    gain_ref,
    y_ref,
    blocks,
    wdt_own,
    window,
    gate,
    raws,
    conv,
    state,
    out,
    landed,
    load_sem,
    send_sem,
    recv_sem,
):
    me = lax.axis_index("seq")
    rows = blocks.shape[1]
    inner = gate.shape[1]
    width = inner + 2 * N
    heads = inner // P_SIZE
    kw = taps_ref.shape[0]

    barrier = pltpu.get_barrier_semaphore()
    for d in range(1, n):
        signal_seq(barrier, lax.rem(me + d, n))
    pl.semaphore_wait(barrier, n - 1)

    def load(i, slot):
        return pltpu.make_async_copy(
            hidden_ref.at[pl.ds(pl.multiple_of(i * rows, rows), rows), :],
            blocks.at[slot],
            load_sem.at[slot],
        )

    load(0, 0).start()
    all_heads = wdt_ref.shape[0]
    pick_row = lax.broadcasted_iota(jnp.int32, (LANES, all_heads), 0)
    pick_col = lax.broadcasted_iota(jnp.int32, (LANES, all_heads), 1)
    chosen = jnp.logical_and(pick_col == me * heads + pick_row, pick_row < heads)
    wdt_own[...] = jnp.dot(
        jnp.where(chosen, 1.0, 0.0).astype(BF16), wdt_ref[...], preferred_element_type=F32
    ).astype(BF16)

    lane_head = lax.broadcasted_iota(jnp.int32, (LANES, inner), 1) // P_SIZE
    expand = jnp.where(
        lax.broadcasted_iota(jnp.int32, (LANES, inner), 0) == lane_head, 1.0, 0.0
    ).astype(BF16)
    window[0:8, :] = jnp.zeros((8, width), F32)
    state[...] = jnp.zeros_like(state)
    row_id = lax.broadcasted_iota(jnp.int32, (QB, QB), 0)
    col_id = lax.broadcasted_iota(jnp.int32, (QB, QB), 1)
    causal = row_id >= col_id
    low_lanes = col_id < P_SIZE
    tri = jnp.where(causal, 1.0, 0.0).astype(F32)

    def hand_over(i):
        return pltpu.make_async_remote_copy(
            src_ref=out.at[i],
            dst_ref=landed.at[me],
            send_sem=send_sem.at[i],
            recv_sem=recv_sem.at[me],
            device_id={"seq": i},
            device_id_type=pl.DeviceIdType.MESH,
        )

    def block(i, carry_none):
        slot = lax.rem(i, 2)

        @pl.when(i + 1 < n)
        def _():
            load(i + 1, 1 - slot).start()

        load(i, slot).wait()
        source = blocks.at[slot]
        window[8 : 8 + rows, 0:inner] = jnp.dot(
            source[...], w_ref[:, 0:inner], preferred_element_type=F32
        )
        gate[...] = jnp.dot(source[...], w_ref[:, inner : 2 * inner], preferred_element_type=F32)
        window[8 : 8 + rows, inner:width] = jnp.dot(
            source[...], w_ref[:, 2 * inner : 2 * inner + 2 * N], preferred_element_type=F32
        )
        raws[...] = lax.dot_general(
            source[...], wdt_own[...], (((1,), (1,)), ((), ())), preferred_element_type=F32
        )
        for sub in range(rows // QB):
            at = sub * QB
            here = slice(at, at + QB)
            for start in range(0, width, LANES):
                cs = slice(start, start + LANES)
                total = None
                for j in range(kw):
                    first = 8 - kw + 1 + j + at
                    term = taps_ref[j : j + 1, cs] * window[first : first + QB, cs]
                    total = term if total is None else total + term
                conv[sub, :, cs] = silu(total)
            raw = raws[here, :] + bias_ref[...]
            steps = jnp.maximum(raw, 0.0) + jnp.log1p(jnp.exp(-jnp.abs(raw)))
            decays = -rate_ref[...] * steps
            cum = jnp.dot(tri, decays, precision=HIGH, preferred_element_type=F32)
            cum_t = jnp.transpose(cum)
            grown = jnp.exp(cum)
            tail = jnp.exp(cum[QB - 1 : QB, :] - cum)
            x = conv[sub, :, 0:inner]
            b = conv[sub, :, inner : inner + N].astype(BF16)
            c = conv[sub, :, inner + N : width].astype(BF16)
            scaled = x * spread_heads(steps, expand)
            grown_e = spread_heads(grown, expand)
            tailed = (scaled * spread_heads(tail, expand)).astype(BF16)
            scaled_low = scaled.astype(BF16)
            held = state[...]
            carried = grown_e * jnp.dot(c, held.astype(BF16), preferred_element_type=F32)
            fresh = lax.dot_general(b, tailed, (((0,), (0,)), ((), ())), preferred_element_type=F32)
            state[...] = grown_e[QB - 1 : QB, :] * held + fresh
            affinity = lax.dot_general(c, b, (((1,), (1,)), ((), ())), preferred_element_type=F32)
            affinity = jnp.where(causal, affinity, 0.0)
            full = carried + skip_ref[...] * x
            for pair in range(inner // LANES):
                lanes = slice(pair * LANES, (pair + 1) * LANES)
                outs = []
                for k in range(2):
                    h = pair * 2 + k
                    spread_h = jnp.minimum(cum[:, h : h + 1] - cum_t[h : h + 1, :], 0.0)
                    mixing = (affinity * jnp.exp(spread_h)).astype(BF16)
                    outs.append(
                        jnp.dot(mixing, scaled_low[:, lanes], preferred_element_type=F32)
                    )
                inside = jnp.where(low_lanes, outs[0], outs[1])
                out[i, here, lanes] = (
                    (full[:, lanes] + inside) * silu(gate[here, lanes])
                ).astype(BF16)
        window[0:8, :] = window[rows : rows + 8, :]

        @pl.when(i != me)
        def _():
            hand_over(i).start()

        return carry_none

    lax.fori_loop(0, n, block, 0)

    for s in range(n):

        @pl.when(s != me)
        def _():
            pltpu.make_async_copy(landed.at[s], landed.at[s], recv_sem.at[s]).wait()

        @pl.when(s == me)
        def _():
            landed[s] = out[s]

    per = n // groups
    for g in range(groups):
        members = range(g * per, (g + 1) * per)

        def finish(i, carry_none):
            at = pl.ds(pl.multiple_of(i * QB, QB), QB)
            power = None
            for s in members:
                v = landed[s, at, :].astype(F32)
                part = jnp.sum(v * v, axis=-1, keepdims=True)
                power = part if power is None else power + part
            scale = lax.rsqrt(power / (per * inner) + 1e-05)
            for s in members:
                lanes = slice(s * inner, (s + 1) * inner)
                v = landed[s, at, :].astype(F32)
                y_ref[at, lanes] = (v * scale * gain_ref[:, lanes]).astype(BF16)
            return carry_none

        lax.fori_loop(0, rows // QB, finish, 0)
    for s in range(n):

        @pl.when(s != me)
        def _():
            hand_over(s).wait_send()


def mix_heads(hidden, weights, w_dt, taps, bias, rate, skip, gain, groups):
    n = lax.axis_size("seq")
    rows = hidden.shape[0] // n
    features = hidden.shape[1]
    inner = skip.shape[1]
    width = inner + 2 * N
    vmem = pl.BlockSpec(memory_space=pltpu.VMEM)
    return pl.pallas_call(
        functools.partial(heads_kernel, n, groups),
        out_shape=jax.ShapeDtypeStruct((rows, n * inner), BF16),
        in_specs=[pl.BlockSpec(memory_space=pl.ANY)] + [vmem] * 7,
        out_specs=vmem,
        scratch_shapes=[
            pltpu.VMEM((2, rows, features), BF16),
            pltpu.VMEM((LANES, features), BF16),
            pltpu.VMEM((8 + rows, width), F32),
            pltpu.VMEM((rows, inner), F32),
            pltpu.VMEM((rows, LANES), F32),
            pltpu.VMEM((rows // QB, QB, width), F32),
            pltpu.VMEM((N, inner), F32),
            pltpu.VMEM((n, rows, inner), BF16),
            pltpu.VMEM((n, rows, inner), BF16),
            pltpu.SemaphoreType.DMA((2,)),
            pltpu.SemaphoreType.DMA((n,)),
            pltpu.SemaphoreType.DMA((n,)),
        ],
        compiler_params=pltpu.CompilerParams(
            collective_id=4, has_side_effects=True, vmem_limit_bytes=48 * 1024 * 1024
        ),
        cost_estimate=pl.CostEstimate(
            flops=40_000_000_000, bytes_accessed=50_000_000, transcendentals=8_000_000
        ),
    )(hidden, weights, w_dt, taps, bias, rate, skip, gain)


def own_slice(values, index, size):
    return lax.dynamic_slice_in_dim(values, index * size, size, values.ndim - 1)


def mixer_by_heads(
    hidden_in, norm_gain, w_z, w_x, w_b, w_c, w_dt, conv_x, conv_b, conv_c, dt_bias, a_rate,
    skip_gain, group_gain,
):
    n = lax.axis_size("seq")
    me = lax.axis_index("seq")
    groups = conv_b.shape[1] // N
    inner = conv_x.shape[1] // n
    heads = dt_bias.shape[0] // n
    group = me * groups // n
    pieces = []
    for g in range(groups):
        pieces += [w_b[:, g * N : (g + 1) * N], w_c[:, g * N : (g + 1) * N]]
    gain = own_slice(norm_gain[None, :], lax.axis_index("mp"), hidden_in.shape[1])
    hidden, weights, steps = spread(
        hidden_in, gain, w_x, w_z, jnp.concatenate(pieces, axis=1), jnp.transpose(w_dt), groups
    )
    taps = jnp.concatenate(
        [own_slice(conv_x, me, inner), own_slice(conv_b, group, N), own_slice(conv_c, group, N)],
        axis=1,
    )
    return hidden, functools.partial(
        mix_heads,
        weights=weights,
        w_dt=steps,
        taps=taps,
        bias=pad_lanes(own_slice(dt_bias[None, :], me, heads)),
        rate=pad_lanes(own_slice(a_rate[None, :], me, heads)),
        skip=jnp.repeat(own_slice(skip_gain[None, :], me, heads), P_SIZE, axis=1),
        gain=group_gain[None, :],
        groups=groups,
    )


def splits_by_heads(conv_x, conv_b):
    n, m = lax.axis_size("seq"), lax.axis_size("mp")
    groups = conv_b.shape[1] // N
    whole = conv_x.shape[1] % (n * LANES) == 0 and n % groups == 0
    return m == 4 and n % 2 == 0 and n >= 4 and whole


def on_device(
    hidden_in,
    norm_gain,
    w_z,
    w_x,
    w_b,
    w_c,
    w_dt,
    conv_x,
    conv_b,
    conv_c,
    dt_bias,
    a_rate,
    skip_gain,
    group_gain,
    w_out,
    attn_gain,
    w_q,
    w_k,
    w_v,
):
    if splits_by_heads(conv_x, conv_b):
        hidden, mix = mixer_by_heads(
            hidden_in, norm_gain, w_z, w_x, w_b, w_c, w_dt, conv_x, conv_b, conv_c, dt_bias,
            a_rate, skip_gain, group_gain,
        )
        hidden, w_out = lax.optimization_barrier((hidden, w_out))
        out_columns = lax.all_gather(w_out, "seq", axis=1, tiled=True)
        y_normed = mix(hidden)
    else:
        proj = gather_dot(
            hidden_in,
            norm_gain[None, :],
            jnp.concatenate([w_x, w_b, w_c, pad_lanes(w_dt), w_z], axis=1),
        )
        proj, w_out = lax.optimization_barrier((proj, w_out))
        out_columns = lax.all_gather(w_out, "seq", axis=1, tiled=True)
        heads = dt_bias.shape[0]
        groups = conv_b.shape[1] // N
        width = conv_x.shape[1] + conv_b.shape[1] + conv_c.shape[1]
        rim = from_behind(proj[proj.shape[0] - 8 :, :width], "seq", 1)
        y_normed = mixer(
            proj,
            rim,
            jnp.concatenate([conv_x, conv_b, conv_c], axis=1),
            pad_lanes(dt_bias[None, :]),
            pad_lanes(a_rate[None, :]),
            jnp.repeat(skip_gain, P_SIZE)[None, :],
            group_gain[None, :],
            heads,
            groups,
        )
    mixed, normed_two = output_stage(y_normed, out_columns, hidden_in, attn_gain[None, :])
    own_keys = jnp.dot(normed_two, w_k, preferred_element_type=F32).astype(BF16)
    own_values = jnp.dot(normed_two, w_v, preferred_element_type=F32).astype(BF16)
    pairs = lax.all_gather(
        jnp.concatenate([own_keys, own_values], axis=1), "seq", axis=0, tiled=True
    )
    queries = jnp.dot(normed_two, w_q, preferred_element_type=F32).astype(BF16)
    context = attention(queries, pairs, own_keys.shape[1] // HD)
    return (mixed, context)


def solution(mesh):
    placed = (
        P("seq", "mp"),
        P(),
        P("seq", "mp"),
        P("seq", "mp"),
        P("seq", "mp"),
        P("seq", "mp"),
        P("seq", "mp"),
        P(None, "mp"),
        P(None, "mp"),
        P(None, "mp"),
        P("mp"),
        P("mp"),
        P("mp"),
        P("mp"),
        P("mp", "seq"),
        P(),
        P(None, "mp"),
        P(None, "mp"),
        P(None, "mp"),
    )
    return jax.shard_map(
        on_device,
        mesh=mesh,
        in_specs=placed,
        out_specs=(P("seq", "mp"), P("seq", "mp")),
        check_vma=False,
    )
```

```python
import functools
import math

import jax
import jax.numpy as jnp
from jax import lax
from jax.experimental import pallas as pl
from jax.experimental.pallas import tpu as pltpu
from jax.sharding import PartitionSpec as P

P_SIZE = 64
N = 128
HD = 128
WINDOW = 4096
QB = 128
LANES = 128
VMEM_LIMIT = 62 * 1024 * 1024

HIGH = lax.Precision.HIGHEST
F32 = jnp.float32
BF16 = jnp.bfloat16


def from_behind(block, axis, distance):
    devices = range(lax.axis_size(axis))
    route = [(i - distance, i) for i in devices if i - distance in devices]
    return lax.ppermute(block, axis, route)


def rms_norm(values, gain):
    return values * lax.rsqrt(jnp.mean(values * values, axis=-1, keepdims=True) + 1e-05) * gain


def signal_seq(sem, index):
    pl.semaphore_signal(
        sem, inc=1, device_id={"seq": index}, device_id_type=pl.DeviceIdType.MESH
    )


def signal_mp(sem, index):
    pl.semaphore_signal(
        sem, inc=1, device_id={"mp": index}, device_id_type=pl.DeviceIdType.MESH
    )


def norm_rows(source, gain_ref, target):
    rows = source.shape[0]
    tile = min(64, rows)

    def body(i, carry_none):
        here = pl.ds(pl.multiple_of(i * tile, tile), tile)
        target[here, :] = rms_norm(source[here, :].astype(F32), gain_ref[...]).astype(BF16)
        return carry_none

    lax.fori_loop(0, rows // tile, body, 0)


def share_features(m, source, whole, send_sem, recv_sem):
    member = lax.axis_index("mp")
    wide = source.shape[1]
    own = pl.ds(pl.multiple_of(member * wide, wide), wide)
    copies = [
        pltpu.make_async_remote_copy(
            src_ref=source,
            dst_ref=whole.at[:, own],
            send_sem=send_sem.at[d - 1],
            recv_sem=recv_sem.at[d - 1],
            device_id={"mp": lax.rem(member + d, m)},
            device_id_type=pl.DeviceIdType.MESH,
        )
        for d in range(1, m)
    ]
    for copy in copies:
        copy.start()
    return copies, own


def features_arrived(m, whole, wide, recv_sem):
    member = lax.axis_index("mp")
    for d in range(1, m):
        sender = lax.rem(member - d + m, m)
        there = whole.at[:, pl.ds(pl.multiple_of(sender * wide, wide), wide)]
        pltpu.make_async_copy(there, there, recv_sem.at[d - 1]).wait()


def gather_dot_kernel(
    n,
    m,
    hidden_ref,
    gain_ref,
    w_ref,
    out_ref,
    slots,
    normed_ref,
    local_sem,
    send_sem,
    recv_sem,
    own_sem,
    mp_send_sem,
    mp_recv_sem,
):
    me = lax.axis_index("seq")
    member = lax.axis_index("mp")
    ring = n // 2
    half = ring // 2
    chip, core = me // 2, lax.rem(me, 2)
    up = lax.rem(chip + 1, ring) * 2 + core
    down = lax.rem(chip + ring - 1, ring) * 2 + core
    partner = chip * 2 + 1 - core
    depth, cols = w_ref.shape
    mid = depth // 2

    barrier = pltpu.get_barrier_semaphore()
    for other in (up, down, partner):
        signal_seq(barrier, other)
    for d in range(1, m):
        signal_mp(barrier, lax.rem(member + d, m))
    pl.semaphore_wait(barrier, 3 + m - 1)

    shared, own = share_features(m, hidden_ref, normed_ref, mp_send_sem, mp_recv_sem)
    own_copy = pltpu.make_async_copy(hidden_ref, normed_ref.at[:, own], own_sem)
    own_copy.start()
    local = pltpu.make_async_copy(w_ref, slots.at[0], local_sem)
    local.start()
    started = []

    def send(source, slot, rows, part, target):
        copy = pltpu.make_async_remote_copy(
            src_ref=source,
            dst_ref=slots.at[slot, rows],
            send_sem=send_sem.at[len(started)],
            recv_sem=recv_sem.at[2 * slot + part],
            device_id={"seq": target},
            device_id_type=pl.DeviceIdType.MESH,
        )
        copy.start()
        started.append(copy)

    def arrived(slot, rows, part):
        pltpu.make_async_copy(
            slots.at[slot, rows], slots.at[slot, rows], recv_sem.at[2 * slot + part]
        ).wait()

    whole, upper, lower = pl.ds(0, depth), pl.ds(0, mid), pl.ds(mid, mid)
    send(w_ref, 2 * 1, whole, 0, up)
    send(w_ref, 2 * (ring - 1), whole, 0, down)
    send(w_ref, 1, whole, 0, partner)

    def multiply(slot, first=False):
        step, lane = slot // 2, slot % 2
        origin = lax.rem(chip - step + ring, ring) * 2
        owner = origin + (core if lane == 0 else 1 - core)
        features = pl.ds(pl.multiple_of(owner * depth, depth), depth)

        def tile(start, width):
            where = pl.ds(start, width)
            product = jnp.dot(
                normed_ref[:, features], slots[slot, :, where], preferred_element_type=F32
            )
            if first:
                out_ref[:, where] = product
            else:
                out_ref[:, where] += product

        width = 512
        full = cols // width

        def body(i, carry):
            tile(pl.multiple_of(i * width, width), width)
            return carry

        lax.fori_loop(0, full, body, 0)
        if cols % width:
            tile(full * width, cols % width)

    own_copy.wait()
    features_arrived(m, normed_ref, hidden_ref.shape[1], mp_recv_sem)
    norm_rows(normed_ref, gain_ref, normed_ref)
    local.wait()
    multiply(0, True)
    arrived(1, whole, 0)
    multiply(1)
    for d in range(1, half):
        s_up, s_down = 2 * d, 2 * (ring - d)
        last = d + 1 == half
        arrived(s_up, whole, 0)
        rows = upper if last else whole
        send(slots.at[s_up, rows], 2 * (d + 1), rows, 0, up)
        arrived(s_down, whole, 0)
        rows = lower if last else whole
        send(slots.at[s_down, rows], 2 * (ring - d - 1), rows, 1 if last else 0, down)
        send(slots.at[s_up, whole], s_up + 1, whole, 0, partner)
        send(slots.at[s_down, whole], s_down + 1, whole, 0, partner)
        multiply(s_up)
        multiply(s_down)
        arrived(s_up + 1, whole, 0)
        multiply(s_up + 1)
        arrived(s_down + 1, whole, 0)
        multiply(s_down + 1)
    far = 2 * half
    arrived(far, upper, 0)
    send(slots.at[far, upper], far + 1, upper, 0, partner)
    arrived(far, lower, 1)
    send(slots.at[far, lower], far + 1, lower, 1, partner)
    multiply(far)
    arrived(far + 1, upper, 0)
    arrived(far + 1, lower, 1)
    multiply(far + 1)
    for copy in started + shared:
        copy.wait_send()


def gather_dot(hidden, gain, weights):
    n, m = lax.axis_size("seq"), lax.axis_size("mp")
    depth, cols = weights.shape
    rows, features = hidden.shape[0], hidden.shape[1] * m
    ring = n // 2
    sends = 3 + 4 * (ring // 2 - 1) + 2
    return pl.pallas_call(
        functools.partial(gather_dot_kernel, n, m),
        out_shape=jax.ShapeDtypeStruct((rows, cols), F32),
        in_specs=[
            pl.BlockSpec(memory_space=pl.ANY),
            pl.BlockSpec(memory_space=pltpu.VMEM),
            pl.BlockSpec(memory_space=pl.ANY),
        ],
        out_specs=pl.BlockSpec(memory_space=pltpu.VMEM),
        scratch_shapes=[
            pltpu.VMEM((n, depth, cols), BF16),
            pltpu.VMEM((rows, features), BF16),
            pltpu.SemaphoreType.DMA,
            pltpu.SemaphoreType.DMA((sends,)),
            pltpu.SemaphoreType.DMA((2 * n,)),
            pltpu.SemaphoreType.DMA,
            pltpu.SemaphoreType.DMA((m - 1,)),
            pltpu.SemaphoreType.DMA((m - 1,)),
        ],
        compiler_params=pltpu.CompilerParams(
            collective_id=0, has_side_effects=True, vmem_limit_bytes=VMEM_LIMIT
        ),
        cost_estimate=pl.CostEstimate(
            flops=2 * rows * features * cols,
            bytes_accessed=160_000_000,
            transcendentals=0,
        ),
    )(hidden, gain, weights)


def silu(v):
    return v / (1.0 + jnp.exp(-v))


def spread_heads(values, expand):
    high = values.astype(BF16)
    low = (values - high.astype(F32)).astype(BF16)
    return jnp.dot(high, expand, preferred_element_type=F32) + jnp.dot(
        low, expand, preferred_element_type=F32
    )


def mixer_kernel(
    n,
    heads,
    groups,
    proj_ref,
    rim_ref,
    taps_ref,
    bias_ref,
    rate_ref,
    skip_ref,
    gain_ref,
    expand_ref,
    y_ref,
    window,
    conv,
    ssd,
    reads,
    logs,
    state,
    carry,
    state_out,
    state_in,
    send_sem,
    recv_sem,
):
    me = lax.axis_index("seq")
    rows = proj_ref.shape[0]
    inner = heads * P_SIZE
    width = inner + 2 * groups * N
    gate_at = width + LANES
    per_group = inner // groups
    blocks = rows // QB
    kw = taps_ref.shape[0]

    barrier = pltpu.get_barrier_semaphore()
    signal_seq(barrier, lax.rem(me + 1, n))
    signal_seq(barrier, lax.rem(me + n - 1, n))
    pl.semaphore_wait(barrier, 2)

    expand = expand_ref[...]
    window[0:8, :] = rim_ref[...]
    state[...] = jnp.zeros_like(state)
    carry[...] = jnp.zeros_like(carry)
    row_id = lax.broadcasted_iota(jnp.int32, (QB, QB), 0)
    col_id = lax.broadcasted_iota(jnp.int32, (QB, QB), 1)
    causal = row_id >= col_id
    low_lanes = col_id < P_SIZE
    tri = jnp.where(causal, 1.0, 0.0).astype(F32)

    def block(i, carry_none):
        base = pl.multiple_of(i * QB, QB)
        here = pl.ds(base, QB)
        window[8 : 8 + QB, :] = proj_ref[here, 0:width]
        step_cols = 256 if width % 256 == 0 else 128
        for at in range(0, width, step_cols):
            cs = slice(at, at + step_cols)
            total = None
            for j in range(kw):
                term = taps_ref[j : j + 1, cs] * window[8 - kw + 1 + j : 8 - kw + 1 + j + QB, cs]
                total = term if total is None else total + term
            conv[:, cs] = silu(total)
        window[0:8, :] = window[QB : QB + 8, :]

        raw = proj_ref[here, width : width + LANES] + bias_ref[...]
        steps = jnp.maximum(raw, 0.0) + jnp.log1p(jnp.exp(-jnp.abs(raw)))
        decays = -rate_ref[...] * steps
        cum = jnp.dot(tri, decays, precision=HIGH, preferred_element_type=F32)
        cum_t = jnp.transpose(cum)
        logs[here, :] = cum + carry[0:1, :]
        carry[...] = carry[...] + cum[QB - 1 : QB, :]
        grown = jnp.exp(cum)
        tail = jnp.exp(cum[QB - 1 : QB, :] - cum)

        for g in range(groups):
            lanes = slice(g * per_group, (g + 1) * per_group)
            expand_g = expand[:, lanes]
            x = conv[:, lanes]
            b = conv[:, inner + g * N : inner + (g + 1) * N].astype(BF16)
            c = conv[:, inner + (groups + g) * N : inner + (groups + g + 1) * N].astype(BF16)
            reads[here, g * N : (g + 1) * N] = c
            scaled = x * spread_heads(steps, expand_g)
            grown_e = spread_heads(grown, expand_g)
            tailed = (scaled * spread_heads(tail, expand_g)).astype(BF16)
            scaled_low = scaled.astype(BF16)
            held = state[:, lanes]
            carried = grown_e * jnp.dot(c, held.astype(BF16), preferred_element_type=F32)
            ssd[here, lanes] = carried + skip_ref[:, lanes] * x
            fresh = lax.dot_general(
                b, tailed, (((0,), (0,)), ((), ())), preferred_element_type=F32
            )
            state[:, lanes] = grown_e[QB - 1 : QB, :] * held + fresh
            affinity = lax.dot_general(
                c, b, (((1,), (1,)), ((), ())), preferred_element_type=F32
            )
            affinity = jnp.where(causal, affinity, 0.0)
            for pair in range(per_group // LANES):
                at = pair * LANES
                inputs = scaled_low[:, at : at + LANES]
                outs = []
                for k in range(2):
                    h = (g * per_group + at) // P_SIZE + k
                    spread = jnp.minimum(cum[:, h : h + 1] - cum_t[h : h + 1, :], 0.0)
                    mixing = (affinity * jnp.exp(spread)).astype(BF16)
                    outs.append(jnp.dot(mixing, inputs, preferred_element_type=F32))
                where = slice(g * per_group + at, g * per_group + at + LANES)
                ssd[here, where] += jnp.where(low_lanes, outs[0], outs[1])
        return carry_none

    lax.fori_loop(0, blocks, block, 0)

    parts = 4
    piece = inner // parts
    decay = jnp.exp(carry[...])

    def hand_on(k):
        lanes = slice(k * piece, (k + 1) * piece)
        return pltpu.make_async_remote_copy(
            src_ref=state_out.at[:, lanes],
            dst_ref=state_in.at[:, lanes],
            send_sem=send_sem.at[k],
            recv_sem=recv_sem.at[k],
            device_id={"seq": jnp.minimum(me + 1, n - 1)},
            device_id_type=pl.DeviceIdType.MESH,
        )

    for k in range(parts):
        lanes = slice(k * piece, (k + 1) * piece)
        weight = spread_heads(decay, expand[:, lanes])[0:1, :]

        @pl.when(me > 0)
        def _():
            hand_on(k).wait_recv()
            before = state_in[:, lanes].astype(F32)
            state_out[:, lanes] = (weight * before + state[:, lanes]).astype(BF16)

        @pl.when(me == 0)
        def _():
            state_out[:, lanes] = state[:, lanes].astype(BF16)
            state_in[:, lanes] = jnp.zeros((N, piece), BF16)

        @pl.when(me < n - 1)
        def _():
            hand_on(k).start()

    def finish(i, carry_none):
        here = pl.ds(pl.multiple_of(i * QB, QB), QB)
        grown = jnp.exp(logs[here, :])
        for g in range(groups):
            lanes = slice(g * per_group, (g + 1) * per_group)
            late = jnp.dot(
                reads[here, g * N : (g + 1) * N],
                state_in[:, lanes],
                preferred_element_type=F32,
            )
            full = ssd[here, lanes] + spread_heads(grown, expand[:, lanes]) * late
            gate = proj_ref[here, gate_at + g * per_group : gate_at + (g + 1) * per_group]
            gated = full * silu(gate)
            power = jnp.mean(gated * gated, axis=-1, keepdims=True)
            y_ref[here, lanes] = (gated * lax.rsqrt(power + 1e-05) * gain_ref[:, lanes]).astype(BF16)
        return carry_none

    lax.fori_loop(0, blocks, finish, 0)

    @pl.when(me < n - 1)
    def _():
        for k in range(parts):
            hand_on(k).wait_send()


def mixer(proj, rim, taps, bias, rate, skip, gain, heads, groups):
    n = lax.axis_size("seq")
    rows = proj.shape[0]
    inner = heads * P_SIZE
    width = inner + 2 * groups * N
    expand = (
        jnp.arange(LANES)[:, None] == (jnp.arange(inner) // P_SIZE)[None, :]
    ).astype(BF16)
    vmem = pl.BlockSpec(memory_space=pltpu.VMEM)
    return pl.pallas_call(
        functools.partial(mixer_kernel, n, heads, groups),
        out_shape=jax.ShapeDtypeStruct((rows, inner), BF16),
        in_specs=[vmem] * 8,
        out_specs=vmem,
        scratch_shapes=[
            pltpu.VMEM((8 + QB, width), F32),
            pltpu.VMEM((QB, width), F32),
            pltpu.VMEM((rows, inner), F32),
            pltpu.VMEM((rows, groups * N), BF16),
            pltpu.VMEM((rows, LANES), F32),
            pltpu.VMEM((N, inner), F32),
            pltpu.VMEM((8, LANES), F32),
            pltpu.VMEM((N, inner), BF16),
            pltpu.VMEM((N, inner), BF16),
            pltpu.SemaphoreType.DMA((4,)),
            pltpu.SemaphoreType.DMA((4,)),
        ],
        compiler_params=pltpu.CompilerParams(
            collective_id=1, has_side_effects=True, vmem_limit_bytes=48 * 1024 * 1024
        ),
        cost_estimate=pl.CostEstimate(
            flops=8_000_000_000, bytes_accessed=100_000_000, transcendentals=8_000_000
        ),
    )(proj, rim, taps, bias, rate, skip, gain, expand)


def output_kernel(
    m,
    y_ref,
    w_ref,
    hidden_ref,
    gain_ref,
    mixed_ref,
    normed_ref,
    outgoing,
    incoming,
    low,
    part_send,
    part_recv,
    own_sem,
    mp_send,
    mp_recv,
):
    member = lax.axis_index("mp")
    wide = hidden_ref.shape[1]
    barrier = pltpu.get_barrier_semaphore()
    for d in range(1, m):
        signal_mp(barrier, lax.rem(member + d, m))
    pl.semaphore_wait(barrier, m - 1)
    tile = min(512, wide)

    def part(target, store):
        for at in range(0, wide, tile):
            where = pl.ds(pl.multiple_of(target * wide + at, tile), tile)
            term = jnp.dot(y_ref[...], w_ref[:, where], preferred_element_type=F32)
            store(slice(at, at + tile), term.astype(BF16))

    copies = []
    for d in range(1, m):
        target = lax.rem(member + d, m)

        def keep(where, term):
            outgoing[d - 1, :, where] = term

        part(target, keep)
        copy = pltpu.make_async_remote_copy(
            src_ref=outgoing.at[d - 1],
            dst_ref=incoming.at[d - 1],
            send_sem=part_send.at[d - 1],
            recv_sem=part_recv.at[d - 1],
            device_id={"mp": target},
            device_id_type=pl.DeviceIdType.MESH,
        )
        copy.start()
        copies.append(copy)

    def begin(where, term):
        mixed_ref[:, where] = hidden_ref[:, where].astype(F32) + term.astype(F32)

    part(member, begin)
    for d in range(1, m):
        copies[d - 1].wait_recv()
        if d < m - 1:
            mixed_ref[...] += incoming[d - 1].astype(F32)
        else:
            total = mixed_ref[...] + incoming[d - 1].astype(F32)
            mixed_ref[...] = total
            low[...] = total.astype(BF16)
    shared, own = share_features(m, low, normed_ref, mp_send, mp_recv)
    own_copy = pltpu.make_async_copy(low, normed_ref.at[:, own], own_sem)
    own_copy.start()
    own_copy.wait()
    features_arrived(m, normed_ref, wide, mp_recv)
    norm_rows(normed_ref, gain_ref, normed_ref)
    for copy in copies + shared:
        copy.wait_send()


def output_stage(y, weights, hidden, gain):
    m = lax.axis_size("mp")
    rows, wide = hidden.shape
    vmem = pl.BlockSpec(memory_space=pltpu.VMEM)
    return pl.pallas_call(
        functools.partial(output_kernel, m),
        out_shape=(
            jax.ShapeDtypeStruct((rows, wide), F32),
            jax.ShapeDtypeStruct((rows, wide * m), BF16),
        ),
        in_specs=[vmem] * 4,
        out_specs=(vmem, vmem),
        scratch_shapes=[
            pltpu.VMEM((m - 1, rows, wide), BF16),
            pltpu.VMEM((m - 1, rows, wide), BF16),
            pltpu.VMEM((rows, wide), BF16),
            pltpu.SemaphoreType.DMA((m - 1,)),
            pltpu.SemaphoreType.DMA((m - 1,)),
            pltpu.SemaphoreType.DMA,
            pltpu.SemaphoreType.DMA((m - 1,)),
            pltpu.SemaphoreType.DMA((m - 1,)),
        ],
        compiler_params=pltpu.CompilerParams(
            collective_id=2, has_side_effects=True, vmem_limit_bytes=56 * 1024 * 1024
        ),
        cost_estimate=pl.CostEstimate(
            flops=2 * rows * y.shape[1] * wide * m, bytes_accessed=60_000_000, transcendentals=0
        ),
    )(y, weights, hidden, gain)


def attention_kernel(n, rows, q_ref, k_ref, v_ref, o_ref, peak, total, acc):
    me = lax.axis_index("seq")
    reach = WINDOW // rows
    factor = HD ** (-0.5) * math.log2(math.e)
    query = q_ref[...]
    row_id = lax.broadcasted_iota(jnp.int32, (rows, rows), 0)
    col_id = lax.broadcasted_iota(jnp.int32, (rows, rows), 1)

    def visit(block, allowed, first, count=1):
        here = pl.ds(pl.multiple_of(block * rows, rows), count * rows)
        scores = lax.dot_general(
            query, k_ref[here, :], (((1,), (1,)), ((), ())), preferred_element_type=F32
        )
        if allowed is not None:
            scores = jnp.where(allowed, scores, -1e30)
        top = jnp.max(scores, axis=1, keepdims=True)
        if not first:
            before = peak[...]
            top = jnp.maximum(before, top)
        weights = jnp.exp2((scores - top) * factor)
        added = jnp.sum(weights, axis=1, keepdims=True)
        product = jnp.dot(weights.astype(BF16), v_ref[here, :], preferred_element_type=F32)
        if first:
            total[...] = added
            acc[...] = product
        else:
            shrink = jnp.exp2((before - top) * factor)
            total[...] = total[...] * shrink + added
            acc[...] = acc[...] * shrink + product
        peak[...] = top

    visit(me, row_id >= col_id, True)
    lowest = jnp.maximum(me - reach + 1, 0)

    twos = (me - lowest) // 2

    def body(i, carry_none):
        visit(lowest + 2 * i, None, False, 2)
        return carry_none

    lax.fori_loop(0, twos, body, 0)

    @pl.when(lowest + 2 * twos < me)
    def _():
        visit(me - 1, None, False)

    if n > reach:

        @pl.when(me >= reach)
        def _():
            visit(me - reach, col_id > row_id, False)

    o_ref[...] = acc[...] / total[...]


def attention(queries, pairs, kv_heads):
    n = lax.axis_size("seq")
    rows = queries.shape[0]
    keys = pairs.shape[0]
    per_kv = queries.shape[1] // HD // kv_heads
    return pl.pallas_call(
        functools.partial(attention_kernel, n, rows),
        grid=(kv_heads, per_kv),
        out_shape=jax.ShapeDtypeStruct(queries.shape, F32),
        in_specs=[
            pl.BlockSpec((rows, HD), lambda i, j: (0, i * per_kv + j)),
            pl.BlockSpec((keys, HD), lambda i, j: (0, i)),
            pl.BlockSpec((keys, HD), lambda i, j: (0, kv_heads + i)),
        ],
        out_specs=pl.BlockSpec((rows, HD), lambda i, j: (0, i * per_kv + j)),
        scratch_shapes=[
            pltpu.VMEM((rows, 1), F32),
            pltpu.VMEM((rows, 1), F32),
            pltpu.VMEM((rows, HD), F32),
        ],
        compiler_params=pltpu.CompilerParams(
            dimension_semantics=("arbitrary", "arbitrary"), vmem_limit_bytes=40 * 1024 * 1024
        ),
        cost_estimate=pl.CostEstimate(
            flops=9_000_000_000, bytes_accessed=20_000_000, transcendentals=17_000_000
        ),
    )(queries, pairs, pairs)


def line_attention_kernel(
    n,
    nt_ref,
    wq_ref,
    wk_ref,
    wv_ref,
    o_ref,
    keys,
    values,
    queries,
    peak,
    total,
    acc,
    send_sem,
    recv_sem,
):
    me = lax.axis_index("seq")
    chips = n // 2
    z, c = me // 2, lax.rem(me, 2)
    partner = 2 * z + 1 - c
    rows = nt_ref.shape[0]
    kv_heads = wk_ref.shape[1] // HD
    per_kv = wq_ref.shape[1] // HD // kv_heads
    factor = HD ** (-0.5) * math.log2(math.e)

    barrier = pltpu.get_barrier_semaphore()
    signal_seq(barrier, partner)
    has_up, has_down = z + 1 <= chips - 1, z >= 1

    @pl.when(has_up)
    def _():
        signal_seq(barrier, me + 2)

    @pl.when(has_down)
    def _():
        signal_seq(barrier, me - 2)

    inner_chip = jnp.logical_and(has_up, has_down)

    @pl.when(inner_chip)
    def _():
        pl.semaphore_wait(barrier, 3)

    @pl.when(jnp.logical_not(inner_chip))
    def _():
        pl.semaphore_wait(barrier, 2)

    stores = (keys, values)

    def copies(slot, kind, d, target):
        return [
            pltpu.make_async_remote_copy(
                src_ref=store.at[slot],
                dst_ref=store.at[slot],
                send_sem=send_sem.at[kind, d, which],
                recv_sem=recv_sem.at[kind, d, which],
                device_id={"seq": target},
                device_id_type=pl.DeviceIdType.MESH,
            )
            for which, store in enumerate(stores)
        ]

    def send(slot, kind, d, target):
        for copy in copies(slot, kind, d, target):
            copy.start()

    def sent(slot, kind, d, target):
        for copy in copies(slot, kind, d, target):
            copy.wait_send()

    def arrived(slot, kind, d):
        for which, store in enumerate(stores):
            place = store.at[slot]
            pltpu.make_async_copy(place, place, recv_sem.at[kind, d, which]).wait()

    keys[me] = jnp.dot(nt_ref[...], wk_ref[...], preferred_element_type=F32).astype(BF16)
    values[me] = jnp.transpose(
        jnp.dot(nt_ref[...], wv_ref[...], preferred_element_type=F32)
    ).astype(BF16)

    @pl.when(has_up)
    def _():
        send(me, 0, 1, me + 2)

    @pl.when(c == 0)
    def _():
        send(me, 1, 0, partner)

    tile = min(256, wq_ref.shape[1])
    for at in range(0, wq_ref.shape[1], tile):
        queries[:, at : at + tile] = jnp.dot(
            nt_ref[...], wq_ref[:, at : at + tile], preferred_element_type=F32
        ).astype(BF16)

    def visit(block, first):
        def group(g, carry_none):
            lanes = pl.ds(pl.multiple_of(g * HD, HD), HD)
            key = keys[block, :, lanes]
            value = values[block, lanes, :]
            for j in range(per_kv):
                h = g * per_kv + j
                query = queries[:, pl.ds(pl.multiple_of(h * HD, HD), HD)]
                scores = lax.dot_general(
                    key, query, (((1,), (1,)), ((), ())), preferred_element_type=F32
                )
                if first:
                    row_id = lax.broadcasted_iota(jnp.int32, (rows, rows), 0)
                    col_id = lax.broadcasted_iota(jnp.int32, (rows, rows), 1)
                    scores = jnp.where(row_id <= col_id, scores, -1e30)
                top = jnp.max(scores, axis=0, keepdims=True)
                if not first:
                    before = peak[h]
                    top = jnp.maximum(before, top)
                weights = jnp.exp2((scores - top) * factor)
                added = jnp.sum(weights, axis=0, keepdims=True)
                product = jnp.dot(value, weights.astype(BF16), preferred_element_type=F32)
                if first:
                    total[h] = added
                    acc[h] = product
                else:
                    shrink = jnp.exp2((before - top) * factor)
                    total[h] = total[h] * shrink + added
                    acc[h] = acc[h] * shrink + product
                peak[h] = top
            return carry_none

        lax.fori_loop(0, kv_heads, group, 0)

    visit(me, True)

    def earlier(t, carry_none):
        d = (t + 1) // 2
        mine = me - 2 * d
        theirs = partner - 2 * d

        @pl.when(lax.rem(t, 2) == 1)
        def _():
            arrived(mine, 0, d)

            @pl.when(has_up)
            def _():
                send(mine, 0, d + 1, me + 2)

            send(mine, 1, d, partner)

        @pl.when(lax.rem(t, 2) == 0)
        def _():
            arrived(theirs, 1, d)

        visit(partner - 2 * d + lax.rem(t, 2) * (me - partner), False)
        return carry_none

    lax.fori_loop(1 - c, 2 * z + 1, earlier, 0)

    for h in range(kv_heads * per_kv):
        o_ref[:, h * HD : (h + 1) * HD] = jnp.transpose(acc[h] / total[h])

    @pl.when(has_up)
    def _():
        sent(me, 0, 1, me + 2)

    @pl.when(c == 0)
    def _():
        sent(me, 1, 0, partner)

    def flush(d, carry_none):
        @pl.when(has_up)
        def _():
            sent(me - 2 * d, 0, d + 1, me + 2)

        sent(me - 2 * d, 1, d, partner)
        return carry_none

    lax.fori_loop(1, z + 1, flush, 0)


def line_attention(normed_two, w_q, w_k, w_v):
    n = lax.axis_size("seq")
    rows = normed_two.shape[0]
    heads = w_q.shape[1] // HD
    wide = w_k.shape[1]
    chips = n // 2
    vmem = pl.BlockSpec(memory_space=pltpu.VMEM)
    return pl.pallas_call(
        functools.partial(line_attention_kernel, n),
        out_shape=jax.ShapeDtypeStruct((rows, w_q.shape[1]), F32),
        in_specs=[vmem] * 4,
        out_specs=vmem,
        scratch_shapes=[
            pltpu.VMEM((n, rows, wide), BF16),
            pltpu.VMEM((n, wide, rows), BF16),
            pltpu.VMEM((rows, w_q.shape[1]), BF16),
            pltpu.VMEM((heads, 1, rows), F32),
            pltpu.VMEM((heads, 1, rows), F32),
            pltpu.VMEM((heads, HD, rows), F32),
            pltpu.SemaphoreType.DMA((2, chips, 2)),
            pltpu.SemaphoreType.DMA((2, chips, 2)),
        ],
        compiler_params=pltpu.CompilerParams(
            collective_id=5, has_side_effects=True, vmem_limit_bytes=56 * 1024 * 1024
        ),
        cost_estimate=pl.CostEstimate(
            flops=18_000_000_000, bytes_accessed=30_000_000, transcendentals=17_000_000
        ),
    )(normed_two, w_q, w_k, w_v)


def pad_lanes(values):
    return jnp.pad(values, ((0, 0), (0, LANES - values.shape[1])))


def spread_kernel(
    n,
    groups,
    hidden_ref,
    gain_ref,
    wx_ref,
    wz_ref,
    wbc_ref,
    wdt_ref,
    all_ref,
    w_ref,
    dt_ref,
    own,
    cols,
    sums,
    local_sem,
    send_sem,
    recv_sem,
):
    me = lax.axis_index("seq")
    member = lax.axis_index("mp")
    chips = n // 2
    z, c = me // 2, lax.rem(me, 2)
    partner = 2 * z + 1 - c
    across = member + 1 - 2 * lax.rem(member, 2)
    along = lax.rem(member + 2, 4)
    far = 3 - member
    rows, wide = own.shape
    depth = wx_ref.shape[0]
    piece = wx_ref.shape[1] // n
    pair = wbc_ref.shape[1] // groups

    names, started = {}, []

    def sem_of(key):
        return recv_sem.at[names.setdefault(key, len(names))]

    def guarded(cond, body):
        if cond is True:
            body()
        else:
            pl.when(cond)(body)

    def send(cond, make_refs, key, **target):
        index = len(started)

        def make():
            source, place = make_refs()
            return pltpu.make_async_remote_copy(
                src_ref=source,
                dst_ref=place,
                send_sem=send_sem.at[index],
                recv_sem=sem_of(key),
                device_id=target,
                device_id_type=pl.DeviceIdType.MESH,
            )

        started.append((cond, make))
        guarded(cond, lambda: make().start())

    def arrived(cond, make_ref, key):
        def body():
            place = make_ref()
            pltpu.make_async_copy(place, place, sem_of(key)).wait()

        guarded(cond, body)

    def both(first, second):
        return second if first is True else jnp.logical_and(first, second)

    barrier = pltpu.get_barrier_semaphore()
    for d in range(1, n):
        signal_seq(barrier, lax.rem(me + d, n))
    for other in (across, along, far):
        signal_mp(barrier, other)
    pl.semaphore_wait(barrier, n - 1 + 3)

    def rows_of(chip, core):
        return pl.ds(pl.multiple_of((2 * chip + core) * depth, depth), depth)

    def send_weights(way, d, same, cond, chip):
        core = c if same else 1 - c
        target = 2 * chip + core
        here = pl.ds(pl.multiple_of(me * depth, depth), depth)
        take = pl.ds(pl.multiple_of(target * piece, piece), piece)
        group = target * groups // n
        key = ("w", way, d, same)
        send(cond, lambda: (wx_ref.at[:, take], w_ref.at[here, 0:piece]), key, seq=target)
        send(cond, lambda: (wz_ref.at[:, take], w_ref.at[here, piece : 2 * piece]), key, seq=target)
        if same or d == 0:
            send(
                cond,
                lambda: (
                    wbc_ref.at[:, pl.ds(pl.multiple_of(group * pair, pair), pair)],
                    w_ref.at[here, 2 * piece : 2 * piece + pair],
                ),
                key,
                seq=target,
            )
        send(cond, lambda: (wdt_ref, dt_ref.at[:, here]), ("dt", way, d, same), seq=target)

    def weights_at(t):
        for d in range(1, chips - (t if t > 1 else 0)):
            for way in (1, -1):
                chip = z + way * d
                behind = z if way == 1 else chips - 1 - z
                now = behind <= 1 if t == 1 else behind == t
                cond = both(now, chip <= chips - 1 if way == 1 else chip >= 0)
                for same in (True, False):
                    send_weights(way, d, same, cond, chip)

    send_weights(0, 0, False, True, z)
    here = pl.ds(pl.multiple_of(me * depth, depth), depth)
    take = pl.ds(pl.multiple_of(me * piece, piece), piece)
    group = pl.ds(pl.multiple_of(me * groups // n * pair, pair), pair)
    locals_ = [
        pltpu.make_async_copy(wx_ref.at[:, take], w_ref.at[here, 0:piece], local_sem.at[0]),
        pltpu.make_async_copy(wz_ref.at[:, take], w_ref.at[here, piece : 2 * piece], local_sem.at[1]),
        pltpu.make_async_copy(
            wbc_ref.at[:, group], w_ref.at[here, 2 * piece : 2 * piece + pair], local_sem.at[2]
        ),
        pltpu.make_async_copy(wdt_ref, dt_ref.at[:, here], local_sem.at[3]),
    ]
    for copy in locals_:
        copy.start()

    tile = min(64, rows)

    def square(i, carry):
        at = pl.ds(pl.multiple_of(i * tile, tile), tile)
        v = hidden_ref[at, :].astype(F32)
        cols[at, :] = jnp.broadcast_to(jnp.sum(v * v, axis=-1, keepdims=True), (tile, LANES))
        return carry

    lax.fori_loop(0, rows // tile, square, 0)
    sums[0] = jnp.transpose(cols[...])[0:8, :]
    for i, other in enumerate((across, along, far)):
        send(True, lambda i=i: (sums.at[0], sums.at[i + 1]), ("sum", i), mp=other)
    for i in range(3):
        arrived(True, lambda i=i: sums.at[i + 1], ("sum", i))
    power = sums[0] + sums[1] + sums[2] + sums[3]
    cols[...] = jnp.transpose(jnp.broadcast_to(power[0:1, :], (LANES, rows)))

    def normalise(i, carry):
        at = pl.ds(pl.multiple_of(i * tile, tile), tile)
        scale = lax.rsqrt(cols[at, 0:1] / (4 * wide) + 1e-05)
        own[at, :] = (hidden_ref[at, :].astype(F32) * scale * gain_ref[...]).astype(BF16)
        return carry

    lax.fori_loop(0, rows // tile, normalise, 0)

    def valid(slot):
        kind, d = slot
        return True if d == 0 else z >= d if kind == "b" else z + d <= chips - 1

    def region(slot, owner, half=None, core=None):
        kind, d = slot
        origin = z - d if kind == "b" else z + d
        core = c if core is None else core
        start = (2 * origin + core) * rows
        size = rows
        if half is not None:
            size = rows // 2
            start = start + half * size
        return all_ref.at[
            pl.ds(pl.multiple_of(start, size), size),
            pl.ds(pl.multiple_of(owner * wide, wide), wide),
        ]

    def stage_a(slot):
        kind, d = slot
        ok = valid(slot)
        if d:
            arrived(ok, lambda: region(slot, member), ("col", slot))

        def source():
            return region(slot, member) if d else own

        if d < chips - 1:
            if kind in "ob":
                up = both(ok, z + 1 <= chips - 1)
                send(up, lambda: (source(), region(slot, member)), ("col", ("b", d + 1)), seq=me + 2)
            if kind in "oa":
                down = both(ok, z >= 1)
                send(down, lambda: (source(), region(slot, member)), ("col", ("a", d + 1)), seq=me - 2)
        send(ok, lambda: (source(), region(slot, member)), ("px", slot), mp=across)
        send(ok, lambda: (source(), region(slot, member)), ("py", slot), mp=along)
        send(ok, lambda: (source(), region(slot, member)), ("d", "col", slot), seq=partner)

    def stage_b(slot):
        ok = valid(slot)
        for q, owner, half, nxt in (("px", across, 0, along), ("py", along, 1, across)):
            arrived(ok, lambda: region(slot, owner), (q, slot))
            send(
                ok,
                lambda owner=owner, half=half: (region(slot, owner, half), region(slot, owner, half)),
                ("half", half, slot),
                mp=nxt,
            )
            send(
                ok,
                lambda owner=owner: (region(slot, owner), region(slot, owner)),
                ("d", q, slot),
                seq=partner,
            )

    def stage_c(slot):
        ok = valid(slot)
        for half in range(2):
            arrived(ok, lambda: region(slot, far, half), ("half", half, slot))
        send(ok, lambda: (region(slot, far), region(slot, far)), ("d", "far", slot), seq=partner)

    own_copy = pltpu.make_async_copy(own, region(("o", 0), member), local_sem.at[4])
    own_copy.start()
    locals_.append(own_copy)

    def step(stage, d):
        for slot in ((("o", 0),) if d == 0 else (("b", d), ("a", d))):
            stage(slot)

    last = chips - 1
    for t in range(chips + 2):
        if t <= last:
            step(stage_a, t)
            if 1 <= t < last:
                weights_at(t)
        if 0 <= t - 1 <= last:
            step(stage_b, t - 1)
        if 0 <= t - 2 <= last:
            step(stage_c, t - 2)

    ways = [(way, d) for d in range(1, chips) for way in (1, -1)]

    def origin_of(way, d):
        chip = z - way * d
        return chip, (chip >= 0 if way == 1 else chip <= chips - 1)

    for way, d in ways:
        chip, ok = origin_of(way, d)
        arrived(ok, lambda: w_ref.at[rows_of(chip, c), :], ("w", way, d, True))

        def shared(chip=chip):
            place = w_ref.at[rows_of(chip, c), 2 * piece : 2 * piece + pair]
            return place, place

        send(ok, shared, ("wd", way, d), seq=partner)
    for way, d in ways:
        chip, ok = origin_of(way, d)
        arrived(ok, lambda: w_ref.at[rows_of(chip, 1 - c), 0 : 2 * piece], ("w", way, d, False))
        arrived(
            ok,
            lambda: w_ref.at[rows_of(chip, 1 - c), 2 * piece : 2 * piece + pair],
            ("wd", way, d),
        )
        for same in (True, False):
            core = c if same else 1 - c
            arrived(ok, lambda: dt_ref.at[:, rows_of(chip, core)], ("dt", way, d, same))
    arrived(True, lambda: w_ref.at[rows_of(z, 1 - c), :], ("w", 0, 0, False))
    arrived(True, lambda: dt_ref.at[:, rows_of(z, 1 - c)], ("dt", 0, 0, False))
    for d in range(chips):
        for slot in ((("o", 0),) if d == 0 else (("b", d), ("a", d))):
            for q, owner in (("col", member), ("px", across), ("py", along), ("far", far)):
                arrived(valid(slot), lambda: region(slot, owner, None, 1 - c), ("d", q, slot))
    for copy in locals_:
        copy.wait()
    for cond, make in started:
        guarded(cond, lambda: make().wait_send())


def spread(hidden, gain, w_x, w_z, w_bc, w_dt, groups):
    n = lax.axis_size("seq")
    rows, wide = hidden.shape
    depth = w_x.shape[0]
    cols = 2 * (w_x.shape[1] // n) + w_bc.shape[1] // groups
    anywhere = pl.BlockSpec(memory_space=pl.ANY)
    vmem = pl.BlockSpec(memory_space=pltpu.VMEM)
    return pl.pallas_call(
        functools.partial(spread_kernel, n, groups),
        out_shape=(
            jax.ShapeDtypeStruct((n * rows, 4 * wide), BF16),
            jax.ShapeDtypeStruct((n * depth, cols), BF16),
            jax.ShapeDtypeStruct((w_dt.shape[0], n * depth), BF16),
        ),
        in_specs=[vmem, vmem] + [anywhere] * 4,
        out_specs=(anywhere,) * 3,
        scratch_shapes=[
            pltpu.VMEM((rows, wide), BF16),
            pltpu.VMEM((rows, LANES), F32),
            pltpu.VMEM((4, 8, rows), F32),
            pltpu.SemaphoreType.DMA((5,)),
            pltpu.SemaphoreType.DMA((50 * n // 2,)),
            pltpu.SemaphoreType.DMA((30 * n // 2,)),
        ],
        compiler_params=pltpu.CompilerParams(
            collective_id=3, has_side_effects=True, vmem_limit_bytes=24 * 1024 * 1024
        ),
        cost_estimate=pl.CostEstimate(
            flops=20_000_000_000, bytes_accessed=100_000_000, transcendentals=0
        ),
    )(hidden, gain, w_x, w_z, w_bc, w_dt)


def heads_kernel(
    n,
    groups,
    hidden_ref,
    w_ref,
    wdt_ref,
    taps_ref,
    bias_ref,
    rate_ref,
    skip_ref,
    gain_ref,
    wout_ref,
    y_ref,
    rows_ref,
    held_ref,
    blocks,
    wdt_own,
    window,
    gate,
    raws,
    conv,
    state,
    out,
    normed,
    power,
    load_sem,
    local_sem,
    power_send,
    power_recv,
    plane_send,
    plane_recv,
    wout_send,
    wout_recv,
):
    me = lax.axis_index("seq")
    member = lax.axis_index("mp")
    m = lax.axis_size("mp")
    chips = n // 2
    z, c = me // 2, lax.rem(me, 2)
    partner = 2 * z + 1 - c
    per = n // groups
    base = me // per * per
    place = member * 2 + c
    quarter = 2 * gate.shape[1]
    strip = wout_ref.shape[1]
    rows = blocks.shape[1]
    inner = gate.shape[1]
    width = inner + 2 * N
    heads = inner // P_SIZE
    kw = taps_ref.shape[0]

    barrier = pltpu.get_barrier_semaphore()
    for d in range(1, n):
        signal_seq(barrier, lax.rem(me + d, n))
    for d in range(1, m):
        for core in range(2):
            pl.semaphore_signal(
                barrier,
                inc=1,
                device_id={"mp": lax.rem(member + d, m), "seq": 2 * z + core},
                device_id_type=pl.DeviceIdType.MESH,
            )
    pl.semaphore_wait(barrier, n - 1 + 2 * (m - 1))

    def remote(source, target_ref, sends, recvs, **target):
        return pltpu.make_async_remote_copy(
            src_ref=source,
            dst_ref=target_ref,
            send_sem=sends,
            recv_sem=recvs,
            device_id=target,
            device_id_type=pl.DeviceIdType.MESH,
        )

    def landed(target_ref, recvs):
        pltpu.make_async_copy(target_ref, target_ref, recvs).wait()

    def own_rows(chip):
        return wout_ref.at[pl.ds(pl.multiple_of(chip * quarter, quarter), quarter), :]

    def first_leg(d):
        chip = lax.rem(z + d, chips)
        return remote(
            own_rows(chip), held_ref.at[z], wout_send.at[0, d], wout_recv.at[0, d], seq=2 * chip + c
        )

    def second_place(of):
        return rows_ref.at[
            pl.ds(pl.multiple_of(of * quarter, quarter), quarter),
            pl.ds(pl.multiple_of(c * strip, strip), strip),
        ]

    def second_leg(d):
        q = lax.rem(member + d, m)
        return remote(
            held_ref.at[q], second_place(member), wout_send.at[1, d], wout_recv.at[1, d], mp=q
        )

    def third_leg(d):
        of = second_place(lax.rem(member + d, m))
        return remote(of, of, wout_send.at[2, d], wout_recv.at[2, d], seq=partner)

    def keep_held():
        return pltpu.make_async_copy(own_rows(z), held_ref.at[z], local_sem.at[0])

    def keep_rows():
        return pltpu.make_async_copy(held_ref.at[member], second_place(member), local_sem.at[1])

    for d in range(1, chips):
        first_leg(d).start()
    keep_held().start()

    def load(i, slot):
        return pltpu.make_async_copy(
            hidden_ref.at[pl.ds(pl.multiple_of(i * rows, rows), rows), :],
            blocks.at[slot],
            load_sem.at[slot],
        )

    load(0, 0).start()
    all_heads = wdt_ref.shape[0]
    pick_row = lax.broadcasted_iota(jnp.int32, (LANES, all_heads), 0)
    pick_col = lax.broadcasted_iota(jnp.int32, (LANES, all_heads), 1)
    chosen = jnp.logical_and(pick_col == me * heads + pick_row, pick_row < heads)
    wdt_own[...] = jnp.dot(
        jnp.where(chosen, 1.0, 0.0).astype(BF16), wdt_ref[...], preferred_element_type=F32
    ).astype(BF16)

    lane_head = lax.broadcasted_iota(jnp.int32, (LANES, inner), 1) // P_SIZE
    expand = jnp.where(
        lax.broadcasted_iota(jnp.int32, (LANES, inner), 0) == lane_head, 1.0, 0.0
    ).astype(BF16)
    window[0:8, :] = jnp.zeros((8, width), F32)
    state[...] = jnp.zeros_like(state)
    row_id = lax.broadcasted_iota(jnp.int32, (QB, QB), 0)
    col_id = lax.broadcasted_iota(jnp.int32, (QB, QB), 1)
    causal = row_id >= col_id
    low_lanes = col_id < P_SIZE
    tri = jnp.where(causal, 1.0, 0.0).astype(F32)

    def tell(i, k):
        target = base + lax.rem(me - base + k, per)
        return remote(
            power.at[i, 0], power.at[i, k], power_send.at[i, k], power_recv.at[i, k], seq=target
        )

    def spot(i, at):
        return y_ref.at[i // 2, :, pl.ds(pl.multiple_of(at * inner, inner), inner)]

    def to_plane(i, d):
        return remote(
            normed.at[i],
            spot(i, place),
            plane_send.at[i, d],
            plane_recv.at[i // 2, place],
            mp=lax.rem(member + d, m),
            seq=2 * z + lax.rem(i, 2),
        )

    def to_partner(i):
        return remote(
            normed.at[i],
            spot(i, place),
            plane_send.at[i, 0],
            plane_recv.at[i // 2, place],
            seq=partner,
        )

    def to_self(i):
        return pltpu.make_async_copy(normed.at[i], spot(i, place), plane_send.at[i, 0])

    def finish(i):
        for k in range(1, per):
            landed(power.at[i, k], power_recv.at[i, k])
        sums = power[i, 0]
        for k in range(1, per):
            sums = sums + power[i, k]
        column = jnp.transpose(jnp.broadcast_to(sums[0:1, :], (LANES, rows)))
        for sub in range(rows // QB):
            here = slice(sub * QB, (sub + 1) * QB)
            scale = lax.rsqrt(column[here, 0:1] / (per * inner) + 1e-05)
            normed[i, here, :] = (out[i, here, :].astype(F32) * scale * gain_ref[...]).astype(BF16)
        for d in range(1, m):
            to_plane(i, d).start()

        @pl.when(lax.rem(i, 2) == c)
        def _():
            to_self(i).start()

        @pl.when(lax.rem(i, 2) != c)
        def _():
            to_partner(i).start()

    def block(i, carry_none):
        slot = lax.rem(i, 2)

        @pl.when(i + 1 < n)
        def _():
            load(i + 1, 1 - slot).start()

        load(i, slot).wait()
        source = blocks.at[slot]
        window[8 : 8 + rows, 0:inner] = jnp.dot(
            source[...], w_ref[:, 0:inner], preferred_element_type=F32
        )
        gate[...] = jnp.dot(source[...], w_ref[:, inner : 2 * inner], preferred_element_type=F32)
        window[8 : 8 + rows, inner:width] = jnp.dot(
            source[...], w_ref[:, 2 * inner : 2 * inner + 2 * N], preferred_element_type=F32
        )
        raws[...] = lax.dot_general(
            source[...], wdt_own[...], (((1,), (1,)), ((), ())), preferred_element_type=F32
        )

        @pl.when(i > 0)
        def _():
            finish(i - 1)

        for sub in range(rows // QB):
            at = sub * QB
            here = slice(at, at + QB)
            for start in range(0, width, LANES):
                cs = slice(start, start + LANES)
                total = None
                for j in range(kw):
                    first = 8 - kw + 1 + j + at
                    term = taps_ref[j : j + 1, cs] * window[first : first + QB, cs]
                    total = term if total is None else total + term
                conv[sub, :, cs] = silu(total)
            raw = raws[here, :] + bias_ref[...]
            steps = jnp.maximum(raw, 0.0) + jnp.log1p(jnp.exp(-jnp.abs(raw)))
            decays = -rate_ref[...] * steps
            cum = jnp.dot(tri, decays, precision=HIGH, preferred_element_type=F32)
            cum_t = jnp.transpose(cum)
            grown = jnp.exp(cum)
            tail = jnp.exp(cum[QB - 1 : QB, :] - cum)
            x = conv[sub, :, 0:inner]
            b = conv[sub, :, inner : inner + N].astype(BF16)
            c = conv[sub, :, inner + N : width].astype(BF16)
            scaled = x * spread_heads(steps, expand)
            grown_e = spread_heads(grown, expand)
            tailed = (scaled * spread_heads(tail, expand)).astype(BF16)
            scaled_low = scaled.astype(BF16)
            held = state[...]
            carried = grown_e * jnp.dot(c, held.astype(BF16), preferred_element_type=F32)
            fresh = lax.dot_general(b, tailed, (((0,), (0,)), ((), ())), preferred_element_type=F32)
            state[...] = grown_e[QB - 1 : QB, :] * held + fresh
            affinity = lax.dot_general(c, b, (((1,), (1,)), ((), ())), preferred_element_type=F32)
            affinity = jnp.where(causal, affinity, 0.0)
            full = carried + skip_ref[...] * x
            squares = None
            for pair in range(inner // LANES):
                lanes = slice(pair * LANES, (pair + 1) * LANES)
                outs = []
                for k in range(2):
                    h = pair * 2 + k
                    spread_h = jnp.minimum(cum[:, h : h + 1] - cum_t[h : h + 1, :], 0.0)
                    mixing = (affinity * jnp.exp(spread_h)).astype(BF16)
                    outs.append(
                        jnp.dot(mixing, scaled_low[:, lanes], preferred_element_type=F32)
                    )
                inside = jnp.where(low_lanes, outs[0], outs[1])
                gated = (full[:, lanes] + inside) * silu(gate[here, lanes])
                out[i, here, lanes] = gated.astype(BF16)
                squares = gated * gated if squares is None else squares + gated * gated
            totals = jnp.broadcast_to(jnp.sum(squares, axis=-1, keepdims=True), (QB, LANES))
            power[i, 0, :, here] = jnp.transpose(totals)[0:8, :]
        window[0:8, :] = window[rows : rows + 8, :]

        for k in range(1, per):
            tell(i, k).start()

        @pl.when(i == n // 2)
        def _():
            keep_held().wait()
            for d in range(1, chips):
                landed(held_ref.at[lax.rem(z + d, chips)], wout_recv.at[0, chips - d])
            keep_rows().start()
            for d in range(1, m):
                second_leg(d).start()

        @pl.when(i == n - 2)
        def _():
            keep_rows().wait()
            third_leg(0).start()
            for d in range(1, m):
                landed(second_place(lax.rem(member + d, m)), wout_recv.at[1, m - d])
                third_leg(d).start()

        return carry_none

    lax.fori_loop(0, n, block, 0)
    finish(n - 1)
    for d in range(m):
        strips = pl.ds(pl.multiple_of((1 - c) * strip, strip), strip)
        of = lax.rem(member + d, m)
        landed(
            rows_ref.at[pl.ds(pl.multiple_of(of * quarter, quarter), quarter), strips],
            wout_recv.at[2, d],
        )
    for j in range(chips):
        for at in range(2 * m):

            @pl.when(at != place)
            def _():
                landed(y_ref.at[j, :, at * inner : (at + 1) * inner], plane_recv.at[j, at])

    def flush(i, carry_none):
        for k in range(1, per):
            tell(i, k).wait_send()
        for d in range(1, m):
            to_plane(i, d).wait_send()

        @pl.when(lax.rem(i, 2) == c)
        def _():
            to_self(i).wait()

        @pl.when(lax.rem(i, 2) != c)
        def _():
            to_partner(i).wait_send()

        return carry_none

    lax.fori_loop(0, n, flush, 0)
    for d in range(1, chips):
        first_leg(d).wait_send()
    for d in range(1, m):
        second_leg(d).wait_send()
    for d in range(m):
        third_leg(d).wait_send()


def mix_heads(hidden, w_out, weights, w_dt, taps, bias, rate, skip, gain, groups):
    n, m = lax.axis_size("seq"), lax.axis_size("mp")
    rows = hidden.shape[0] // n
    features = hidden.shape[1]
    inner = skip.shape[1]
    width = inner + 2 * N
    quarter, strip = 2 * inner, w_out.shape[1]
    per = n // groups
    vmem = pl.BlockSpec(memory_space=pltpu.VMEM)
    anywhere = pl.BlockSpec(memory_space=pl.ANY)
    return pl.pallas_call(
        functools.partial(heads_kernel, n, groups),
        out_shape=(
            jax.ShapeDtypeStruct((n // 2, rows, 2 * m * inner), BF16),
            jax.ShapeDtypeStruct((m * quarter, 2 * strip), BF16),
            jax.ShapeDtypeStruct((n // 2, quarter, strip), BF16),
        ),
        in_specs=[anywhere] + [vmem] * 7 + [anywhere],
        out_specs=(anywhere,) * 3,
        scratch_shapes=[
            pltpu.VMEM((2, rows, features), BF16),
            pltpu.VMEM((LANES, features), BF16),
            pltpu.VMEM((8 + rows, width), F32),
            pltpu.VMEM((rows, inner), F32),
            pltpu.VMEM((rows, LANES), F32),
            pltpu.VMEM((rows // QB, QB, width), F32),
            pltpu.VMEM((N, inner), F32),
            pltpu.VMEM((n, rows, inner), BF16),
            pltpu.VMEM((n, rows, inner), BF16),
            pltpu.VMEM((n, per, 8, rows), F32),
            pltpu.SemaphoreType.DMA((2,)),
            pltpu.SemaphoreType.DMA((2,)),
            pltpu.SemaphoreType.DMA((n, per)),
            pltpu.SemaphoreType.DMA((n, per)),
            pltpu.SemaphoreType.DMA((n, m)),
            pltpu.SemaphoreType.DMA((n // 2, 2 * m)),
            pltpu.SemaphoreType.DMA((3, m)),
            pltpu.SemaphoreType.DMA((3, m)),
        ],
        compiler_params=pltpu.CompilerParams(
            collective_id=4, has_side_effects=True, vmem_limit_bytes=48 * 1024 * 1024
        ),
        cost_estimate=pl.CostEstimate(
            flops=40_000_000_000, bytes_accessed=50_000_000, transcendentals=8_000_000
        ),
    )(hidden, weights, w_dt, taps, bias, rate, skip, gain, w_out)


def combine_kernel(
    n,
    y_ref,
    w_ref,
    hidden_ref,
    gain_ref,
    mixed_ref,
    normed_ref,
    part,
    outgoing,
    incoming,
    low,
    send_sem,
    recv_sem,
    own_sem,
    mp_send,
    mp_recv,
):
    me = lax.axis_index("seq")
    member = lax.axis_index("mp")
    chips = n // 2
    z = me // 2
    across = member + 1 - 2 * lax.rem(member, 2)
    along = lax.rem(member + 2, 4)
    far = 3 - member
    rows, wide = hidden_ref.shape
    tile = part.shape[1]
    tiles = wide // tile
    has_up, has_down = z + 1 <= chips - 1, z >= 1

    barrier = pltpu.get_barrier_semaphore()
    signal_mp(barrier, across)
    signal_mp(barrier, along)

    @pl.when(has_up)
    def _():
        signal_seq(barrier, me + 2)

    @pl.when(has_down)
    def _():
        signal_seq(barrier, me - 2)

    ends = jnp.logical_and(has_up, has_down)

    @pl.when(ends)
    def _():
        pl.semaphore_wait(barrier, 4)

    @pl.when(jnp.logical_not(ends))
    def _():
        pl.semaphore_wait(barrier, 3)

    def hand_on(j, t, way):
        here = slice(t * tile, (t + 1) * tile)
        return pltpu.make_async_remote_copy(
            src_ref=outgoing.at[j, :, here],
            dst_ref=incoming.at[way, j, :, here],
            send_sem=send_sem.at[j, t],
            recv_sem=recv_sem.at[way, j, t],
            device_id={"seq": me + 2 if way == 0 else me - 2},
            device_id_type=pl.DeviceIdType.MESH,
        )

    def take(j, t, way):
        here = slice(t * tile, (t + 1) * tile)
        where = incoming.at[way, j, :, here]
        pltpu.make_async_copy(where, where, recv_sem.at[way, j, t]).wait()
        return incoming[way, j, :, here].astype(F32)

    order = []
    for k in range((chips + 1) // 2):
        order += [chips - 1 - k] + ([k] if k != chips - 1 - k else [])
    for j in order:
        for t in range(tiles):
            here = slice(t * tile, (t + 1) * tile)

            @pl.when(z != j)
            def _():
                part[...] = jnp.dot(y_ref[j], w_ref[:, here], preferred_element_type=F32)

            @pl.when(jnp.logical_and(z < j, z >= 1))
            def _():
                part[...] += take(j, t, 0)

            @pl.when(jnp.logical_and(z > j, z <= chips - 2))
            def _():
                part[...] += take(j, t, 1)

            @pl.when(z != j)
            def _():
                outgoing[j, :, here] = part[...].astype(BF16)

            @pl.when(z < j)
            def _():
                hand_on(j, t, 0).start()

            @pl.when(z > j)
            def _():
                hand_on(j, t, 1).start()

    for t in range(tiles):
        here = slice(t * tile, (t + 1) * tile)
        mixed_ref[:, here] = hidden_ref[:, here].astype(F32) + jnp.dot(
            y_ref[z], w_ref[:, here], preferred_element_type=F32
        )
    for t in range(tiles):
        here = slice(t * tile, (t + 1) * tile)

        @pl.when(has_down)
        def _():
            mixed_ref[:, here] += take(z, t, 0)

        @pl.when(has_up)
        def _():
            mixed_ref[:, here] += take(z, t, 1)

        low[:, here] = mixed_ref[:, here].astype(BF16)

    def feature(owner, half=None):
        at = pl.ds(pl.multiple_of(owner * wide, wide), wide)
        if half is None:
            return normed_ref.at[:, at]
        return normed_ref.at[half * (rows // 2) : (half + 1) * (rows // 2), at]

    def share(index, source, place, target):
        return pltpu.make_async_remote_copy(
            src_ref=source,
            dst_ref=place,
            send_sem=mp_send.at[index],
            recv_sem=mp_recv.at[index],
            device_id={"mp": target},
            device_id_type=pl.DeviceIdType.MESH,
        )

    def arrived(index, place):
        pltpu.make_async_copy(place, place, mp_recv.at[index]).wait()

    shared = [
        share(0, low, feature(member), across),
        share(1, low, feature(member), along),
        share(2, feature(across, 0), feature(across, 0), along),
        share(3, feature(along, 1), feature(along, 1), across),
    ]
    shared[0].start()
    shared[1].start()
    own_copy = pltpu.make_async_copy(low, feature(member), own_sem)
    own_copy.start()
    arrived(0, feature(across))
    shared[2].start()
    arrived(1, feature(along))
    shared[3].start()
    arrived(2, feature(far, 0))
    arrived(3, feature(far, 1))
    own_copy.wait()
    for copy in shared:
        copy.wait_send()
    norm_rows(normed_ref, gain_ref, normed_ref)
    for j in range(chips):
        for t in range(tiles):

            @pl.when(z < j)
            def _():
                hand_on(j, t, 0).wait_send()

            @pl.when(z > j)
            def _():
                hand_on(j, t, 1).wait_send()


def combine(y, weights, hidden, gain):
    n = lax.axis_size("seq")
    rows, wide = hidden.shape
    chips = n // 2
    tile = min(256, wide)
    vmem = pl.BlockSpec(memory_space=pltpu.VMEM)
    return pl.pallas_call(
        functools.partial(combine_kernel, n),
        out_shape=(
            jax.ShapeDtypeStruct((rows, wide), F32),
            jax.ShapeDtypeStruct((rows, 4 * wide), BF16),
        ),
        in_specs=[vmem] * 4,
        out_specs=(vmem, vmem),
        scratch_shapes=[
            pltpu.VMEM((rows, tile), F32),
            pltpu.VMEM((chips, rows, wide), BF16),
            pltpu.VMEM((2, chips, rows, wide), BF16),
            pltpu.VMEM((rows, wide), BF16),
            pltpu.SemaphoreType.DMA((chips, wide // tile)),
            pltpu.SemaphoreType.DMA((2, chips, wide // tile)),
            pltpu.SemaphoreType.DMA,
            pltpu.SemaphoreType.DMA((4,)),
            pltpu.SemaphoreType.DMA((4,)),
        ],
        compiler_params=pltpu.CompilerParams(
            collective_id=6, has_side_effects=True, vmem_limit_bytes=56 * 1024 * 1024
        ),
        cost_estimate=pl.CostEstimate(
            flops=2 * chips * rows * y.shape[2] * wide,
            bytes_accessed=60_000_000,
            transcendentals=0,
        ),
    )(y, weights, hidden, gain)


def own_slice(values, index, size):
    return lax.dynamic_slice_in_dim(values, index * size, size, values.ndim - 1)


def mixer_by_heads(
    hidden_in, norm_gain, w_z, w_x, w_b, w_c, w_dt, conv_x, conv_b, conv_c, dt_bias, a_rate,
    skip_gain, group_gain,
):
    n = lax.axis_size("seq")
    me = lax.axis_index("seq")
    groups = conv_b.shape[1] // N
    inner = conv_x.shape[1] // n
    heads = dt_bias.shape[0] // n
    group = me * groups // n
    pieces = []
    for g in range(groups):
        pieces += [w_b[:, g * N : (g + 1) * N], w_c[:, g * N : (g + 1) * N]]
    gain = own_slice(norm_gain[None, :], lax.axis_index("mp"), hidden_in.shape[1])
    hidden, weights, steps = spread(
        hidden_in, gain, w_x, w_z, jnp.concatenate(pieces, axis=1), jnp.transpose(w_dt), groups
    )
    taps = jnp.concatenate(
        [own_slice(conv_x, me, inner), own_slice(conv_b, group, N), own_slice(conv_c, group, N)],
        axis=1,
    )
    return hidden, functools.partial(
        mix_heads,
        weights=weights,
        w_dt=steps,
        taps=taps,
        bias=pad_lanes(own_slice(dt_bias[None, :], me, heads)),
        rate=pad_lanes(own_slice(a_rate[None, :], me, heads)),
        skip=jnp.repeat(own_slice(skip_gain[None, :], me, heads), P_SIZE, axis=1),
        gain=own_slice(group_gain[None, :], me, inner),
        groups=groups,
    )


def splits_by_heads(conv_x, conv_b):
    n, m = lax.axis_size("seq"), lax.axis_size("mp")
    groups = conv_b.shape[1] // N
    whole = conv_x.shape[1] % (n * LANES) == 0 and n % groups == 0
    return m == 4 and n == 2 * m and whole


def on_device(
    hidden_in,
    norm_gain,
    w_z,
    w_x,
    w_b,
    w_c,
    w_dt,
    conv_x,
    conv_b,
    conv_c,
    dt_bias,
    a_rate,
    skip_gain,
    group_gain,
    w_out,
    attn_gain,
    w_q,
    w_k,
    w_v,
):
    if splits_by_heads(conv_x, conv_b):
        hidden, mix = mixer_by_heads(
            hidden_in, norm_gain, w_z, w_x, w_b, w_c, w_dt, conv_x, conv_b, conv_c, dt_bias,
            a_rate, skip_gain, group_gain,
        )
        y_normed, out_rows, _ = mix(hidden, w_out)
        mixed, normed_two = combine(y_normed, out_rows, hidden_in, attn_gain[None, :])
    else:
        proj = gather_dot(
            hidden_in,
            norm_gain[None, :],
            jnp.concatenate([w_x, w_b, w_c, pad_lanes(w_dt), w_z], axis=1),
        )
        proj, w_out = lax.optimization_barrier((proj, w_out))
        out_columns = lax.all_gather(w_out, "seq", axis=1, tiled=True)
        heads = dt_bias.shape[0]
        groups = conv_b.shape[1] // N
        width = conv_x.shape[1] + conv_b.shape[1] + conv_c.shape[1]
        rim = from_behind(proj[proj.shape[0] - 8 :, :width], "seq", 1)
        y_normed = mixer(
            proj,
            rim,
            jnp.concatenate([conv_x, conv_b, conv_c], axis=1),
            pad_lanes(dt_bias[None, :]),
            pad_lanes(a_rate[None, :]),
            jnp.repeat(skip_gain, P_SIZE)[None, :],
            group_gain[None, :],
            heads,
            groups,
        )
        mixed, normed_two = output_stage(
            y_normed, out_columns, hidden_in, attn_gain[None, :]
        )
    n = lax.axis_size("seq")
    if n % 2 == 0 and n >= 4 and WINDOW >= n * hidden_in.shape[0]:
        context = line_attention(normed_two, w_q, w_k, w_v)
    else:
        own_keys = jnp.dot(normed_two, w_k, preferred_element_type=F32).astype(BF16)
        own_values = jnp.dot(normed_two, w_v, preferred_element_type=F32).astype(BF16)
        pairs = lax.all_gather(
            jnp.concatenate([own_keys, own_values], axis=1), "seq", axis=0, tiled=True
        )
        queries = jnp.dot(normed_two, w_q, preferred_element_type=F32).astype(BF16)
        context = attention(queries, pairs, own_keys.shape[1] // HD)
    return (mixed, context)


def solution(mesh):
    placed = (
        P("seq", "mp"),
        P(),
        P("seq", "mp"),
        P("seq", "mp"),
        P("seq", "mp"),
        P("seq", "mp"),
        P("seq", "mp"),
        P(None, "mp"),
        P(None, "mp"),
        P(None, "mp"),
        P("mp"),
        P("mp"),
        P("mp"),
        P("mp"),
        P("mp", "seq"),
        P(),
        P(None, "mp"),
        P(None, "mp"),
        P(None, "mp"),
    )
    return jax.shard_map(
        on_device,
        mesh=mesh,
        in_specs=placed,
        out_specs=(P("seq", "mp"), P("seq", "mp")),
        check_vma=False,
    )
```

```python
import functools
import math

import jax
import jax.numpy as jnp
from jax import lax
from jax.experimental import pallas as pl
from jax.experimental.pallas import tpu as pltpu
from jax.sharding import PartitionSpec as P

P_SIZE = 64
N = 128
HD = 128
WINDOW = 4096
QB = 128
LANES = 128
VMEM_LIMIT = 62 * 1024 * 1024

HIGH = lax.Precision.HIGHEST
F32 = jnp.float32
BF16 = jnp.bfloat16


def from_behind(block, axis, distance):
    devices = range(lax.axis_size(axis))
    route = [(i - distance, i) for i in devices if i - distance in devices]
    return lax.ppermute(block, axis, route)


def rms_norm(values, gain):
    return values * lax.rsqrt(jnp.mean(values * values, axis=-1, keepdims=True) + 1e-05) * gain


def signal_seq(sem, index):
    pl.semaphore_signal(
        sem, inc=1, device_id={"seq": index}, device_id_type=pl.DeviceIdType.MESH
    )


def signal_mp(sem, index):
    pl.semaphore_signal(
        sem, inc=1, device_id={"mp": index}, device_id_type=pl.DeviceIdType.MESH
    )


def norm_rows(source, gain_ref, target):
    rows = source.shape[0]
    tile = min(64, rows)

    def body(i, carry_none):
        here = pl.ds(pl.multiple_of(i * tile, tile), tile)
        target[here, :] = rms_norm(source[here, :].astype(F32), gain_ref[...]).astype(BF16)
        return carry_none

    lax.fori_loop(0, rows // tile, body, 0)


def share_features(m, source, whole, send_sem, recv_sem):
    member = lax.axis_index("mp")
    wide = source.shape[1]
    own = pl.ds(pl.multiple_of(member * wide, wide), wide)
    copies = [
        pltpu.make_async_remote_copy(
            src_ref=source,
            dst_ref=whole.at[:, own],
            send_sem=send_sem.at[d - 1],
            recv_sem=recv_sem.at[d - 1],
            device_id={"mp": lax.rem(member + d, m)},
            device_id_type=pl.DeviceIdType.MESH,
        )
        for d in range(1, m)
    ]
    for copy in copies:
        copy.start()
    return copies, own


def features_arrived(m, whole, wide, recv_sem):
    member = lax.axis_index("mp")
    for d in range(1, m):
        sender = lax.rem(member - d + m, m)
        there = whole.at[:, pl.ds(pl.multiple_of(sender * wide, wide), wide)]
        pltpu.make_async_copy(there, there, recv_sem.at[d - 1]).wait()


def gather_dot_kernel(
    n,
    m,
    hidden_ref,
    gain_ref,
    w_ref,
    out_ref,
    slots,
    normed_ref,
    local_sem,
    send_sem,
    recv_sem,
    own_sem,
    mp_send_sem,
    mp_recv_sem,
):
    me = lax.axis_index("seq")
    member = lax.axis_index("mp")
    ring = n // 2
    half = ring // 2
    chip, core = me // 2, lax.rem(me, 2)
    up = lax.rem(chip + 1, ring) * 2 + core
    down = lax.rem(chip + ring - 1, ring) * 2 + core
    partner = chip * 2 + 1 - core
    depth, cols = w_ref.shape
    mid = depth // 2

    barrier = pltpu.get_barrier_semaphore()
    for other in (up, down, partner):
        signal_seq(barrier, other)
    for d in range(1, m):
        signal_mp(barrier, lax.rem(member + d, m))
    pl.semaphore_wait(barrier, 3 + m - 1)

    shared, own = share_features(m, hidden_ref, normed_ref, mp_send_sem, mp_recv_sem)
    own_copy = pltpu.make_async_copy(hidden_ref, normed_ref.at[:, own], own_sem)
    own_copy.start()
    local = pltpu.make_async_copy(w_ref, slots.at[0], local_sem)
    local.start()
    started = []

    def send(source, slot, rows, part, target):
        copy = pltpu.make_async_remote_copy(
            src_ref=source,
            dst_ref=slots.at[slot, rows],
            send_sem=send_sem.at[len(started)],
            recv_sem=recv_sem.at[2 * slot + part],
            device_id={"seq": target},
            device_id_type=pl.DeviceIdType.MESH,
        )
        copy.start()
        started.append(copy)

    def arrived(slot, rows, part):
        pltpu.make_async_copy(
            slots.at[slot, rows], slots.at[slot, rows], recv_sem.at[2 * slot + part]
        ).wait()

    whole, upper, lower = pl.ds(0, depth), pl.ds(0, mid), pl.ds(mid, mid)
    send(w_ref, 2 * 1, whole, 0, up)
    send(w_ref, 2 * (ring - 1), whole, 0, down)
    send(w_ref, 1, whole, 0, partner)

    def multiply(slot, first=False):
        step, lane = slot // 2, slot % 2
        origin = lax.rem(chip - step + ring, ring) * 2
        owner = origin + (core if lane == 0 else 1 - core)
        features = pl.ds(pl.multiple_of(owner * depth, depth), depth)

        def tile(start, width):
            where = pl.ds(start, width)
            product = jnp.dot(
                normed_ref[:, features], slots[slot, :, where], preferred_element_type=F32
            )
            if first:
                out_ref[:, where] = product
            else:
                out_ref[:, where] += product

        width = 512
        full = cols // width

        def body(i, carry):
            tile(pl.multiple_of(i * width, width), width)
            return carry

        lax.fori_loop(0, full, body, 0)
        if cols % width:
            tile(full * width, cols % width)

    own_copy.wait()
    features_arrived(m, normed_ref, hidden_ref.shape[1], mp_recv_sem)
    norm_rows(normed_ref, gain_ref, normed_ref)
    local.wait()
    multiply(0, True)
    arrived(1, whole, 0)
    multiply(1)
    for d in range(1, half):
        s_up, s_down = 2 * d, 2 * (ring - d)
        last = d + 1 == half
        arrived(s_up, whole, 0)
        rows = upper if last else whole
        send(slots.at[s_up, rows], 2 * (d + 1), rows, 0, up)
        arrived(s_down, whole, 0)
        rows = lower if last else whole
        send(slots.at[s_down, rows], 2 * (ring - d - 1), rows, 1 if last else 0, down)
        send(slots.at[s_up, whole], s_up + 1, whole, 0, partner)
        send(slots.at[s_down, whole], s_down + 1, whole, 0, partner)
        multiply(s_up)
        multiply(s_down)
        arrived(s_up + 1, whole, 0)
        multiply(s_up + 1)
        arrived(s_down + 1, whole, 0)
        multiply(s_down + 1)
    far = 2 * half
    arrived(far, upper, 0)
    send(slots.at[far, upper], far + 1, upper, 0, partner)
    arrived(far, lower, 1)
    send(slots.at[far, lower], far + 1, lower, 1, partner)
    multiply(far)
    arrived(far + 1, upper, 0)
    arrived(far + 1, lower, 1)
    multiply(far + 1)
    for copy in started + shared:
        copy.wait_send()


def gather_dot(hidden, gain, weights):
    n, m = lax.axis_size("seq"), lax.axis_size("mp")
    depth, cols = weights.shape
    rows, features = hidden.shape[0], hidden.shape[1] * m
    ring = n // 2
    sends = 3 + 4 * (ring // 2 - 1) + 2
    return pl.pallas_call(
        functools.partial(gather_dot_kernel, n, m),
        out_shape=jax.ShapeDtypeStruct((rows, cols), F32),
        in_specs=[
            pl.BlockSpec(memory_space=pl.ANY),
            pl.BlockSpec(memory_space=pltpu.VMEM),
            pl.BlockSpec(memory_space=pl.ANY),
        ],
        out_specs=pl.BlockSpec(memory_space=pltpu.VMEM),
        scratch_shapes=[
            pltpu.VMEM((n, depth, cols), BF16),
            pltpu.VMEM((rows, features), BF16),
            pltpu.SemaphoreType.DMA,
            pltpu.SemaphoreType.DMA((sends,)),
            pltpu.SemaphoreType.DMA((2 * n,)),
            pltpu.SemaphoreType.DMA,
            pltpu.SemaphoreType.DMA((m - 1,)),
            pltpu.SemaphoreType.DMA((m - 1,)),
        ],
        compiler_params=pltpu.CompilerParams(
            collective_id=0, has_side_effects=True, vmem_limit_bytes=VMEM_LIMIT
        ),
        cost_estimate=pl.CostEstimate(
            flops=2 * rows * features * cols,
            bytes_accessed=160_000_000,
            transcendentals=0,
        ),
    )(hidden, gain, weights)


def silu(v):
    return v / (1.0 + jnp.exp(-v))


def spread_heads(values, expand):
    high = values.astype(BF16)
    low = (values - high.astype(F32)).astype(BF16)
    return jnp.dot(high, expand, preferred_element_type=F32) + jnp.dot(
        low, expand, preferred_element_type=F32
    )


def mixer_kernel(
    n,
    heads,
    groups,
    proj_ref,
    rim_ref,
    taps_ref,
    bias_ref,
    rate_ref,
    skip_ref,
    gain_ref,
    expand_ref,
    y_ref,
    window,
    conv,
    ssd,
    reads,
    logs,
    state,
    carry,
    state_out,
    state_in,
    send_sem,
    recv_sem,
):
    me = lax.axis_index("seq")
    rows = proj_ref.shape[0]
    inner = heads * P_SIZE
    width = inner + 2 * groups * N
    gate_at = width + LANES
    per_group = inner // groups
    blocks = rows // QB
    kw = taps_ref.shape[0]

    barrier = pltpu.get_barrier_semaphore()
    signal_seq(barrier, lax.rem(me + 1, n))
    signal_seq(barrier, lax.rem(me + n - 1, n))
    pl.semaphore_wait(barrier, 2)

    expand = expand_ref[...]
    window[0:8, :] = rim_ref[...]
    state[...] = jnp.zeros_like(state)
    carry[...] = jnp.zeros_like(carry)
    row_id = lax.broadcasted_iota(jnp.int32, (QB, QB), 0)
    col_id = lax.broadcasted_iota(jnp.int32, (QB, QB), 1)
    causal = row_id >= col_id
    low_lanes = col_id < P_SIZE
    tri = jnp.where(causal, 1.0, 0.0).astype(F32)

    def block(i, carry_none):
        base = pl.multiple_of(i * QB, QB)
        here = pl.ds(base, QB)
        window[8 : 8 + QB, :] = proj_ref[here, 0:width]
        step_cols = 256 if width % 256 == 0 else 128
        for at in range(0, width, step_cols):
            cs = slice(at, at + step_cols)
            total = None
            for j in range(kw):
                term = taps_ref[j : j + 1, cs] * window[8 - kw + 1 + j : 8 - kw + 1 + j + QB, cs]
                total = term if total is None else total + term
            conv[:, cs] = silu(total)
        window[0:8, :] = window[QB : QB + 8, :]

        raw = proj_ref[here, width : width + LANES] + bias_ref[...]
        steps = jnp.maximum(raw, 0.0) + jnp.log1p(jnp.exp(-jnp.abs(raw)))
        decays = -rate_ref[...] * steps
        cum = jnp.dot(tri, decays, precision=HIGH, preferred_element_type=F32)
        cum_t = jnp.transpose(cum)
        logs[here, :] = cum + carry[0:1, :]
        carry[...] = carry[...] + cum[QB - 1 : QB, :]
        grown = jnp.exp(cum)
        tail = jnp.exp(cum[QB - 1 : QB, :] - cum)

        for g in range(groups):
            lanes = slice(g * per_group, (g + 1) * per_group)
            expand_g = expand[:, lanes]
            x = conv[:, lanes]
            b = conv[:, inner + g * N : inner + (g + 1) * N].astype(BF16)
            c = conv[:, inner + (groups + g) * N : inner + (groups + g + 1) * N].astype(BF16)
            reads[here, g * N : (g + 1) * N] = c
            scaled = x * spread_heads(steps, expand_g)
            grown_e = spread_heads(grown, expand_g)
            tailed = (scaled * spread_heads(tail, expand_g)).astype(BF16)
            scaled_low = scaled.astype(BF16)
            held = state[:, lanes]
            carried = grown_e * jnp.dot(c, held.astype(BF16), preferred_element_type=F32)
            ssd[here, lanes] = carried + skip_ref[:, lanes] * x
            fresh = lax.dot_general(
                b, tailed, (((0,), (0,)), ((), ())), preferred_element_type=F32
            )
            state[:, lanes] = grown_e[QB - 1 : QB, :] * held + fresh
            affinity = lax.dot_general(
                c, b, (((1,), (1,)), ((), ())), preferred_element_type=F32
            )
            affinity = jnp.where(causal, affinity, 0.0)
            for pair in range(per_group // LANES):
                at = pair * LANES
                inputs = scaled_low[:, at : at + LANES]
                outs = []
                for k in range(2):
                    h = (g * per_group + at) // P_SIZE + k
                    spread = jnp.minimum(cum[:, h : h + 1] - cum_t[h : h + 1, :], 0.0)
                    mixing = (affinity * jnp.exp(spread)).astype(BF16)
                    outs.append(jnp.dot(mixing, inputs, preferred_element_type=F32))
                where = slice(g * per_group + at, g * per_group + at + LANES)
                ssd[here, where] += jnp.where(low_lanes, outs[0], outs[1])
        return carry_none

    lax.fori_loop(0, blocks, block, 0)

    parts = 4
    piece = inner // parts
    decay = jnp.exp(carry[...])

    def hand_on(k):
        lanes = slice(k * piece, (k + 1) * piece)
        return pltpu.make_async_remote_copy(
            src_ref=state_out.at[:, lanes],
            dst_ref=state_in.at[:, lanes],
            send_sem=send_sem.at[k],
            recv_sem=recv_sem.at[k],
            device_id={"seq": jnp.minimum(me + 1, n - 1)},
            device_id_type=pl.DeviceIdType.MESH,
        )

    for k in range(parts):
        lanes = slice(k * piece, (k + 1) * piece)
        weight = spread_heads(decay, expand[:, lanes])[0:1, :]

        @pl.when(me > 0)
        def _():
            hand_on(k).wait_recv()
            before = state_in[:, lanes].astype(F32)
            state_out[:, lanes] = (weight * before + state[:, lanes]).astype(BF16)

        @pl.when(me == 0)
        def _():
            state_out[:, lanes] = state[:, lanes].astype(BF16)
            state_in[:, lanes] = jnp.zeros((N, piece), BF16)

        @pl.when(me < n - 1)
        def _():
            hand_on(k).start()

    def finish(i, carry_none):
        here = pl.ds(pl.multiple_of(i * QB, QB), QB)
        grown = jnp.exp(logs[here, :])
        for g in range(groups):
            lanes = slice(g * per_group, (g + 1) * per_group)
            late = jnp.dot(
                reads[here, g * N : (g + 1) * N],
                state_in[:, lanes],
                preferred_element_type=F32,
            )
            full = ssd[here, lanes] + spread_heads(grown, expand[:, lanes]) * late
            gate = proj_ref[here, gate_at + g * per_group : gate_at + (g + 1) * per_group]
            gated = full * silu(gate)
            power = jnp.mean(gated * gated, axis=-1, keepdims=True)
            y_ref[here, lanes] = (gated * lax.rsqrt(power + 1e-05) * gain_ref[:, lanes]).astype(BF16)
        return carry_none

    lax.fori_loop(0, blocks, finish, 0)

    @pl.when(me < n - 1)
    def _():
        for k in range(parts):
            hand_on(k).wait_send()


def mixer(proj, rim, taps, bias, rate, skip, gain, heads, groups):
    n = lax.axis_size("seq")
    rows = proj.shape[0]
    inner = heads * P_SIZE
    width = inner + 2 * groups * N
    expand = (
        jnp.arange(LANES)[:, None] == (jnp.arange(inner) // P_SIZE)[None, :]
    ).astype(BF16)
    vmem = pl.BlockSpec(memory_space=pltpu.VMEM)
    return pl.pallas_call(
        functools.partial(mixer_kernel, n, heads, groups),
        out_shape=jax.ShapeDtypeStruct((rows, inner), BF16),
        in_specs=[vmem] * 8,
        out_specs=vmem,
        scratch_shapes=[
            pltpu.VMEM((8 + QB, width), F32),
            pltpu.VMEM((QB, width), F32),
            pltpu.VMEM((rows, inner), F32),
            pltpu.VMEM((rows, groups * N), BF16),
            pltpu.VMEM((rows, LANES), F32),
            pltpu.VMEM((N, inner), F32),
            pltpu.VMEM((8, LANES), F32),
            pltpu.VMEM((N, inner), BF16),
            pltpu.VMEM((N, inner), BF16),
            pltpu.SemaphoreType.DMA((4,)),
            pltpu.SemaphoreType.DMA((4,)),
        ],
        compiler_params=pltpu.CompilerParams(
            collective_id=1, has_side_effects=True, vmem_limit_bytes=48 * 1024 * 1024
        ),
        cost_estimate=pl.CostEstimate(
            flops=8_000_000_000, bytes_accessed=100_000_000, transcendentals=8_000_000
        ),
    )(proj, rim, taps, bias, rate, skip, gain, expand)


def output_kernel(
    m,
    y_ref,
    w_ref,
    hidden_ref,
    gain_ref,
    mixed_ref,
    normed_ref,
    outgoing,
    incoming,
    low,
    part_send,
    part_recv,
    own_sem,
    mp_send,
    mp_recv,
):
    member = lax.axis_index("mp")
    wide = hidden_ref.shape[1]
    barrier = pltpu.get_barrier_semaphore()
    for d in range(1, m):
        signal_mp(barrier, lax.rem(member + d, m))
    pl.semaphore_wait(barrier, m - 1)
    tile = min(512, wide)

    def part(target, store):
        for at in range(0, wide, tile):
            where = pl.ds(pl.multiple_of(target * wide + at, tile), tile)
            term = jnp.dot(y_ref[...], w_ref[:, where], preferred_element_type=F32)
            store(slice(at, at + tile), term.astype(BF16))

    copies = []
    for d in range(1, m):
        target = lax.rem(member + d, m)

        def keep(where, term):
            outgoing[d - 1, :, where] = term

        part(target, keep)
        copy = pltpu.make_async_remote_copy(
            src_ref=outgoing.at[d - 1],
            dst_ref=incoming.at[d - 1],
            send_sem=part_send.at[d - 1],
            recv_sem=part_recv.at[d - 1],
            device_id={"mp": target},
            device_id_type=pl.DeviceIdType.MESH,
        )
        copy.start()
        copies.append(copy)

    def begin(where, term):
        mixed_ref[:, where] = hidden_ref[:, where].astype(F32) + term.astype(F32)

    part(member, begin)
    for d in range(1, m):
        copies[d - 1].wait_recv()
        if d < m - 1:
            mixed_ref[...] += incoming[d - 1].astype(F32)
        else:
            total = mixed_ref[...] + incoming[d - 1].astype(F32)
            mixed_ref[...] = total
            low[...] = total.astype(BF16)
    shared, own = share_features(m, low, normed_ref, mp_send, mp_recv)
    own_copy = pltpu.make_async_copy(low, normed_ref.at[:, own], own_sem)
    own_copy.start()
    own_copy.wait()
    features_arrived(m, normed_ref, wide, mp_recv)
    norm_rows(normed_ref, gain_ref, normed_ref)
    for copy in copies + shared:
        copy.wait_send()


def output_stage(y, weights, hidden, gain):
    m = lax.axis_size("mp")
    rows, wide = hidden.shape
    vmem = pl.BlockSpec(memory_space=pltpu.VMEM)
    return pl.pallas_call(
        functools.partial(output_kernel, m),
        out_shape=(
            jax.ShapeDtypeStruct((rows, wide), F32),
            jax.ShapeDtypeStruct((rows, wide * m), BF16),
        ),
        in_specs=[vmem] * 4,
        out_specs=(vmem, vmem),
        scratch_shapes=[
            pltpu.VMEM((m - 1, rows, wide), BF16),
            pltpu.VMEM((m - 1, rows, wide), BF16),
            pltpu.VMEM((rows, wide), BF16),
            pltpu.SemaphoreType.DMA((m - 1,)),
            pltpu.SemaphoreType.DMA((m - 1,)),
            pltpu.SemaphoreType.DMA,
            pltpu.SemaphoreType.DMA((m - 1,)),
            pltpu.SemaphoreType.DMA((m - 1,)),
        ],
        compiler_params=pltpu.CompilerParams(
            collective_id=2, has_side_effects=True, vmem_limit_bytes=56 * 1024 * 1024
        ),
        cost_estimate=pl.CostEstimate(
            flops=2 * rows * y.shape[1] * wide * m, bytes_accessed=60_000_000, transcendentals=0
        ),
    )(y, weights, hidden, gain)


def attention_kernel(n, rows, q_ref, k_ref, v_ref, o_ref, peak, total, acc):
    me = lax.axis_index("seq")
    reach = WINDOW // rows
    factor = HD ** (-0.5) * math.log2(math.e)
    query = q_ref[...]
    row_id = lax.broadcasted_iota(jnp.int32, (rows, rows), 0)
    col_id = lax.broadcasted_iota(jnp.int32, (rows, rows), 1)

    def visit(block, allowed, first, count=1):
        here = pl.ds(pl.multiple_of(block * rows, rows), count * rows)
        scores = lax.dot_general(
            query, k_ref[here, :], (((1,), (1,)), ((), ())), preferred_element_type=F32
        )
        if allowed is not None:
            scores = jnp.where(allowed, scores, -1e30)
        top = jnp.max(scores, axis=1, keepdims=True)
        if not first:
            before = peak[...]
            top = jnp.maximum(before, top)
        weights = jnp.exp2((scores - top) * factor)
        added = jnp.sum(weights, axis=1, keepdims=True)
        product = jnp.dot(weights.astype(BF16), v_ref[here, :], preferred_element_type=F32)
        if first:
            total[...] = added
            acc[...] = product
        else:
            shrink = jnp.exp2((before - top) * factor)
            total[...] = total[...] * shrink + added
            acc[...] = acc[...] * shrink + product
        peak[...] = top

    visit(me, row_id >= col_id, True)
    lowest = jnp.maximum(me - reach + 1, 0)

    twos = (me - lowest) // 2

    def body(i, carry_none):
        visit(lowest + 2 * i, None, False, 2)
        return carry_none

    lax.fori_loop(0, twos, body, 0)

    @pl.when(lowest + 2 * twos < me)
    def _():
        visit(me - 1, None, False)

    if n > reach:

        @pl.when(me >= reach)
        def _():
            visit(me - reach, col_id > row_id, False)

    o_ref[...] = acc[...] / total[...]


def attention(queries, pairs, kv_heads):
    n = lax.axis_size("seq")
    rows = queries.shape[0]
    keys = pairs.shape[0]
    per_kv = queries.shape[1] // HD // kv_heads
    return pl.pallas_call(
        functools.partial(attention_kernel, n, rows),
        grid=(kv_heads, per_kv),
        out_shape=jax.ShapeDtypeStruct(queries.shape, F32),
        in_specs=[
            pl.BlockSpec((rows, HD), lambda i, j: (0, i * per_kv + j)),
            pl.BlockSpec((keys, HD), lambda i, j: (0, i)),
            pl.BlockSpec((keys, HD), lambda i, j: (0, kv_heads + i)),
        ],
        out_specs=pl.BlockSpec((rows, HD), lambda i, j: (0, i * per_kv + j)),
        scratch_shapes=[
            pltpu.VMEM((rows, 1), F32),
            pltpu.VMEM((rows, 1), F32),
            pltpu.VMEM((rows, HD), F32),
        ],
        compiler_params=pltpu.CompilerParams(
            dimension_semantics=("arbitrary", "arbitrary"), vmem_limit_bytes=40 * 1024 * 1024
        ),
        cost_estimate=pl.CostEstimate(
            flops=9_000_000_000, bytes_accessed=20_000_000, transcendentals=17_000_000
        ),
    )(queries, pairs, pairs)


def line_attention_kernel(
    n,
    nt_ref,
    wq_ref,
    wk_ref,
    wv_ref,
    o_ref,
    keys,
    values,
    queries,
    peak,
    total,
    acc,
    send_sem,
    recv_sem,
):
    me = lax.axis_index("seq")
    chips = n // 2
    z, c = me // 2, lax.rem(me, 2)
    partner = 2 * z + 1 - c
    rows = nt_ref.shape[0]
    kv_heads = wk_ref.shape[1] // HD
    per_kv = wq_ref.shape[1] // HD // kv_heads
    factor = HD ** (-0.5) * math.log2(math.e)

    barrier = pltpu.get_barrier_semaphore()
    signal_seq(barrier, partner)
    has_up, has_down = z + 1 <= chips - 1, z >= 1

    @pl.when(has_up)
    def _():
        signal_seq(barrier, me + 2)

    @pl.when(has_down)
    def _():
        signal_seq(barrier, me - 2)

    inner_chip = jnp.logical_and(has_up, has_down)

    @pl.when(inner_chip)
    def _():
        pl.semaphore_wait(barrier, 3)

    @pl.when(jnp.logical_not(inner_chip))
    def _():
        pl.semaphore_wait(barrier, 2)

    stores = (keys, values)

    def copies(slot, kind, d, target):
        return [
            pltpu.make_async_remote_copy(
                src_ref=store.at[slot],
                dst_ref=store.at[slot],
                send_sem=send_sem.at[kind, d, which],
                recv_sem=recv_sem.at[kind, d, which],
                device_id={"seq": target},
                device_id_type=pl.DeviceIdType.MESH,
            )
            for which, store in enumerate(stores)
        ]

    def send(slot, kind, d, target):
        for copy in copies(slot, kind, d, target):
            copy.start()

    def sent(slot, kind, d, target):
        for copy in copies(slot, kind, d, target):
            copy.wait_send()

    def arrived(slot, kind, d):
        for which, store in enumerate(stores):
            place = store.at[slot]
            pltpu.make_async_copy(place, place, recv_sem.at[kind, d, which]).wait()

    keys[me] = jnp.dot(nt_ref[...], wk_ref[...], preferred_element_type=F32).astype(BF16)
    values[me] = jnp.transpose(
        jnp.dot(nt_ref[...], wv_ref[...], preferred_element_type=F32)
    ).astype(BF16)

    @pl.when(has_up)
    def _():
        send(me, 0, 1, me + 2)

    @pl.when(c == 0)
    def _():
        send(me, 1, 0, partner)

    tile = min(256, wq_ref.shape[1])
    for at in range(0, wq_ref.shape[1], tile):
        queries[:, at : at + tile] = jnp.dot(
            nt_ref[...], wq_ref[:, at : at + tile], preferred_element_type=F32
        ).astype(BF16)

    def visit(block, first):
        def group(g, carry_none):
            lanes = pl.ds(pl.multiple_of(g * HD, HD), HD)
            key = keys[block, :, lanes]
            value = values[block, lanes, :]
            for j in range(per_kv):
                h = g * per_kv + j
                query = queries[:, pl.ds(pl.multiple_of(h * HD, HD), HD)]
                scores = lax.dot_general(
                    key, query, (((1,), (1,)), ((), ())), preferred_element_type=F32
                )
                if first:
                    row_id = lax.broadcasted_iota(jnp.int32, (rows, rows), 0)
                    col_id = lax.broadcasted_iota(jnp.int32, (rows, rows), 1)
                    scores = jnp.where(row_id <= col_id, scores, -1e30)
                top = jnp.max(scores, axis=0, keepdims=True)
                if not first:
                    before = peak[h]
                    top = jnp.maximum(before, top)
                weights = jnp.exp2((scores - top) * factor)
                added = jnp.sum(weights, axis=0, keepdims=True)
                product = jnp.dot(value, weights.astype(BF16), preferred_element_type=F32)
                if first:
                    total[h] = added
                    acc[h] = product
                else:
                    shrink = jnp.exp2((before - top) * factor)
                    total[h] = total[h] * shrink + added
                    acc[h] = acc[h] * shrink + product
                peak[h] = top
            return carry_none

        lax.fori_loop(0, kv_heads, group, 0)

    visit(me, True)

    def earlier(t, carry_none):
        d = (t + 1) // 2
        mine = me - 2 * d
        theirs = partner - 2 * d

        @pl.when(lax.rem(t, 2) == 1)
        def _():
            arrived(mine, 0, d)

            @pl.when(has_up)
            def _():
                send(mine, 0, d + 1, me + 2)

            send(mine, 1, d, partner)

        @pl.when(lax.rem(t, 2) == 0)
        def _():
            arrived(theirs, 1, d)

        visit(partner - 2 * d + lax.rem(t, 2) * (me - partner), False)
        return carry_none

    lax.fori_loop(1 - c, 2 * z + 1, earlier, 0)

    for h in range(kv_heads * per_kv):
        o_ref[:, h * HD : (h + 1) * HD] = jnp.transpose(acc[h] / total[h])

    @pl.when(has_up)
    def _():
        sent(me, 0, 1, me + 2)

    @pl.when(c == 0)
    def _():
        sent(me, 1, 0, partner)

    def flush(d, carry_none):
        @pl.when(has_up)
        def _():
            sent(me - 2 * d, 0, d + 1, me + 2)

        sent(me - 2 * d, 1, d, partner)
        return carry_none

    lax.fori_loop(1, z + 1, flush, 0)


def line_attention(normed_two, w_q, w_k, w_v):
    n = lax.axis_size("seq")
    rows = normed_two.shape[0]
    heads = w_q.shape[1] // HD
    wide = w_k.shape[1]
    chips = n // 2
    vmem = pl.BlockSpec(memory_space=pltpu.VMEM)
    return pl.pallas_call(
        functools.partial(line_attention_kernel, n),
        out_shape=jax.ShapeDtypeStruct((rows, w_q.shape[1]), F32),
        in_specs=[vmem] * 4,
        out_specs=vmem,
        scratch_shapes=[
            pltpu.VMEM((n, rows, wide), BF16),
            pltpu.VMEM((n, wide, rows), BF16),
            pltpu.VMEM((rows, w_q.shape[1]), BF16),
            pltpu.VMEM((heads, 1, rows), F32),
            pltpu.VMEM((heads, 1, rows), F32),
            pltpu.VMEM((heads, HD, rows), F32),
            pltpu.SemaphoreType.DMA((2, chips, 2)),
            pltpu.SemaphoreType.DMA((2, chips, 2)),
        ],
        compiler_params=pltpu.CompilerParams(
            collective_id=5, has_side_effects=True, vmem_limit_bytes=56 * 1024 * 1024
        ),
        cost_estimate=pl.CostEstimate(
            flops=18_000_000_000, bytes_accessed=30_000_000, transcendentals=17_000_000
        ),
    )(normed_two, w_q, w_k, w_v)


def pad_lanes(values):
    return jnp.pad(values, ((0, 0), (0, LANES - values.shape[1])))


def spread_kernel(
    n,
    groups,
    hidden_ref,
    gain_ref,
    wx_ref,
    wz_ref,
    wbc_ref,
    wdt_ref,
    all_ref,
    w_ref,
    dt_ref,
    own,
    cols,
    sums,
    local_sem,
    send_sem,
    recv_sem,
):
    me = lax.axis_index("seq")
    member = lax.axis_index("mp")
    chips = n // 2
    z, c = me // 2, lax.rem(me, 2)
    partner = 2 * z + 1 - c
    across = member + 1 - 2 * lax.rem(member, 2)
    along = lax.rem(member + 2, 4)
    far = 3 - member
    rows, wide = own.shape
    depth = wx_ref.shape[0]
    piece = wx_ref.shape[1] // n
    pair = wbc_ref.shape[1] // groups

    names, started = {}, []

    def sem_of(key):
        return recv_sem.at[names.setdefault(key, len(names))]

    def guarded(cond, body):
        if cond is True:
            body()
        else:
            pl.when(cond)(body)

    def send(cond, make_refs, key, **target):
        index = len(started)

        def make():
            source, place = make_refs()
            return pltpu.make_async_remote_copy(
                src_ref=source,
                dst_ref=place,
                send_sem=send_sem.at[index],
                recv_sem=sem_of(key),
                device_id=target,
                device_id_type=pl.DeviceIdType.MESH,
            )

        started.append((cond, make))
        guarded(cond, lambda: make().start())

    def arrived(cond, make_ref, key):
        def body():
            place = make_ref()
            pltpu.make_async_copy(place, place, sem_of(key)).wait()

        guarded(cond, body)

    def both(first, second):
        return second if first is True else jnp.logical_and(first, second)

    barrier = pltpu.get_barrier_semaphore()
    for d in range(1, n):
        signal_seq(barrier, lax.rem(me + d, n))
    for other in (across, along, far):
        signal_mp(barrier, other)
    pl.semaphore_wait(barrier, n - 1 + 3)

    def rows_of(chip, core):
        return pl.ds(pl.multiple_of((2 * chip + core) * depth, depth), depth)

    def send_weights(way, d, same, cond, chip):
        core = c if same else 1 - c
        target = 2 * chip + core
        here = pl.ds(pl.multiple_of(me * depth, depth), depth)
        take = pl.ds(pl.multiple_of(target * piece, piece), piece)
        group = target * groups // n
        key = ("w", way, d, same)
        send(cond, lambda: (wx_ref.at[:, take], w_ref.at[here, 0:piece]), key, seq=target)
        send(cond, lambda: (wz_ref.at[:, take], w_ref.at[here, piece : 2 * piece]), key, seq=target)
        if same or d == 0:
            send(
                cond,
                lambda: (
                    wbc_ref.at[:, pl.ds(pl.multiple_of(group * pair, pair), pair)],
                    w_ref.at[here, 2 * piece : 2 * piece + pair],
                ),
                key,
                seq=target,
            )
        send(cond, lambda: (wdt_ref, dt_ref.at[:, here]), ("dt", way, d, same), seq=target)

    def weights_at(t):
        for d in range(1, chips - (t if t > 1 else 0)):
            for way in (1, -1):
                chip = z + way * d
                behind = z if way == 1 else chips - 1 - z
                now = behind <= 1 if t == 1 else behind == t
                cond = both(now, chip <= chips - 1 if way == 1 else chip >= 0)
                for same in (True, False):
                    send_weights(way, d, same, cond, chip)

    send_weights(0, 0, False, True, z)
    here = pl.ds(pl.multiple_of(me * depth, depth), depth)
    take = pl.ds(pl.multiple_of(me * piece, piece), piece)
    group = pl.ds(pl.multiple_of(me * groups // n * pair, pair), pair)
    locals_ = [
        pltpu.make_async_copy(wx_ref.at[:, take], w_ref.at[here, 0:piece], local_sem.at[0]),
        pltpu.make_async_copy(wz_ref.at[:, take], w_ref.at[here, piece : 2 * piece], local_sem.at[1]),
        pltpu.make_async_copy(
            wbc_ref.at[:, group], w_ref.at[here, 2 * piece : 2 * piece + pair], local_sem.at[2]
        ),
        pltpu.make_async_copy(wdt_ref, dt_ref.at[:, here], local_sem.at[3]),
    ]
    for copy in locals_:
        copy.start()

    tile = min(64, rows)

    def square(i, carry):
        at = pl.ds(pl.multiple_of(i * tile, tile), tile)
        v = hidden_ref[at, :].astype(F32)
        cols[at, :] = jnp.broadcast_to(jnp.sum(v * v, axis=-1, keepdims=True), (tile, LANES))
        return carry

    lax.fori_loop(0, rows // tile, square, 0)
    sums[0] = jnp.transpose(cols[...])[0:8, :]
    for i, other in enumerate((across, along, far)):
        send(True, lambda i=i: (sums.at[0], sums.at[i + 1]), ("sum", i), mp=other)
    for i in range(3):
        arrived(True, lambda i=i: sums.at[i + 1], ("sum", i))
    power = sums[0] + sums[1] + sums[2] + sums[3]
    cols[...] = jnp.transpose(jnp.broadcast_to(power[0:1, :], (LANES, rows)))

    def normalise(i, carry):
        at = pl.ds(pl.multiple_of(i * tile, tile), tile)
        scale = lax.rsqrt(cols[at, 0:1] / (4 * wide) + 1e-05)
        own[at, :] = (hidden_ref[at, :].astype(F32) * scale * gain_ref[...]).astype(BF16)
        return carry

    lax.fori_loop(0, rows // tile, normalise, 0)

    def valid(slot):
        kind, d = slot
        return True if d == 0 else z >= d if kind == "b" else z + d <= chips - 1

    def region(slot, owner, half=None, core=None):
        kind, d = slot
        origin = z - d if kind == "b" else z + d
        core = c if core is None else core
        start = (2 * origin + core) * rows
        size = rows
        if half is not None:
            size = rows // 2
            start = start + half * size
        return all_ref.at[
            pl.ds(pl.multiple_of(start, size), size),
            pl.ds(pl.multiple_of(owner * wide, wide), wide),
        ]

    def stage_a(slot):
        kind, d = slot
        ok = valid(slot)
        if d:
            arrived(ok, lambda: region(slot, member), ("col", slot))

        def source():
            return region(slot, member) if d else own

        if d < chips - 1:
            if kind in "ob":
                up = both(ok, z + 1 <= chips - 1)
                send(up, lambda: (source(), region(slot, member)), ("col", ("b", d + 1)), seq=me + 2)
            if kind in "oa":
                down = both(ok, z >= 1)
                send(down, lambda: (source(), region(slot, member)), ("col", ("a", d + 1)), seq=me - 2)
        send(ok, lambda: (source(), region(slot, member)), ("px", slot), mp=across)
        send(ok, lambda: (source(), region(slot, member)), ("py", slot), mp=along)
        send(ok, lambda: (source(), region(slot, member)), ("d", "col", slot), seq=partner)

    def stage_b(slot):
        ok = valid(slot)
        for q, owner, half, nxt in (("px", across, 0, along), ("py", along, 1, across)):
            arrived(ok, lambda: region(slot, owner), (q, slot))
            send(
                ok,
                lambda owner=owner, half=half: (region(slot, owner, half), region(slot, owner, half)),
                ("half", half, slot),
                mp=nxt,
            )
            send(
                ok,
                lambda owner=owner: (region(slot, owner), region(slot, owner)),
                ("d", q, slot),
                seq=partner,
            )

    def stage_c(slot):
        ok = valid(slot)
        for half in range(2):
            arrived(ok, lambda: region(slot, far, half), ("half", half, slot))
        send(ok, lambda: (region(slot, far), region(slot, far)), ("d", "far", slot), seq=partner)

    own_copy = pltpu.make_async_copy(own, region(("o", 0), member), local_sem.at[4])
    own_copy.start()
    locals_.append(own_copy)

    def step(stage, d):
        for slot in ((("o", 0),) if d == 0 else (("b", d), ("a", d))):
            stage(slot)

    last = chips - 1
    for t in range(chips + 2):
        if t <= last:
            step(stage_a, t)
            if 1 <= t < last:
                weights_at(t)
        if 0 <= t - 1 <= last:
            step(stage_b, t - 1)
        if 0 <= t - 2 <= last:
            step(stage_c, t - 2)

    ways = [(way, d) for d in range(1, chips) for way in (1, -1)]

    def origin_of(way, d):
        chip = z - way * d
        return chip, (chip >= 0 if way == 1 else chip <= chips - 1)

    for way, d in ways:
        chip, ok = origin_of(way, d)
        arrived(ok, lambda: w_ref.at[rows_of(chip, c), :], ("w", way, d, True))

        def shared(chip=chip):
            place = w_ref.at[rows_of(chip, c), 2 * piece : 2 * piece + pair]
            return place, place

        send(ok, shared, ("wd", way, d), seq=partner)
    for way, d in ways:
        chip, ok = origin_of(way, d)
        arrived(ok, lambda: w_ref.at[rows_of(chip, 1 - c), 0 : 2 * piece], ("w", way, d, False))
        arrived(
            ok,
            lambda: w_ref.at[rows_of(chip, 1 - c), 2 * piece : 2 * piece + pair],
            ("wd", way, d),
        )
        for same in (True, False):
            core = c if same else 1 - c
            arrived(ok, lambda: dt_ref.at[:, rows_of(chip, core)], ("dt", way, d, same))
    arrived(True, lambda: w_ref.at[rows_of(z, 1 - c), :], ("w", 0, 0, False))
    arrived(True, lambda: dt_ref.at[:, rows_of(z, 1 - c)], ("dt", 0, 0, False))
    for d in range(chips):
        for slot in ((("o", 0),) if d == 0 else (("b", d), ("a", d))):
            for q, owner in (("col", member), ("px", across), ("py", along), ("far", far)):
                arrived(valid(slot), lambda: region(slot, owner, None, 1 - c), ("d", q, slot))
    for copy in locals_:
        copy.wait()
    for cond, make in started:
        guarded(cond, lambda: make().wait_send())


def spread(hidden, gain, w_x, w_z, w_bc, w_dt, groups):
    n = lax.axis_size("seq")
    rows, wide = hidden.shape
    depth = w_x.shape[0]
    cols = 2 * (w_x.shape[1] // n) + w_bc.shape[1] // groups
    anywhere = pl.BlockSpec(memory_space=pl.ANY)
    vmem = pl.BlockSpec(memory_space=pltpu.VMEM)
    return pl.pallas_call(
        functools.partial(spread_kernel, n, groups),
        out_shape=(
            jax.ShapeDtypeStruct((n * rows, 4 * wide), BF16),
            jax.ShapeDtypeStruct((n * depth, cols), BF16),
            jax.ShapeDtypeStruct((w_dt.shape[0], n * depth), BF16),
        ),
        in_specs=[vmem, vmem] + [anywhere] * 4,
        out_specs=(anywhere,) * 3,
        scratch_shapes=[
            pltpu.VMEM((rows, wide), BF16),
            pltpu.VMEM((rows, LANES), F32),
            pltpu.VMEM((4, 8, rows), F32),
            pltpu.SemaphoreType.DMA((5,)),
            pltpu.SemaphoreType.DMA((50 * n // 2,)),
            pltpu.SemaphoreType.DMA((30 * n // 2,)),
        ],
        compiler_params=pltpu.CompilerParams(
            collective_id=3, has_side_effects=True, vmem_limit_bytes=24 * 1024 * 1024
        ),
        cost_estimate=pl.CostEstimate(
            flops=20_000_000_000, bytes_accessed=100_000_000, transcendentals=0
        ),
    )(hidden, gain, w_x, w_z, w_bc, w_dt)


def heads_kernel(
    n,
    groups,
    hidden_ref,
    w_ref,
    wdt_ref,
    taps_ref,
    bias_ref,
    rate_ref,
    skip_ref,
    gain_ref,
    wout_ref,
    y_ref,
    rows_ref,
    held_ref,
    blocks,
    wdt_own,
    window,
    gate,
    raws,
    conv,
    state,
    out,
    normed,
    power,
    load_sem,
    local_sem,
    power_send,
    power_recv,
    plane_send,
    plane_recv,
    relay_send,
    first_send,
    first_recv,
    wout_send,
    wout_recv,
):
    me = lax.axis_index("seq")
    member = lax.axis_index("mp")
    m = lax.axis_size("mp")
    chips = n // 2
    z, c = me // 2, lax.rem(me, 2)
    partner = 2 * z + 1 - c
    per = n // groups
    base = me // per * per
    place = member * 2 + c
    quarter = 2 * gate.shape[1]
    strip = wout_ref.shape[1]
    across = member + 1 - 2 * lax.rem(member, 2)
    along = lax.rem(member + 2, 4)
    far = 3 - member
    rows = blocks.shape[1]
    inner = gate.shape[1]
    width = inner + 2 * N
    heads = inner // P_SIZE
    kw = taps_ref.shape[0]

    barrier = pltpu.get_barrier_semaphore()
    for d in range(1, n):
        signal_seq(barrier, lax.rem(me + d, n))
    for d in range(1, m):
        for core in range(2):
            pl.semaphore_signal(
                barrier,
                inc=1,
                device_id={"mp": lax.rem(member + d, m), "seq": 2 * z + core},
                device_id_type=pl.DeviceIdType.MESH,
            )
    pl.semaphore_wait(barrier, n - 1 + 2 * (m - 1))

    def remote(source, target_ref, sends, recvs, **target):
        return pltpu.make_async_remote_copy(
            src_ref=source,
            dst_ref=target_ref,
            send_sem=sends,
            recv_sem=recvs,
            device_id=target,
            device_id_type=pl.DeviceIdType.MESH,
        )

    def landed(target_ref, recvs):
        pltpu.make_async_copy(target_ref, target_ref, recvs).wait()

    def own_rows(chip):
        return wout_ref.at[pl.ds(pl.multiple_of(chip * quarter, quarter), quarter), :]

    parts = first_send.shape[0]
    slim = quarter // parts

    def first_leg(d, q):
        chip = lax.rem(z + d, chips)
        return remote(
            wout_ref.at[pl.ds(pl.multiple_of(chip * quarter + q * slim, slim), slim), :],
            held_ref.at[z, pl.ds(pl.multiple_of(q * slim, slim), slim), :],
            first_send.at[q, d],
            first_recv.at[q, d],
            seq=2 * chip + c,
        )

    def second_place(of):
        return rows_ref.at[
            pl.ds(pl.multiple_of(of * quarter, quarter), quarter),
            pl.ds(pl.multiple_of(c * strip, strip), strip),
        ]

    def second_leg(d):
        q = lax.rem(member + d, m)
        return remote(
            held_ref.at[q], second_place(member), wout_send.at[1, d], wout_recv.at[1, d], mp=q
        )

    def third_leg(d):
        of = second_place(lax.rem(member + d, m))
        return remote(of, of, wout_send.at[2, d], wout_recv.at[2, d], seq=partner)

    def keep_held():
        return pltpu.make_async_copy(own_rows(z), held_ref.at[z], local_sem.at[0])

    def keep_rows():
        return pltpu.make_async_copy(held_ref.at[member], second_place(member), local_sem.at[1])

    keep_held().start()

    def load(i, slot):
        return pltpu.make_async_copy(
            hidden_ref.at[pl.ds(pl.multiple_of(i * rows, rows), rows), :],
            blocks.at[slot],
            load_sem.at[slot],
        )

    load(0, 0).start()
    all_heads = wdt_ref.shape[0]
    pick_row = lax.broadcasted_iota(jnp.int32, (LANES, all_heads), 0)
    pick_col = lax.broadcasted_iota(jnp.int32, (LANES, all_heads), 1)
    chosen = jnp.logical_and(pick_col == me * heads + pick_row, pick_row < heads)
    wdt_own[...] = jnp.dot(
        jnp.where(chosen, 1.0, 0.0).astype(BF16), wdt_ref[...], preferred_element_type=F32
    ).astype(BF16)

    lane_head = lax.broadcasted_iota(jnp.int32, (LANES, inner), 1) // P_SIZE
    expand = jnp.where(
        lax.broadcasted_iota(jnp.int32, (LANES, inner), 0) == lane_head, 1.0, 0.0
    ).astype(BF16)
    window[0:8, :] = jnp.zeros((8, width), F32)
    state[...] = jnp.zeros_like(state)
    row_id = lax.broadcasted_iota(jnp.int32, (QB, QB), 0)
    col_id = lax.broadcasted_iota(jnp.int32, (QB, QB), 1)
    causal = row_id >= col_id
    low_lanes = col_id < P_SIZE
    tri = jnp.where(causal, 1.0, 0.0).astype(F32)

    def tell(i, k):
        target = base + lax.rem(me - base + k, per)
        return remote(
            power.at[i, 0], power.at[i, k], power_send.at[i, k], power_recv.at[i, k], seq=target
        )

    def spot(i, at, half=None):
        if half is None:
            return y_ref.at[i // 2, at]
        return y_ref.at[i // 2, at, half * (rows // 2) : (half + 1) * (rows // 2), :]

    def to_plane(i, k):
        return remote(
            normed.at[i],
            spot(i, place),
            plane_send.at[i, k + 1],
            plane_recv.at[i // 2, place, 0],
            mp=(across, along)[k],
            seq=2 * z + lax.rem(i, 2),
        )

    def to_partner(i):
        return remote(
            normed.at[i],
            spot(i, place),
            plane_send.at[i, 0],
            plane_recv.at[i // 2, place, 0],
            seq=partner,
        )

    def to_self(i):
        return pltpu.make_async_copy(normed.at[i], spot(i, place), plane_send.at[i, 0])

    def relay(i, k, core):
        at = (across, along)[k] * 2 + core
        return remote(
            spot(i, at, k),
            spot(i, at, k),
            relay_send.at[i // 2, k, core],
            plane_recv.at[i // 2, at, k],
            mp=(along, across)[k],
        )

    def forward(i):
        @pl.when(lax.rem(i, 2) == c)
        def _():
            for k in range(2):
                for core in range(2):
                    at = (across, along)[k] * 2 + core
                    landed(spot(i, at), plane_recv.at[i // 2, at, 0])
                    relay(i, k, core).start()

    def finish(i):
        for k in range(1, per):
            landed(power.at[i, k], power_recv.at[i, k])
        sums = power[i, 0]
        for k in range(1, per):
            sums = sums + power[i, k]
        column = jnp.transpose(jnp.broadcast_to(sums[0:1, :], (LANES, rows)))
        for sub in range(rows // QB):
            here = slice(sub * QB, (sub + 1) * QB)
            scale = lax.rsqrt(column[here, 0:1] / (per * inner) + 1e-05)
            normed[i, here, :] = (out[i, here, :].astype(F32) * scale * gain_ref[...]).astype(BF16)
        for k in range(2):
            to_plane(i, k).start()

        @pl.when(lax.rem(i, 2) == c)
        def _():
            to_self(i).start()

        @pl.when(lax.rem(i, 2) != c)
        def _():
            to_partner(i).start()

    def block(i, carry_none):
        slot = lax.rem(i, 2)

        @pl.when(i + 1 < n)
        def _():
            load(i + 1, 1 - slot).start()

        load(i, slot).wait()
        source = blocks.at[slot]
        window[8 : 8 + rows, 0:inner] = jnp.dot(
            source[...], w_ref[:, 0:inner], preferred_element_type=F32
        )
        gate[...] = jnp.dot(source[...], w_ref[:, inner : 2 * inner], preferred_element_type=F32)
        window[8 : 8 + rows, inner:width] = jnp.dot(
            source[...], w_ref[:, 2 * inner : 2 * inner + 2 * N], preferred_element_type=F32
        )
        raws[...] = lax.dot_general(
            source[...], wdt_own[...], (((1,), (1,)), ((), ())), preferred_element_type=F32
        )

        @pl.when(i > 0)
        def _():
            finish(i - 1)

        for sub in range(rows // QB):
            at = sub * QB
            here = slice(at, at + QB)
            for start in range(0, width, LANES):
                cs = slice(start, start + LANES)
                total = None
                for j in range(kw):
                    first = 8 - kw + 1 + j + at
                    term = taps_ref[j : j + 1, cs] * window[first : first + QB, cs]
                    total = term if total is None else total + term
                conv[sub, :, cs] = silu(total)
            raw = raws[here, :] + bias_ref[...]
            steps = jnp.maximum(raw, 0.0) + jnp.log1p(jnp.exp(-jnp.abs(raw)))
            decays = -rate_ref[...] * steps
            cum = jnp.dot(tri, decays, precision=HIGH, preferred_element_type=F32)
            cum_t = jnp.transpose(cum)
            grown = jnp.exp(cum)
            tail = jnp.exp(cum[QB - 1 : QB, :] - cum)
            x = conv[sub, :, 0:inner]
            b = conv[sub, :, inner : inner + N].astype(BF16)
            c = conv[sub, :, inner + N : width].astype(BF16)
            scaled = x * spread_heads(steps, expand)
            grown_e = spread_heads(grown, expand)
            tailed = (scaled * spread_heads(tail, expand)).astype(BF16)
            scaled_low = scaled.astype(BF16)
            held = state[...]
            carried = grown_e * jnp.dot(c, held.astype(BF16), preferred_element_type=F32)
            fresh = lax.dot_general(b, tailed, (((0,), (0,)), ((), ())), preferred_element_type=F32)
            state[...] = grown_e[QB - 1 : QB, :] * held + fresh
            affinity = lax.dot_general(c, b, (((1,), (1,)), ((), ())), preferred_element_type=F32)
            affinity = jnp.where(causal, affinity, 0.0)
            full = carried + skip_ref[...] * x
            squares = None
            for pair in range(inner // LANES):
                lanes = slice(pair * LANES, (pair + 1) * LANES)
                outs = []
                for k in range(2):
                    h = pair * 2 + k
                    spread_h = jnp.minimum(cum[:, h : h + 1] - cum_t[h : h + 1, :], 0.0)
                    mixing = (affinity * jnp.exp(spread_h)).astype(BF16)
                    outs.append(
                        jnp.dot(mixing, scaled_low[:, lanes], preferred_element_type=F32)
                    )
                inside = jnp.where(low_lanes, outs[0], outs[1])
                gated = (full[:, lanes] + inside) * silu(gate[here, lanes])
                out[i, here, lanes] = gated.astype(BF16)
                squares = gated * gated if squares is None else squares + gated * gated
            totals = jnp.broadcast_to(jnp.sum(squares, axis=-1, keepdims=True), (QB, LANES))
            power[i, 0, :, here] = jnp.transpose(totals)[0:8, :]
        window[0:8, :] = window[rows : rows + 8, :]

        for k in range(1, per):
            tell(i, k).start()

        @pl.when(i < parts)
        def _():
            for d in range(1, chips):
                first_leg(d, i).start()

        @pl.when(i > 1)
        def _():
            forward(i - 2)

        @pl.when(i == n - 3)
        def _():
            keep_held().wait()
            for d in range(1, chips):
                for q in range(parts):
                    landed(
                        held_ref.at[lax.rem(z + d, chips), q * slim : (q + 1) * slim, :],
                        first_recv.at[q, chips - d],
                    )
            keep_rows().start()
            for d in range(1, m):
                second_leg(d).start()

        return carry_none

    lax.fori_loop(0, n, block, 0)
    finish(n - 1)
    forward(n - 2)
    keep_rows().wait()
    third_leg(0).start()
    for d in range(1, m):
        landed(second_place(lax.rem(member + d, m)), wout_recv.at[1, m - d])
        third_leg(d).start()
    forward(n - 1)
    for d in range(m):
        strips = pl.ds(pl.multiple_of((1 - c) * strip, strip), strip)
        of = lax.rem(member + d, m)
        landed(
            rows_ref.at[pl.ds(pl.multiple_of(of * quarter, quarter), quarter), strips],
            wout_recv.at[2, d],
        )
    for j in range(chips):
        at = member * 2 + 1 - c
        landed(spot(2 * j, at), plane_recv.at[j, at, 0])
        for half in range(2):
            for core in range(2):
                at = far * 2 + core
                landed(spot(2 * j, at, half), plane_recv.at[j, at, half])
                relay(2 * j, half, core).wait_send()

    def flush(i, carry_none):
        for k in range(1, per):
            tell(i, k).wait_send()
        for k in range(2):
            to_plane(i, k).wait_send()

        @pl.when(lax.rem(i, 2) == c)
        def _():
            to_self(i).wait()

        @pl.when(lax.rem(i, 2) != c)
        def _():
            to_partner(i).wait_send()

        return carry_none

    lax.fori_loop(0, n, flush, 0)
    for d in range(1, chips):
        for q in range(parts):
            first_leg(d, q).wait_send()
    for d in range(1, m):
        second_leg(d).wait_send()
    for d in range(m):
        third_leg(d).wait_send()


def mix_heads(hidden, w_out, weights, w_dt, taps, bias, rate, skip, gain, groups):
    n, m = lax.axis_size("seq"), lax.axis_size("mp")
    rows = hidden.shape[0] // n
    features = hidden.shape[1]
    inner = skip.shape[1]
    width = inner + 2 * N
    quarter, strip = 2 * inner, w_out.shape[1]
    per = n // groups
    vmem = pl.BlockSpec(memory_space=pltpu.VMEM)
    anywhere = pl.BlockSpec(memory_space=pl.ANY)
    return pl.pallas_call(
        functools.partial(heads_kernel, n, groups),
        out_shape=(
            jax.ShapeDtypeStruct((n // 2, 2 * m, rows, inner), BF16),
            jax.ShapeDtypeStruct((m * quarter, 2 * strip), BF16),
        ),
        in_specs=[anywhere] + [vmem] * 7 + [anywhere],
        out_specs=(anywhere, vmem),
        scratch_shapes=[
            pltpu.VMEM((n // 2, quarter, strip), BF16),
            pltpu.VMEM((2, rows, features), BF16),
            pltpu.VMEM((LANES, features), BF16),
            pltpu.VMEM((8 + rows, width), F32),
            pltpu.VMEM((rows, inner), F32),
            pltpu.VMEM((rows, LANES), F32),
            pltpu.VMEM((rows // QB, QB, width), F32),
            pltpu.VMEM((N, inner), F32),
            pltpu.VMEM((n, rows, inner), BF16),
            pltpu.VMEM((n, rows, inner), BF16),
            pltpu.VMEM((n, per, 8, rows), F32),
            pltpu.SemaphoreType.DMA((2,)),
            pltpu.SemaphoreType.DMA((2,)),
            pltpu.SemaphoreType.DMA((n, per)),
            pltpu.SemaphoreType.DMA((n, per)),
            pltpu.SemaphoreType.DMA((n, 3)),
            pltpu.SemaphoreType.DMA((n // 2, 2 * m, 2)),
            pltpu.SemaphoreType.DMA((n // 2, 2, 2)),
            pltpu.SemaphoreType.DMA((n // 2, n // 2)),
            pltpu.SemaphoreType.DMA((n // 2, n // 2)),
            pltpu.SemaphoreType.DMA((3, m)),
            pltpu.SemaphoreType.DMA((3, m)),
        ],
        compiler_params=pltpu.CompilerParams(
            collective_id=4, has_side_effects=True, vmem_limit_bytes=48 * 1024 * 1024
        ),
        cost_estimate=pl.CostEstimate(
            flops=40_000_000_000, bytes_accessed=50_000_000, transcendentals=8_000_000
        ),
    )(hidden, weights, w_dt, taps, bias, rate, skip, gain, w_out)


def combine_kernel(
    n,
    y_ref,
    w_ref,
    hidden_ref,
    gain_ref,
    mixed_ref,
    normed_ref,
    part,
    outgoing,
    incoming,
    low,
    send_sem,
    recv_sem,
    own_sem,
    mp_send,
    mp_recv,
):
    me = lax.axis_index("seq")
    member = lax.axis_index("mp")
    chips = n // 2
    z = me // 2
    across = member + 1 - 2 * lax.rem(member, 2)
    along = lax.rem(member + 2, 4)
    far = 3 - member
    rows, wide = hidden_ref.shape
    tall = part.shape[0]
    chunks = rows // tall
    has_up, has_down = z + 1 <= chips - 1, z >= 1

    barrier = pltpu.get_barrier_semaphore()
    signal_mp(barrier, across)
    signal_mp(barrier, along)

    @pl.when(has_up)
    def _():
        signal_seq(barrier, me + 2)

    @pl.when(has_down)
    def _():
        signal_seq(barrier, me - 2)

    ends = jnp.logical_and(has_up, has_down)

    @pl.when(ends)
    def _():
        pl.semaphore_wait(barrier, 4)

    @pl.when(jnp.logical_not(ends))
    def _():
        pl.semaphore_wait(barrier, 3)

    def span(r):
        return pl.ds(pl.multiple_of(r * tall, tall), tall)

    def hand_on(j, r, way):
        return pltpu.make_async_remote_copy(
            src_ref=outgoing.at[j, span(r), :],
            dst_ref=incoming.at[way, j, span(r), :],
            send_sem=send_sem.at[j, r],
            recv_sem=recv_sem.at[way, j, r],
            device_id={"seq": me + 2 if way == 0 else me - 2},
            device_id_type=pl.DeviceIdType.MESH,
        )

    def take(j, r, way):
        where = incoming.at[way, j, span(r), :]
        pltpu.make_async_copy(where, where, recv_sem.at[way, j, r]).wait()
        return incoming[way, j, span(r), :].astype(F32)

    def feature(owner, r, half=None):
        at = pl.ds(pl.multiple_of(owner * wide, wide), wide)
        if half is None:
            return normed_ref.at[span(r), at]
        size = tall // 2
        return normed_ref.at[pl.ds(pl.multiple_of(r * tall + half * size, size), size), at]

    def shares(r):
        return [
            pltpu.make_async_remote_copy(
                src_ref=source,
                dst_ref=place,
                send_sem=mp_send.at[r, index],
                recv_sem=mp_recv.at[r, index],
                device_id={"mp": target},
                device_id_type=pl.DeviceIdType.MESH,
            )
            for index, (source, place, target) in enumerate(
                (
                    (low.at[span(r), :], feature(member, r), across),
                    (low.at[span(r), :], feature(member, r), along),
                    (feature(across, r, 0), feature(across, r, 0), along),
                    (feature(along, r, 1), feature(along, r, 1), across),
                )
            )
        ]

    def own_copy(r):
        return pltpu.make_async_copy(low.at[span(r), :], feature(member, r), own_sem.at[r])

    def arrived(r, index, place):
        pltpu.make_async_copy(place, place, mp_recv.at[r, index]).wait()

    def relay(r):
        mine = shares(r)
        arrived(r, 0, feature(across, r))
        mine[2].start()
        arrived(r, 1, feature(along, r))
        mine[3].start()

    def settle(r):
        arrived(r, 2, feature(far, r, 0))
        arrived(r, 3, feature(far, r, 1))
        own_copy(r).wait()
        for copy in shares(r):
            copy.wait_send()
        step = min(64, tall)
        for at in range(0, tall, step):
            here = pl.ds(pl.multiple_of(r * tall + at, step), step)
            normed_ref[here, :] = rms_norm(
                normed_ref[here, :].astype(F32), gain_ref[...]
            ).astype(BF16)

    order = []
    for k in range((chips + 1) // 2):
        order += [chips - 1 - k] + ([k] if k != chips - 1 - k else [])

    def product(j, r):
        y = jnp.concatenate([y_ref[j, at, span(r), :] for at in range(y_ref.shape[1])], axis=1)
        return jnp.dot(y, w_ref[...], preferred_element_type=F32)

    def outward(r):
        for j in order:

            @pl.when(z != j)
            def _():
                part[...] = product(j, r)

            @pl.when(jnp.logical_and(z < j, z >= 1))
            def _():
                part[...] += take(j, r, 0)

            @pl.when(jnp.logical_and(z > j, z <= chips - 2))
            def _():
                part[...] += take(j, r, 1)

            @pl.when(z != j)
            def _():
                outgoing[j, span(r), :] = part[...].astype(BF16)

            @pl.when(z < j)
            def _():
                hand_on(j, r, 0).start()

            @pl.when(z > j)
            def _():
                hand_on(j, r, 1).start()

    def final(r):
        part[...] = hidden_ref[span(r), :].astype(F32) + product(z, r)

        @pl.when(has_down)
        def _():
            part[...] += take(z, r, 0)

        @pl.when(has_up)
        def _():
            part[...] += take(z, r, 1)

        mixed_ref[span(r), :] = part[...]
        low[span(r), :] = part[...].astype(BF16)
        mine = shares(r)
        mine[0].start()
        mine[1].start()
        own_copy(r).start()

    def chunk(r, carry_none):
        for lag, stage in enumerate((outward, final, relay, settle)):

            @pl.when(jnp.logical_and(r >= lag, r < chunks + lag))
            def _():
                stage(r - lag)

        return carry_none

    lax.fori_loop(0, chunks + 3, chunk, 0)

    def flush(r, carry_none):
        for j in range(chips):

            @pl.when(z < j)
            def _():
                hand_on(j, r, 0).wait_send()

            @pl.when(z > j)
            def _():
                hand_on(j, r, 1).wait_send()

        return carry_none

    lax.fori_loop(0, chunks, flush, 0)


def combine(y, weights, hidden, gain):
    n = lax.axis_size("seq")
    rows, wide = hidden.shape
    chips = n // 2
    tall = min(128, rows)
    chunks = rows // tall
    vmem = pl.BlockSpec(memory_space=pltpu.VMEM)
    return pl.pallas_call(
        functools.partial(combine_kernel, n),
        out_shape=(
            jax.ShapeDtypeStruct((rows, wide), F32),
            jax.ShapeDtypeStruct((rows, 4 * wide), BF16),
        ),
        in_specs=[vmem] * 4,
        out_specs=(vmem, vmem),
        scratch_shapes=[
            pltpu.VMEM((tall, wide), F32),
            pltpu.VMEM((chips, rows, wide), BF16),
            pltpu.VMEM((2, chips, rows, wide), BF16),
            pltpu.VMEM((rows, wide), BF16),
            pltpu.SemaphoreType.DMA((chips, chunks)),
            pltpu.SemaphoreType.DMA((2, chips, chunks)),
            pltpu.SemaphoreType.DMA((chunks,)),
            pltpu.SemaphoreType.DMA((chunks, 4)),
            pltpu.SemaphoreType.DMA((chunks, 4)),
        ],
        compiler_params=pltpu.CompilerParams(
            collective_id=6, has_side_effects=True, vmem_limit_bytes=56 * 1024 * 1024
        ),
        cost_estimate=pl.CostEstimate(
            flops=2 * chips * rows * y.shape[2] * wide,
            bytes_accessed=60_000_000,
            transcendentals=0,
        ),
    )(y, weights, hidden, gain)


def own_slice(values, index, size):
    return lax.dynamic_slice_in_dim(values, index * size, size, values.ndim - 1)


def mixer_by_heads(
    hidden_in, norm_gain, w_z, w_x, w_b, w_c, w_dt, conv_x, conv_b, conv_c, dt_bias, a_rate,
    skip_gain, group_gain,
):
    n = lax.axis_size("seq")
    me = lax.axis_index("seq")
    groups = conv_b.shape[1] // N
    inner = conv_x.shape[1] // n
    heads = dt_bias.shape[0] // n
    group = me * groups // n
    pieces = []
    for g in range(groups):
        pieces += [w_b[:, g * N : (g + 1) * N], w_c[:, g * N : (g + 1) * N]]
    gain = own_slice(norm_gain[None, :], lax.axis_index("mp"), hidden_in.shape[1])
    hidden, weights, steps = spread(
        hidden_in, gain, w_x, w_z, jnp.concatenate(pieces, axis=1), jnp.transpose(w_dt), groups
    )
    taps = jnp.concatenate(
        [own_slice(conv_x, me, inner), own_slice(conv_b, group, N), own_slice(conv_c, group, N)],
        axis=1,
    )
    return hidden, functools.partial(
        mix_heads,
        weights=weights,
        w_dt=steps,
        taps=taps,
        bias=pad_lanes(own_slice(dt_bias[None, :], me, heads)),
        rate=pad_lanes(own_slice(a_rate[None, :], me, heads)),
        skip=jnp.repeat(own_slice(skip_gain[None, :], me, heads), P_SIZE, axis=1),
        gain=own_slice(group_gain[None, :], me, inner),
        groups=groups,
    )


def splits_by_heads(conv_x, conv_b):
    n, m = lax.axis_size("seq"), lax.axis_size("mp")
    groups = conv_b.shape[1] // N
    whole = conv_x.shape[1] % (n * LANES) == 0 and n % groups == 0
    return m == 4 and n == 2 * m and whole


def on_device(
    hidden_in,
    norm_gain,
    w_z,
    w_x,
    w_b,
    w_c,
    w_dt,
    conv_x,
    conv_b,
    conv_c,
    dt_bias,
    a_rate,
    skip_gain,
    group_gain,
    w_out,
    attn_gain,
    w_q,
    w_k,
    w_v,
):
    if splits_by_heads(conv_x, conv_b):
        hidden, mix = mixer_by_heads(
            hidden_in, norm_gain, w_z, w_x, w_b, w_c, w_dt, conv_x, conv_b, conv_c, dt_bias,
            a_rate, skip_gain, group_gain,
        )
        y_normed, out_rows = mix(hidden, w_out)
        mixed, normed_two = combine(y_normed, out_rows, hidden_in, attn_gain[None, :])
    else:
        proj = gather_dot(
            hidden_in,
            norm_gain[None, :],
            jnp.concatenate([w_x, w_b, w_c, pad_lanes(w_dt), w_z], axis=1),
        )
        proj, w_out = lax.optimization_barrier((proj, w_out))
        out_columns = lax.all_gather(w_out, "seq", axis=1, tiled=True)
        heads = dt_bias.shape[0]
        groups = conv_b.shape[1] // N
        width = conv_x.shape[1] + conv_b.shape[1] + conv_c.shape[1]
        rim = from_behind(proj[proj.shape[0] - 8 :, :width], "seq", 1)
        y_normed = mixer(
            proj,
            rim,
            jnp.concatenate([conv_x, conv_b, conv_c], axis=1),
            pad_lanes(dt_bias[None, :]),
            pad_lanes(a_rate[None, :]),
            jnp.repeat(skip_gain, P_SIZE)[None, :],
            group_gain[None, :],
            heads,
            groups,
        )
        mixed, normed_two = output_stage(
            y_normed, out_columns, hidden_in, attn_gain[None, :]
        )
    n = lax.axis_size("seq")
    if n % 2 == 0 and n >= 4 and WINDOW >= n * hidden_in.shape[0]:
        context = line_attention(normed_two, w_q, w_k, w_v)
    else:
        own_keys = jnp.dot(normed_two, w_k, preferred_element_type=F32).astype(BF16)
        own_values = jnp.dot(normed_two, w_v, preferred_element_type=F32).astype(BF16)
        pairs = lax.all_gather(
            jnp.concatenate([own_keys, own_values], axis=1), "seq", axis=0, tiled=True
        )
        queries = jnp.dot(normed_two, w_q, preferred_element_type=F32).astype(BF16)
        context = attention(queries, pairs, own_keys.shape[1] // HD)
    return (mixed, context)


def solution(mesh):
    placed = (
        P("seq", "mp"),
        P(),
        P("seq", "mp"),
        P("seq", "mp"),
        P("seq", "mp"),
        P("seq", "mp"),
        P("seq", "mp"),
        P(None, "mp"),
        P(None, "mp"),
        P(None, "mp"),
        P("mp"),
        P("mp"),
        P("mp"),
        P("mp"),
        P("mp", "seq"),
        P(),
        P(None, "mp"),
        P(None, "mp"),
        P(None, "mp"),
    )
    return jax.shard_map(
        on_device,
        mesh=mesh,
        in_specs=placed,
        out_specs=(P("seq", "mp"), P("seq", "mp")),
        check_vma=False,
    )
```

```python
import functools
import math

import jax
import jax.numpy as jnp
from jax import lax
from jax.experimental import pallas as pl
from jax.experimental.pallas import tpu as pltpu
from jax.sharding import PartitionSpec as P

P_SIZE = 64
N = 128
HD = 128
WINDOW = 4096
QB = 128
LANES = 128
VMEM_LIMIT = 62 * 1024 * 1024

HIGH = lax.Precision.HIGHEST
F32 = jnp.float32
BF16 = jnp.bfloat16


def from_behind(block, axis, distance):
    devices = range(lax.axis_size(axis))
    route = [(i - distance, i) for i in devices if i - distance in devices]
    return lax.ppermute(block, axis, route)


def rms_norm(values, gain):
    return values * lax.rsqrt(jnp.mean(values * values, axis=-1, keepdims=True) + 1e-05) * gain


def signal_seq(sem, index):
    pl.semaphore_signal(
        sem, inc=1, device_id={"seq": index}, device_id_type=pl.DeviceIdType.MESH
    )


def signal_mp(sem, index):
    pl.semaphore_signal(
        sem, inc=1, device_id={"mp": index}, device_id_type=pl.DeviceIdType.MESH
    )


def norm_rows(source, gain_ref, target):
    rows = source.shape[0]
    tile = min(64, rows)

    def body(i, carry_none):
        here = pl.ds(pl.multiple_of(i * tile, tile), tile)
        target[here, :] = rms_norm(source[here, :].astype(F32), gain_ref[...]).astype(BF16)
        return carry_none

    lax.fori_loop(0, rows // tile, body, 0)


def share_features(m, source, whole, send_sem, recv_sem):
    member = lax.axis_index("mp")
    wide = source.shape[1]
    own = pl.ds(pl.multiple_of(member * wide, wide), wide)
    copies = [
        pltpu.make_async_remote_copy(
            src_ref=source,
            dst_ref=whole.at[:, own],
            send_sem=send_sem.at[d - 1],
            recv_sem=recv_sem.at[d - 1],
            device_id={"mp": lax.rem(member + d, m)},
            device_id_type=pl.DeviceIdType.MESH,
        )
        for d in range(1, m)
    ]
    for copy in copies:
        copy.start()
    return copies, own


def features_arrived(m, whole, wide, recv_sem):
    member = lax.axis_index("mp")
    for d in range(1, m):
        sender = lax.rem(member - d + m, m)
        there = whole.at[:, pl.ds(pl.multiple_of(sender * wide, wide), wide)]
        pltpu.make_async_copy(there, there, recv_sem.at[d - 1]).wait()


def gather_dot_kernel(
    n,
    m,
    hidden_ref,
    gain_ref,
    w_ref,
    out_ref,
    slots,
    normed_ref,
    local_sem,
    send_sem,
    recv_sem,
    own_sem,
    mp_send_sem,
    mp_recv_sem,
):
    me = lax.axis_index("seq")
    member = lax.axis_index("mp")
    ring = n // 2
    half = ring // 2
    chip, core = me // 2, lax.rem(me, 2)
    up = lax.rem(chip + 1, ring) * 2 + core
    down = lax.rem(chip + ring - 1, ring) * 2 + core
    partner = chip * 2 + 1 - core
    depth, cols = w_ref.shape
    mid = depth // 2

    barrier = pltpu.get_barrier_semaphore()
    for other in (up, down, partner):
        signal_seq(barrier, other)
    for d in range(1, m):
        signal_mp(barrier, lax.rem(member + d, m))
    pl.semaphore_wait(barrier, 3 + m - 1)

    shared, own = share_features(m, hidden_ref, normed_ref, mp_send_sem, mp_recv_sem)
    own_copy = pltpu.make_async_copy(hidden_ref, normed_ref.at[:, own], own_sem)
    own_copy.start()
    local = pltpu.make_async_copy(w_ref, slots.at[0], local_sem)
    local.start()
    started = []

    def send(source, slot, rows, part, target):
        copy = pltpu.make_async_remote_copy(
            src_ref=source,
            dst_ref=slots.at[slot, rows],
            send_sem=send_sem.at[len(started)],
            recv_sem=recv_sem.at[2 * slot + part],
            device_id={"seq": target},
            device_id_type=pl.DeviceIdType.MESH,
        )
        copy.start()
        started.append(copy)

    def arrived(slot, rows, part):
        pltpu.make_async_copy(
            slots.at[slot, rows], slots.at[slot, rows], recv_sem.at[2 * slot + part]
        ).wait()

    whole, upper, lower = pl.ds(0, depth), pl.ds(0, mid), pl.ds(mid, mid)
    send(w_ref, 2 * 1, whole, 0, up)
    send(w_ref, 2 * (ring - 1), whole, 0, down)
    send(w_ref, 1, whole, 0, partner)

    def multiply(slot, first=False):
        step, lane = slot // 2, slot % 2
        origin = lax.rem(chip - step + ring, ring) * 2
        owner = origin + (core if lane == 0 else 1 - core)
        features = pl.ds(pl.multiple_of(owner * depth, depth), depth)

        def tile(start, width):
            where = pl.ds(start, width)
            product = jnp.dot(
                normed_ref[:, features], slots[slot, :, where], preferred_element_type=F32
            )
            if first:
                out_ref[:, where] = product
            else:
                out_ref[:, where] += product

        width = 512
        full = cols // width

        def body(i, carry):
            tile(pl.multiple_of(i * width, width), width)
            return carry

        lax.fori_loop(0, full, body, 0)
        if cols % width:
            tile(full * width, cols % width)

    own_copy.wait()
    features_arrived(m, normed_ref, hidden_ref.shape[1], mp_recv_sem)
    norm_rows(normed_ref, gain_ref, normed_ref)
    local.wait()
    multiply(0, True)
    arrived(1, whole, 0)
    multiply(1)
    for d in range(1, half):
        s_up, s_down = 2 * d, 2 * (ring - d)
        last = d + 1 == half
        arrived(s_up, whole, 0)
        rows = upper if last else whole
        send(slots.at[s_up, rows], 2 * (d + 1), rows, 0, up)
        arrived(s_down, whole, 0)
        rows = lower if last else whole
        send(slots.at[s_down, rows], 2 * (ring - d - 1), rows, 1 if last else 0, down)
        send(slots.at[s_up, whole], s_up + 1, whole, 0, partner)
        send(slots.at[s_down, whole], s_down + 1, whole, 0, partner)
        multiply(s_up)
        multiply(s_down)
        arrived(s_up + 1, whole, 0)
        multiply(s_up + 1)
        arrived(s_down + 1, whole, 0)
        multiply(s_down + 1)
    far = 2 * half
    arrived(far, upper, 0)
    send(slots.at[far, upper], far + 1, upper, 0, partner)
    arrived(far, lower, 1)
    send(slots.at[far, lower], far + 1, lower, 1, partner)
    multiply(far)
    arrived(far + 1, upper, 0)
    arrived(far + 1, lower, 1)
    multiply(far + 1)
    for copy in started + shared:
        copy.wait_send()


def gather_dot(hidden, gain, weights):
    n, m = lax.axis_size("seq"), lax.axis_size("mp")
    depth, cols = weights.shape
    rows, features = hidden.shape[0], hidden.shape[1] * m
    ring = n // 2
    sends = 3 + 4 * (ring // 2 - 1) + 2
    return pl.pallas_call(
        functools.partial(gather_dot_kernel, n, m),
        out_shape=jax.ShapeDtypeStruct((rows, cols), F32),
        in_specs=[
            pl.BlockSpec(memory_space=pl.ANY),
            pl.BlockSpec(memory_space=pltpu.VMEM),
            pl.BlockSpec(memory_space=pl.ANY),
        ],
        out_specs=pl.BlockSpec(memory_space=pltpu.VMEM),
        scratch_shapes=[
            pltpu.VMEM((n, depth, cols), BF16),
            pltpu.VMEM((rows, features), BF16),
            pltpu.SemaphoreType.DMA,
            pltpu.SemaphoreType.DMA((sends,)),
            pltpu.SemaphoreType.DMA((2 * n,)),
            pltpu.SemaphoreType.DMA,
            pltpu.SemaphoreType.DMA((m - 1,)),
            pltpu.SemaphoreType.DMA((m - 1,)),
        ],
        compiler_params=pltpu.CompilerParams(
            collective_id=0, has_side_effects=True, vmem_limit_bytes=VMEM_LIMIT
        ),
        cost_estimate=pl.CostEstimate(
            flops=2 * rows * features * cols,
            bytes_accessed=160_000_000,
            transcendentals=0,
        ),
    )(hidden, gain, weights)


def silu(v):
    return v / (1.0 + jnp.exp(-v))


def spread_heads(values, expand):
    high = values.astype(BF16)
    low = (values - high.astype(F32)).astype(BF16)
    return jnp.dot(high, expand, preferred_element_type=F32) + jnp.dot(
        low, expand, preferred_element_type=F32
    )


def mixer_kernel(
    n,
    heads,
    groups,
    proj_ref,
    rim_ref,
    taps_ref,
    bias_ref,
    rate_ref,
    skip_ref,
    gain_ref,
    expand_ref,
    y_ref,
    window,
    conv,
    ssd,
    reads,
    logs,
    state,
    carry,
    state_out,
    state_in,
    send_sem,
    recv_sem,
):
    me = lax.axis_index("seq")
    rows = proj_ref.shape[0]
    inner = heads * P_SIZE
    width = inner + 2 * groups * N
    gate_at = width + LANES
    per_group = inner // groups
    blocks = rows // QB
    kw = taps_ref.shape[0]

    barrier = pltpu.get_barrier_semaphore()
    signal_seq(barrier, lax.rem(me + 1, n))
    signal_seq(barrier, lax.rem(me + n - 1, n))
    pl.semaphore_wait(barrier, 2)

    expand = expand_ref[...]
    window[0:8, :] = rim_ref[...]
    state[...] = jnp.zeros_like(state)
    carry[...] = jnp.zeros_like(carry)
    row_id = lax.broadcasted_iota(jnp.int32, (QB, QB), 0)
    col_id = lax.broadcasted_iota(jnp.int32, (QB, QB), 1)
    causal = row_id >= col_id
    low_lanes = col_id < P_SIZE
    tri = jnp.where(causal, 1.0, 0.0).astype(F32)

    def block(i, carry_none):
        base = pl.multiple_of(i * QB, QB)
        here = pl.ds(base, QB)
        window[8 : 8 + QB, :] = proj_ref[here, 0:width]
        step_cols = 256 if width % 256 == 0 else 128
        for at in range(0, width, step_cols):
            cs = slice(at, at + step_cols)
            total = None
            for j in range(kw):
                term = taps_ref[j : j + 1, cs] * window[8 - kw + 1 + j : 8 - kw + 1 + j + QB, cs]
                total = term if total is None else total + term
            conv[:, cs] = silu(total)
        window[0:8, :] = window[QB : QB + 8, :]

        raw = proj_ref[here, width : width + LANES] + bias_ref[...]
        steps = jnp.maximum(raw, 0.0) + jnp.log1p(jnp.exp(-jnp.abs(raw)))
        decays = -rate_ref[...] * steps
        cum = jnp.dot(tri, decays, precision=HIGH, preferred_element_type=F32)
        cum_t = jnp.transpose(cum)
        logs[here, :] = cum + carry[0:1, :]
        carry[...] = carry[...] + cum[QB - 1 : QB, :]
        grown = jnp.exp(cum)
        tail = jnp.exp(cum[QB - 1 : QB, :] - cum)

        for g in range(groups):
            lanes = slice(g * per_group, (g + 1) * per_group)
            expand_g = expand[:, lanes]
            x = conv[:, lanes]
            b = conv[:, inner + g * N : inner + (g + 1) * N].astype(BF16)
            c = conv[:, inner + (groups + g) * N : inner + (groups + g + 1) * N].astype(BF16)
            reads[here, g * N : (g + 1) * N] = c
            scaled = x * spread_heads(steps, expand_g)
            grown_e = spread_heads(grown, expand_g)
            tailed = (scaled * spread_heads(tail, expand_g)).astype(BF16)
            scaled_low = scaled.astype(BF16)
            held = state[:, lanes]
            carried = grown_e * jnp.dot(c, held.astype(BF16), preferred_element_type=F32)
            ssd[here, lanes] = carried + skip_ref[:, lanes] * x
            fresh = lax.dot_general(
                b, tailed, (((0,), (0,)), ((), ())), preferred_element_type=F32
            )
            state[:, lanes] = grown_e[QB - 1 : QB, :] * held + fresh
            affinity = lax.dot_general(
                c, b, (((1,), (1,)), ((), ())), preferred_element_type=F32
            )
            affinity = jnp.where(causal, affinity, 0.0)
            for pair in range(per_group // LANES):
                at = pair * LANES
                inputs = scaled_low[:, at : at + LANES]
                outs = []
                for k in range(2):
                    h = (g * per_group + at) // P_SIZE + k
                    spread = jnp.minimum(cum[:, h : h + 1] - cum_t[h : h + 1, :], 0.0)
                    mixing = (affinity * jnp.exp(spread)).astype(BF16)
                    outs.append(jnp.dot(mixing, inputs, preferred_element_type=F32))
                where = slice(g * per_group + at, g * per_group + at + LANES)
                ssd[here, where] += jnp.where(low_lanes, outs[0], outs[1])
        return carry_none

    lax.fori_loop(0, blocks, block, 0)

    parts = 4
    piece = inner // parts
    decay = jnp.exp(carry[...])

    def hand_on(k):
        lanes = slice(k * piece, (k + 1) * piece)
        return pltpu.make_async_remote_copy(
            src_ref=state_out.at[:, lanes],
            dst_ref=state_in.at[:, lanes],
            send_sem=send_sem.at[k],
            recv_sem=recv_sem.at[k],
            device_id={"seq": jnp.minimum(me + 1, n - 1)},
            device_id_type=pl.DeviceIdType.MESH,
        )

    for k in range(parts):
        lanes = slice(k * piece, (k + 1) * piece)
        weight = spread_heads(decay, expand[:, lanes])[0:1, :]

        @pl.when(me > 0)
        def _():
            hand_on(k).wait_recv()
            before = state_in[:, lanes].astype(F32)
            state_out[:, lanes] = (weight * before + state[:, lanes]).astype(BF16)

        @pl.when(me == 0)
        def _():
            state_out[:, lanes] = state[:, lanes].astype(BF16)
            state_in[:, lanes] = jnp.zeros((N, piece), BF16)

        @pl.when(me < n - 1)
        def _():
            hand_on(k).start()

    def finish(i, carry_none):
        here = pl.ds(pl.multiple_of(i * QB, QB), QB)
        grown = jnp.exp(logs[here, :])
        for g in range(groups):
            lanes = slice(g * per_group, (g + 1) * per_group)
            late = jnp.dot(
                reads[here, g * N : (g + 1) * N],
                state_in[:, lanes],
                preferred_element_type=F32,
            )
            full = ssd[here, lanes] + spread_heads(grown, expand[:, lanes]) * late
            gate = proj_ref[here, gate_at + g * per_group : gate_at + (g + 1) * per_group]
            gated = full * silu(gate)
            power = jnp.mean(gated * gated, axis=-1, keepdims=True)
            y_ref[here, lanes] = (gated * lax.rsqrt(power + 1e-05) * gain_ref[:, lanes]).astype(BF16)
        return carry_none

    lax.fori_loop(0, blocks, finish, 0)

    @pl.when(me < n - 1)
    def _():
        for k in range(parts):
            hand_on(k).wait_send()


def mixer(proj, rim, taps, bias, rate, skip, gain, heads, groups):
    n = lax.axis_size("seq")
    rows = proj.shape[0]
    inner = heads * P_SIZE
    width = inner + 2 * groups * N
    expand = (
        jnp.arange(LANES)[:, None] == (jnp.arange(inner) // P_SIZE)[None, :]
    ).astype(BF16)
    vmem = pl.BlockSpec(memory_space=pltpu.VMEM)
    return pl.pallas_call(
        functools.partial(mixer_kernel, n, heads, groups),
        out_shape=jax.ShapeDtypeStruct((rows, inner), BF16),
        in_specs=[vmem] * 8,
        out_specs=vmem,
        scratch_shapes=[
            pltpu.VMEM((8 + QB, width), F32),
            pltpu.VMEM((QB, width), F32),
            pltpu.VMEM((rows, inner), F32),
            pltpu.VMEM((rows, groups * N), BF16),
            pltpu.VMEM((rows, LANES), F32),
            pltpu.VMEM((N, inner), F32),
            pltpu.VMEM((8, LANES), F32),
            pltpu.VMEM((N, inner), BF16),
            pltpu.VMEM((N, inner), BF16),
            pltpu.SemaphoreType.DMA((4,)),
            pltpu.SemaphoreType.DMA((4,)),
        ],
        compiler_params=pltpu.CompilerParams(
            collective_id=1, has_side_effects=True, vmem_limit_bytes=48 * 1024 * 1024
        ),
        cost_estimate=pl.CostEstimate(
            flops=8_000_000_000, bytes_accessed=100_000_000, transcendentals=8_000_000
        ),
    )(proj, rim, taps, bias, rate, skip, gain, expand)


def output_kernel(
    m,
    y_ref,
    w_ref,
    hidden_ref,
    gain_ref,
    mixed_ref,
    normed_ref,
    outgoing,
    incoming,
    low,
    part_send,
    part_recv,
    own_sem,
    mp_send,
    mp_recv,
):
    member = lax.axis_index("mp")
    wide = hidden_ref.shape[1]
    barrier = pltpu.get_barrier_semaphore()
    for d in range(1, m):
        signal_mp(barrier, lax.rem(member + d, m))
    pl.semaphore_wait(barrier, m - 1)
    tile = min(512, wide)

    def part(target, store):
        for at in range(0, wide, tile):
            where = pl.ds(pl.multiple_of(target * wide + at, tile), tile)
            term = jnp.dot(y_ref[...], w_ref[:, where], preferred_element_type=F32)
            store(slice(at, at + tile), term.astype(BF16))

    copies = []
    for d in range(1, m):
        target = lax.rem(member + d, m)

        def keep(where, term):
            outgoing[d - 1, :, where] = term

        part(target, keep)
        copy = pltpu.make_async_remote_copy(
            src_ref=outgoing.at[d - 1],
            dst_ref=incoming.at[d - 1],
            send_sem=part_send.at[d - 1],
            recv_sem=part_recv.at[d - 1],
            device_id={"mp": target},
            device_id_type=pl.DeviceIdType.MESH,
        )
        copy.start()
        copies.append(copy)

    def begin(where, term):
        mixed_ref[:, where] = hidden_ref[:, where].astype(F32) + term.astype(F32)

    part(member, begin)
    for d in range(1, m):
        copies[d - 1].wait_recv()
        if d < m - 1:
            mixed_ref[...] += incoming[d - 1].astype(F32)
        else:
            total = mixed_ref[...] + incoming[d - 1].astype(F32)
            mixed_ref[...] = total
            low[...] = total.astype(BF16)
    shared, own = share_features(m, low, normed_ref, mp_send, mp_recv)
    own_copy = pltpu.make_async_copy(low, normed_ref.at[:, own], own_sem)
    own_copy.start()
    own_copy.wait()
    features_arrived(m, normed_ref, wide, mp_recv)
    norm_rows(normed_ref, gain_ref, normed_ref)
    for copy in copies + shared:
        copy.wait_send()


def output_stage(y, weights, hidden, gain):
    m = lax.axis_size("mp")
    rows, wide = hidden.shape
    vmem = pl.BlockSpec(memory_space=pltpu.VMEM)
    return pl.pallas_call(
        functools.partial(output_kernel, m),
        out_shape=(
            jax.ShapeDtypeStruct((rows, wide), F32),
            jax.ShapeDtypeStruct((rows, wide * m), BF16),
        ),
        in_specs=[vmem] * 4,
        out_specs=(vmem, vmem),
        scratch_shapes=[
            pltpu.VMEM((m - 1, rows, wide), BF16),
            pltpu.VMEM((m - 1, rows, wide), BF16),
            pltpu.VMEM((rows, wide), BF16),
            pltpu.SemaphoreType.DMA((m - 1,)),
            pltpu.SemaphoreType.DMA((m - 1,)),
            pltpu.SemaphoreType.DMA,
            pltpu.SemaphoreType.DMA((m - 1,)),
            pltpu.SemaphoreType.DMA((m - 1,)),
        ],
        compiler_params=pltpu.CompilerParams(
            collective_id=2, has_side_effects=True, vmem_limit_bytes=56 * 1024 * 1024
        ),
        cost_estimate=pl.CostEstimate(
            flops=2 * rows * y.shape[1] * wide * m, bytes_accessed=60_000_000, transcendentals=0
        ),
    )(y, weights, hidden, gain)


def attention_kernel(n, rows, q_ref, k_ref, v_ref, o_ref, peak, total, acc):
    me = lax.axis_index("seq")
    reach = WINDOW // rows
    factor = HD ** (-0.5) * math.log2(math.e)
    query = q_ref[...]
    row_id = lax.broadcasted_iota(jnp.int32, (rows, rows), 0)
    col_id = lax.broadcasted_iota(jnp.int32, (rows, rows), 1)

    def visit(block, allowed, first, count=1):
        here = pl.ds(pl.multiple_of(block * rows, rows), count * rows)
        scores = lax.dot_general(
            query, k_ref[here, :], (((1,), (1,)), ((), ())), preferred_element_type=F32
        )
        if allowed is not None:
            scores = jnp.where(allowed, scores, -1e30)
        top = jnp.max(scores, axis=1, keepdims=True)
        if not first:
            before = peak[...]
            top = jnp.maximum(before, top)
        weights = jnp.exp2((scores - top) * factor)
        added = jnp.sum(weights, axis=1, keepdims=True)
        product = jnp.dot(weights.astype(BF16), v_ref[here, :], preferred_element_type=F32)
        if first:
            total[...] = added
            acc[...] = product
        else:
            shrink = jnp.exp2((before - top) * factor)
            total[...] = total[...] * shrink + added
            acc[...] = acc[...] * shrink + product
        peak[...] = top

    visit(me, row_id >= col_id, True)
    lowest = jnp.maximum(me - reach + 1, 0)

    twos = (me - lowest) // 2

    def body(i, carry_none):
        visit(lowest + 2 * i, None, False, 2)
        return carry_none

    lax.fori_loop(0, twos, body, 0)

    @pl.when(lowest + 2 * twos < me)
    def _():
        visit(me - 1, None, False)

    if n > reach:

        @pl.when(me >= reach)
        def _():
            visit(me - reach, col_id > row_id, False)

    o_ref[...] = acc[...] / total[...]


def attention(queries, pairs, kv_heads):
    n = lax.axis_size("seq")
    rows = queries.shape[0]
    keys = pairs.shape[0]
    per_kv = queries.shape[1] // HD // kv_heads
    return pl.pallas_call(
        functools.partial(attention_kernel, n, rows),
        grid=(kv_heads, per_kv),
        out_shape=jax.ShapeDtypeStruct(queries.shape, F32),
        in_specs=[
            pl.BlockSpec((rows, HD), lambda i, j: (0, i * per_kv + j)),
            pl.BlockSpec((keys, HD), lambda i, j: (0, i)),
            pl.BlockSpec((keys, HD), lambda i, j: (0, kv_heads + i)),
        ],
        out_specs=pl.BlockSpec((rows, HD), lambda i, j: (0, i * per_kv + j)),
        scratch_shapes=[
            pltpu.VMEM((rows, 1), F32),
            pltpu.VMEM((rows, 1), F32),
            pltpu.VMEM((rows, HD), F32),
        ],
        compiler_params=pltpu.CompilerParams(
            dimension_semantics=("arbitrary", "arbitrary"), vmem_limit_bytes=40 * 1024 * 1024
        ),
        cost_estimate=pl.CostEstimate(
            flops=9_000_000_000, bytes_accessed=20_000_000, transcendentals=17_000_000
        ),
    )(queries, pairs, pairs)


def line_attention_kernel(
    n,
    nt_ref,
    wq_ref,
    wk_ref,
    wv_ref,
    o_ref,
    keys,
    values,
    queries,
    peak,
    total,
    acc,
    send_sem,
    recv_sem,
):
    me = lax.axis_index("seq")
    chips = n // 2
    z, c = me // 2, lax.rem(me, 2)
    partner = 2 * z + 1 - c
    rows = nt_ref.shape[0]
    kv_heads = wk_ref.shape[1] // HD
    per_kv = wq_ref.shape[1] // HD // kv_heads
    factor = HD ** (-0.5) * math.log2(math.e)

    barrier = pltpu.get_barrier_semaphore()
    signal_seq(barrier, partner)
    has_up, has_down = z + 1 <= chips - 1, z >= 1

    @pl.when(has_up)
    def _():
        signal_seq(barrier, me + 2)

    @pl.when(has_down)
    def _():
        signal_seq(barrier, me - 2)

    inner_chip = jnp.logical_and(has_up, has_down)

    @pl.when(inner_chip)
    def _():
        pl.semaphore_wait(barrier, 3)

    @pl.when(jnp.logical_not(inner_chip))
    def _():
        pl.semaphore_wait(barrier, 2)

    stores = (keys, values)

    def copies(slot, kind, d, target):
        return [
            pltpu.make_async_remote_copy(
                src_ref=store.at[slot],
                dst_ref=store.at[slot],
                send_sem=send_sem.at[kind, d, which],
                recv_sem=recv_sem.at[kind, d, which],
                device_id={"seq": target},
                device_id_type=pl.DeviceIdType.MESH,
            )
            for which, store in enumerate(stores)
        ]

    def send(slot, kind, d, target):
        for copy in copies(slot, kind, d, target):
            copy.start()

    def sent(slot, kind, d, target):
        for copy in copies(slot, kind, d, target):
            copy.wait_send()

    def arrived(slot, kind, d):
        for which, store in enumerate(stores):
            place = store.at[slot]
            pltpu.make_async_copy(place, place, recv_sem.at[kind, d, which]).wait()

    keys[me] = jnp.dot(nt_ref[...], wk_ref[...], preferred_element_type=F32).astype(BF16)
    values[me] = jnp.transpose(
        jnp.dot(nt_ref[...], wv_ref[...], preferred_element_type=F32)
    ).astype(BF16)

    @pl.when(has_up)
    def _():
        send(me, 0, 1, me + 2)

    @pl.when(c == 0)
    def _():
        send(me, 1, 0, partner)

    tile = min(256, wq_ref.shape[1])
    for at in range(0, wq_ref.shape[1], tile):
        queries[:, at : at + tile] = jnp.dot(
            nt_ref[...], wq_ref[:, at : at + tile], preferred_element_type=F32
        ).astype(BF16)

    def visit(block, first):
        def group(g, carry_none):
            lanes = pl.ds(pl.multiple_of(g * HD, HD), HD)
            key = keys[block, :, lanes]
            value = values[block, lanes, :]
            for j in range(per_kv):
                h = g * per_kv + j
                query = queries[:, pl.ds(pl.multiple_of(h * HD, HD), HD)]
                scores = lax.dot_general(
                    key, query, (((1,), (1,)), ((), ())), preferred_element_type=F32
                )
                if first:
                    row_id = lax.broadcasted_iota(jnp.int32, (rows, rows), 0)
                    col_id = lax.broadcasted_iota(jnp.int32, (rows, rows), 1)
                    scores = jnp.where(row_id <= col_id, scores, -1e30)
                top = jnp.max(scores, axis=0, keepdims=True)
                if not first:
                    before = peak[h]
                    top = jnp.maximum(before, top)
                weights = jnp.exp2((scores - top) * factor)
                added = jnp.sum(weights, axis=0, keepdims=True)
                product = jnp.dot(value, weights.astype(BF16), preferred_element_type=F32)
                if first:
                    total[h] = added
                    acc[h] = product
                else:
                    shrink = jnp.exp2((before - top) * factor)
                    total[h] = total[h] * shrink + added
                    acc[h] = acc[h] * shrink + product
                peak[h] = top
            return carry_none

        lax.fori_loop(0, kv_heads, group, 0)

    visit(me, True)

    def earlier(t, carry_none):
        d = (t + 1) // 2
        mine = me - 2 * d
        theirs = partner - 2 * d

        @pl.when(lax.rem(t, 2) == 1)
        def _():
            arrived(mine, 0, d)

            @pl.when(has_up)
            def _():
                send(mine, 0, d + 1, me + 2)

            send(mine, 1, d, partner)

        @pl.when(lax.rem(t, 2) == 0)
        def _():
            arrived(theirs, 1, d)

        visit(partner - 2 * d + lax.rem(t, 2) * (me - partner), False)
        return carry_none

    lax.fori_loop(1 - c, 2 * z + 1, earlier, 0)

    for h in range(kv_heads * per_kv):
        o_ref[:, h * HD : (h + 1) * HD] = jnp.transpose(acc[h] / total[h])

    @pl.when(has_up)
    def _():
        sent(me, 0, 1, me + 2)

    @pl.when(c == 0)
    def _():
        sent(me, 1, 0, partner)

    def flush(d, carry_none):
        @pl.when(has_up)
        def _():
            sent(me - 2 * d, 0, d + 1, me + 2)

        sent(me - 2 * d, 1, d, partner)
        return carry_none

    lax.fori_loop(1, z + 1, flush, 0)


def line_attention(normed_two, w_q, w_k, w_v):
    n = lax.axis_size("seq")
    rows = normed_two.shape[0]
    heads = w_q.shape[1] // HD
    wide = w_k.shape[1]
    chips = n // 2
    vmem = pl.BlockSpec(memory_space=pltpu.VMEM)
    return pl.pallas_call(
        functools.partial(line_attention_kernel, n),
        out_shape=jax.ShapeDtypeStruct((rows, w_q.shape[1]), F32),
        in_specs=[vmem] * 4,
        out_specs=vmem,
        scratch_shapes=[
            pltpu.VMEM((n, rows, wide), BF16),
            pltpu.VMEM((n, wide, rows), BF16),
            pltpu.VMEM((rows, w_q.shape[1]), BF16),
            pltpu.VMEM((heads, 1, rows), F32),
            pltpu.VMEM((heads, 1, rows), F32),
            pltpu.VMEM((heads, HD, rows), F32),
            pltpu.SemaphoreType.DMA((2, chips, 2)),
            pltpu.SemaphoreType.DMA((2, chips, 2)),
        ],
        compiler_params=pltpu.CompilerParams(
            collective_id=5, has_side_effects=True, vmem_limit_bytes=56 * 1024 * 1024
        ),
        cost_estimate=pl.CostEstimate(
            flops=18_000_000_000, bytes_accessed=30_000_000, transcendentals=17_000_000
        ),
    )(normed_two, w_q, w_k, w_v)


def pad_lanes(values):
    return jnp.pad(values, ((0, 0), (0, LANES - values.shape[1])))


def spread_kernel(
    n,
    groups,
    hidden_ref,
    gain_ref,
    wx_ref,
    wz_ref,
    wbc_ref,
    wdt_ref,
    all_ref,
    w_ref,
    dt_ref,
    own,
    cols,
    sums,
    local_sem,
    send_sem,
    recv_sem,
):
    me = lax.axis_index("seq")
    member = lax.axis_index("mp")
    chips = n // 2
    z, c = me // 2, lax.rem(me, 2)
    partner = 2 * z + 1 - c
    across = member + 1 - 2 * lax.rem(member, 2)
    along = lax.rem(member + 2, 4)
    far = 3 - member
    rows, wide = own.shape
    depth = wx_ref.shape[0]
    piece = wx_ref.shape[1] // n
    pair = wbc_ref.shape[1] // groups

    names, started = {}, []

    def sem_of(key):
        return recv_sem.at[names.setdefault(key, len(names))]

    def guarded(cond, body):
        if cond is True:
            body()
        else:
            pl.when(cond)(body)

    def send(cond, make_refs, key, **target):
        index = len(started)

        def make():
            source, place = make_refs()
            return pltpu.make_async_remote_copy(
                src_ref=source,
                dst_ref=place,
                send_sem=send_sem.at[index],
                recv_sem=sem_of(key),
                device_id=target,
                device_id_type=pl.DeviceIdType.MESH,
            )

        started.append((cond, make))
        guarded(cond, lambda: make().start())

    def arrived(cond, make_ref, key):
        def body():
            place = make_ref()
            pltpu.make_async_copy(place, place, sem_of(key)).wait()

        guarded(cond, body)

    def both(first, second):
        return second if first is True else jnp.logical_and(first, second)

    barrier = pltpu.get_barrier_semaphore()
    for d in range(1, n):
        signal_seq(barrier, lax.rem(me + d, n))
    for other in (across, along, far):
        signal_mp(barrier, other)
    pl.semaphore_wait(barrier, n - 1 + 3)

    def rows_of(chip, core):
        return pl.ds(pl.multiple_of((2 * chip + core) * depth, depth), depth)

    def send_weights(way, d, same, cond, chip):
        core = c if same else 1 - c
        target = 2 * chip + core
        here = pl.ds(pl.multiple_of(me * depth, depth), depth)
        take = pl.ds(pl.multiple_of(target * piece, piece), piece)
        group = target * groups // n
        key = ("w", way, d, same)
        send(cond, lambda: (wx_ref.at[:, take], w_ref.at[here, 0:piece]), key, seq=target)
        send(cond, lambda: (wz_ref.at[:, take], w_ref.at[here, piece : 2 * piece]), key, seq=target)
        if same or d == 0:
            send(
                cond,
                lambda: (
                    wbc_ref.at[:, pl.ds(pl.multiple_of(group * pair, pair), pair)],
                    w_ref.at[here, 2 * piece : 2 * piece + pair],
                ),
                key,
                seq=target,
            )
        send(cond, lambda: (wdt_ref, dt_ref.at[:, here]), ("dt", way, d, same), seq=target)

    def weights_at(t):
        for d in range(1, chips - (t if t > 1 else 0)):
            for way in (1, -1):
                chip = z + way * d
                behind = z if way == 1 else chips - 1 - z
                now = behind <= 1 if t == 1 else behind == t
                cond = both(now, chip <= chips - 1 if way == 1 else chip >= 0)
                for same in (True, False):
                    send_weights(way, d, same, cond, chip)

    send_weights(0, 0, False, True, z)
    here = pl.ds(pl.multiple_of(me * depth, depth), depth)
    take = pl.ds(pl.multiple_of(me * piece, piece), piece)
    group = pl.ds(pl.multiple_of(me * groups // n * pair, pair), pair)
    locals_ = [
        pltpu.make_async_copy(wx_ref.at[:, take], w_ref.at[here, 0:piece], local_sem.at[0]),
        pltpu.make_async_copy(wz_ref.at[:, take], w_ref.at[here, piece : 2 * piece], local_sem.at[1]),
        pltpu.make_async_copy(
            wbc_ref.at[:, group], w_ref.at[here, 2 * piece : 2 * piece + pair], local_sem.at[2]
        ),
        pltpu.make_async_copy(wdt_ref, dt_ref.at[:, here], local_sem.at[3]),
    ]
    for copy in locals_:
        copy.start()

    tile = min(64, rows)

    def square(i, carry):
        at = pl.ds(pl.multiple_of(i * tile, tile), tile)
        v = hidden_ref[at, :].astype(F32)
        cols[at, :] = jnp.broadcast_to(jnp.sum(v * v, axis=-1, keepdims=True), (tile, LANES))
        return carry

    lax.fori_loop(0, rows // tile, square, 0)
    sums[0] = jnp.transpose(cols[...])[0:8, :]
    for i, other in enumerate((across, along, far)):
        send(True, lambda i=i: (sums.at[0], sums.at[i + 1]), ("sum", i), mp=other)
    for i in range(3):
        arrived(True, lambda i=i: sums.at[i + 1], ("sum", i))
    power = sums[0] + sums[1] + sums[2] + sums[3]
    cols[...] = jnp.transpose(jnp.broadcast_to(power[0:1, :], (LANES, rows)))

    def normalise(i, carry):
        at = pl.ds(pl.multiple_of(i * tile, tile), tile)
        scale = lax.rsqrt(cols[at, 0:1] / (4 * wide) + 1e-05)
        own[at, :] = (hidden_ref[at, :].astype(F32) * scale * gain).astype(BF16)
        return carry

    gain = gain_ref[:, pl.ds(pl.multiple_of(member * wide, wide), wide)]
    lax.fori_loop(0, rows // tile, normalise, 0)

    def valid(slot):
        kind, d = slot
        return True if d == 0 else z >= d if kind == "b" else z + d <= chips - 1

    def region(slot, owner, half=None, core=None):
        kind, d = slot
        origin = z - d if kind == "b" else z + d
        core = c if core is None else core
        start = (2 * origin + core) * rows
        size = rows
        if half is not None:
            size = rows // 2
            start = start + half * size
        return all_ref.at[
            pl.ds(pl.multiple_of(start, size), size),
            pl.ds(pl.multiple_of(owner * wide, wide), wide),
        ]

    def stage_a(slot):
        kind, d = slot
        ok = valid(slot)
        if d:
            arrived(ok, lambda: region(slot, member), ("col", slot))

        def source():
            return region(slot, member) if d else own

        if d < chips - 1:
            if kind in "ob":
                up = both(ok, z + 1 <= chips - 1)
                send(up, lambda: (source(), region(slot, member)), ("col", ("b", d + 1)), seq=me + 2)
            if kind in "oa":
                down = both(ok, z >= 1)
                send(down, lambda: (source(), region(slot, member)), ("col", ("a", d + 1)), seq=me - 2)
        send(ok, lambda: (source(), region(slot, member)), ("px", slot), mp=across)
        send(ok, lambda: (source(), region(slot, member)), ("py", slot), mp=along)
        send(ok, lambda: (source(), region(slot, member)), ("d", "col", slot), seq=partner)

    def stage_b(slot):
        ok = valid(slot)
        for q, owner, half, nxt in (("px", across, 0, along), ("py", along, 1, across)):
            arrived(ok, lambda: region(slot, owner), (q, slot))
            send(
                ok,
                lambda owner=owner, half=half: (region(slot, owner, half), region(slot, owner, half)),
                ("half", half, slot),
                mp=nxt,
            )
            send(
                ok,
                lambda owner=owner: (region(slot, owner), region(slot, owner)),
                ("d", q, slot),
                seq=partner,
            )

    def stage_c(slot):
        ok = valid(slot)
        for half in range(2):
            arrived(ok, lambda: region(slot, far, half), ("half", half, slot))
        send(ok, lambda: (region(slot, far), region(slot, far)), ("d", "far", slot), seq=partner)

    own_copy = pltpu.make_async_copy(own, region(("o", 0), member), local_sem.at[4])
    own_copy.start()
    locals_.append(own_copy)

    def step(stage, d):
        for slot in ((("o", 0),) if d == 0 else (("b", d), ("a", d))):
            stage(slot)

    last = chips - 1
    for t in range(chips + 2):
        if t <= last:
            step(stage_a, t)
            if 1 <= t < last:
                weights_at(t)
        if 0 <= t - 1 <= last:
            step(stage_b, t - 1)
        if 0 <= t - 2 <= last:
            step(stage_c, t - 2)

    ways = [(way, d) for d in range(1, chips) for way in (1, -1)]

    def origin_of(way, d):
        chip = z - way * d
        return chip, (chip >= 0 if way == 1 else chip <= chips - 1)

    for way, d in ways:
        chip, ok = origin_of(way, d)
        arrived(ok, lambda: w_ref.at[rows_of(chip, c), :], ("w", way, d, True))

        def shared(chip=chip):
            place = w_ref.at[rows_of(chip, c), 2 * piece : 2 * piece + pair]
            return place, place

        send(ok, shared, ("wd", way, d), seq=partner)
    for way, d in ways:
        chip, ok = origin_of(way, d)
        arrived(ok, lambda: w_ref.at[rows_of(chip, 1 - c), 0 : 2 * piece], ("w", way, d, False))
        arrived(
            ok,
            lambda: w_ref.at[rows_of(chip, 1 - c), 2 * piece : 2 * piece + pair],
            ("wd", way, d),
        )
        for same in (True, False):
            core = c if same else 1 - c
            arrived(ok, lambda: dt_ref.at[:, rows_of(chip, core)], ("dt", way, d, same))
    arrived(True, lambda: w_ref.at[rows_of(z, 1 - c), :], ("w", 0, 0, False))
    arrived(True, lambda: dt_ref.at[:, rows_of(z, 1 - c)], ("dt", 0, 0, False))
    for d in range(chips):
        for slot in ((("o", 0),) if d == 0 else (("b", d), ("a", d))):
            for q, owner in (("col", member), ("px", across), ("py", along), ("far", far)):
                arrived(valid(slot), lambda: region(slot, owner, None, 1 - c), ("d", q, slot))
    for copy in locals_:
        copy.wait()
    for cond, make in started:
        guarded(cond, lambda: make().wait_send())


def spread(hidden, gain, w_x, w_z, w_bc, w_dt, groups):
    n = lax.axis_size("seq")
    rows, wide = hidden.shape
    depth = w_x.shape[0]
    cols = 2 * (w_x.shape[1] // n) + w_bc.shape[1] // groups
    anywhere = pl.BlockSpec(memory_space=pl.ANY)
    vmem = pl.BlockSpec(memory_space=pltpu.VMEM)
    return pl.pallas_call(
        functools.partial(spread_kernel, n, groups),
        out_shape=(
            jax.ShapeDtypeStruct((n * rows, 4 * wide), BF16),
            jax.ShapeDtypeStruct((n * depth, cols), BF16),
            jax.ShapeDtypeStruct((w_dt.shape[0], n * depth), BF16),
        ),
        in_specs=[vmem, vmem] + [anywhere] * 4,
        out_specs=(anywhere,) * 3,
        scratch_shapes=[
            pltpu.VMEM((rows, wide), BF16),
            pltpu.VMEM((rows, LANES), F32),
            pltpu.VMEM((4, 8, rows), F32),
            pltpu.SemaphoreType.DMA((5,)),
            pltpu.SemaphoreType.DMA((50 * n // 2,)),
            pltpu.SemaphoreType.DMA((30 * n // 2,)),
        ],
        compiler_params=pltpu.CompilerParams(
            collective_id=3, has_side_effects=True, vmem_limit_bytes=24 * 1024 * 1024
        ),
        cost_estimate=pl.CostEstimate(
            flops=20_000_000_000, bytes_accessed=100_000_000, transcendentals=0
        ),
    )(hidden, gain, w_x, w_z, w_bc, w_dt)


def heads_kernel(
    n,
    groups,
    hidden_ref,
    w_ref,
    wdt_ref,
    cx_ref,
    cb_ref,
    cc_ref,
    bias_ref,
    rate_ref,
    skip_ref,
    gain_ref,
    wout_ref,
    y_ref,
    rows_ref,
    held_ref,
    taps_ref,
    blocks,
    wdt_own,
    window,
    gate,
    raws,
    conv,
    state,
    out,
    normed,
    power,
    load_sem,
    local_sem,
    power_send,
    power_recv,
    plane_send,
    plane_recv,
    relay_send,
    first_send,
    first_recv,
    wout_send,
    wout_recv,
):
    me = lax.axis_index("seq")
    member = lax.axis_index("mp")
    m = lax.axis_size("mp")
    chips = n // 2
    z, c = me // 2, lax.rem(me, 2)
    partner = 2 * z + 1 - c
    per = n // groups
    base = me // per * per
    place = member * 2 + c
    quarter = 2 * gate.shape[1]
    strip = wout_ref.shape[1]
    across = member + 1 - 2 * lax.rem(member, 2)
    along = lax.rem(member + 2, 4)
    far = 3 - member
    rows = blocks.shape[1]
    inner = gate.shape[1]
    width = inner + 2 * N
    heads = inner // P_SIZE
    kw = taps_ref.shape[0]

    barrier = pltpu.get_barrier_semaphore()
    for d in range(1, n):
        signal_seq(barrier, lax.rem(me + d, n))
    for d in range(1, m):
        for core in range(2):
            pl.semaphore_signal(
                barrier,
                inc=1,
                device_id={"mp": lax.rem(member + d, m), "seq": 2 * z + core},
                device_id_type=pl.DeviceIdType.MESH,
            )
    pl.semaphore_wait(barrier, n - 1 + 2 * (m - 1))

    def remote(source, target_ref, sends, recvs, **target):
        return pltpu.make_async_remote_copy(
            src_ref=source,
            dst_ref=target_ref,
            send_sem=sends,
            recv_sem=recvs,
            device_id=target,
            device_id_type=pl.DeviceIdType.MESH,
        )

    def landed(target_ref, recvs):
        pltpu.make_async_copy(target_ref, target_ref, recvs).wait()

    def own_rows(chip):
        return wout_ref.at[pl.ds(pl.multiple_of(chip * quarter, quarter), quarter), :]

    parts = first_send.shape[0]
    slim = quarter // parts

    def first_leg(d, q):
        chip = lax.rem(z + d, chips)
        return remote(
            wout_ref.at[pl.ds(pl.multiple_of(chip * quarter + q * slim, slim), slim), :],
            held_ref.at[z, pl.ds(pl.multiple_of(q * slim, slim), slim), :],
            first_send.at[q, d],
            first_recv.at[q, d],
            seq=2 * chip + c,
        )

    def second_place(of):
        return rows_ref.at[
            pl.ds(pl.multiple_of(of * quarter, quarter), quarter),
            pl.ds(pl.multiple_of(c * strip, strip), strip),
        ]

    def second_leg(d):
        q = lax.rem(member + d, m)
        return remote(
            held_ref.at[q], second_place(member), wout_send.at[1, d], wout_recv.at[1, d], mp=q
        )

    def third_leg(d):
        of = second_place(lax.rem(member + d, m))
        return remote(of, of, wout_send.at[2, d], wout_recv.at[2, d], seq=partner)

    def keep_held():
        return pltpu.make_async_copy(own_rows(z), held_ref.at[z], local_sem.at[0])

    def keep_rows():
        return pltpu.make_async_copy(held_ref.at[member], second_place(member), local_sem.at[1])

    keep_held().start()

    def load(i, slot):
        return pltpu.make_async_copy(
            hidden_ref.at[pl.ds(pl.multiple_of(i * rows, rows), rows), :],
            blocks.at[slot],
            load_sem.at[slot],
        )

    load(0, 0).start()
    shared = pl.ds(pl.multiple_of(me * groups // n * N, N), N)
    taps_ref[:, 0:inner] = cx_ref[:, pl.ds(pl.multiple_of(me * inner, inner), inner)]
    taps_ref[:, inner : inner + N] = cb_ref[:, shared]
    taps_ref[:, inner + N : width] = cc_ref[:, shared]
    own_gain = gain_ref[:, pl.ds(pl.multiple_of(me * inner, inner), inner)]
    all_heads = wdt_ref.shape[0]
    pick_row = lax.broadcasted_iota(jnp.int32, (LANES, all_heads), 0)
    pick_col = lax.broadcasted_iota(jnp.int32, (LANES, all_heads), 1)
    chosen = jnp.logical_and(pick_col == me * heads + pick_row, pick_row < heads)
    wdt_own[...] = jnp.dot(
        jnp.where(chosen, 1.0, 0.0).astype(BF16), wdt_ref[...], preferred_element_type=F32
    ).astype(BF16)

    lane_head = lax.broadcasted_iota(jnp.int32, (LANES, inner), 1) // P_SIZE
    expand = jnp.where(
        lax.broadcasted_iota(jnp.int32, (LANES, inner), 0) == lane_head, 1.0, 0.0
    ).astype(BF16)
    window[0:8, :] = jnp.zeros((8, width), F32)
    state[...] = jnp.zeros_like(state)
    row_id = lax.broadcasted_iota(jnp.int32, (QB, QB), 0)
    col_id = lax.broadcasted_iota(jnp.int32, (QB, QB), 1)
    causal = row_id >= col_id
    low_lanes = col_id < P_SIZE
    tri = jnp.where(causal, 1.0, 0.0).astype(F32)

    def tell(i, k):
        target = base + lax.rem(me - base + k, per)
        return remote(
            power.at[i, 0], power.at[i, k], power_send.at[i, k], power_recv.at[i, k], seq=target
        )

    def spot(i, at, half=None):
        if half is None:
            return y_ref.at[i // 2, at]
        return y_ref.at[i // 2, at, half * (rows // 2) : (half + 1) * (rows // 2), :]

    def to_plane(i, k):
        return remote(
            normed.at[i],
            spot(i, place),
            plane_send.at[i, k + 1],
            plane_recv.at[i // 2, place, 0],
            mp=(across, along)[k],
            seq=2 * z + lax.rem(i, 2),
        )

    def to_partner(i):
        return remote(
            normed.at[i],
            spot(i, place),
            plane_send.at[i, 0],
            plane_recv.at[i // 2, place, 0],
            seq=partner,
        )

    def to_self(i):
        return pltpu.make_async_copy(normed.at[i], spot(i, place), plane_send.at[i, 0])

    def relay(i, k, core):
        at = (across, along)[k] * 2 + core
        return remote(
            spot(i, at, k),
            spot(i, at, k),
            relay_send.at[i // 2, k, core],
            plane_recv.at[i // 2, at, k],
            mp=(along, across)[k],
        )

    def forward(i):
        @pl.when(lax.rem(i, 2) == c)
        def _():
            for k in range(2):
                for core in range(2):
                    at = (across, along)[k] * 2 + core
                    landed(spot(i, at), plane_recv.at[i // 2, at, 0])
                    relay(i, k, core).start()

    def finish(i):
        for k in range(1, per):
            landed(power.at[i, k], power_recv.at[i, k])
        sums = power[i, 0]
        for k in range(1, per):
            sums = sums + power[i, k]
        column = jnp.transpose(jnp.broadcast_to(sums[0:1, :], (LANES, rows)))
        for sub in range(rows // QB):
            here = slice(sub * QB, (sub + 1) * QB)
            scale = lax.rsqrt(column[here, 0:1] / (per * inner) + 1e-05)
            normed[i, here, :] = (out[i, here, :].astype(F32) * scale * own_gain).astype(BF16)
        for k in range(2):
            to_plane(i, k).start()

        @pl.when(lax.rem(i, 2) == c)
        def _():
            to_self(i).start()

        @pl.when(lax.rem(i, 2) != c)
        def _():
            to_partner(i).start()

    def block(i, carry_none):
        slot = lax.rem(i, 2)

        @pl.when(i + 1 < n)
        def _():
            load(i + 1, 1 - slot).start()

        load(i, slot).wait()
        source = blocks.at[slot]
        window[8 : 8 + rows, 0:inner] = jnp.dot(
            source[...], w_ref[:, 0:inner], preferred_element_type=F32
        )
        gate[...] = jnp.dot(source[...], w_ref[:, inner : 2 * inner], preferred_element_type=F32)
        window[8 : 8 + rows, inner:width] = jnp.dot(
            source[...], w_ref[:, 2 * inner : 2 * inner + 2 * N], preferred_element_type=F32
        )
        raws[...] = lax.dot_general(
            source[...], wdt_own[...], (((1,), (1,)), ((), ())), preferred_element_type=F32
        )

        @pl.when(i > 0)
        def _():
            finish(i - 1)

        for sub in range(rows // QB):
            at = sub * QB
            here = slice(at, at + QB)
            for start in range(0, width, LANES):
                cs = slice(start, start + LANES)
                total = None
                for j in range(kw):
                    first = 8 - kw + 1 + j + at
                    term = taps_ref[j : j + 1, cs] * window[first : first + QB, cs]
                    total = term if total is None else total + term
                conv[sub, :, cs] = silu(total)
            raw = raws[here, :] + bias_ref[...]
            steps = jnp.maximum(raw, 0.0) + jnp.log1p(jnp.exp(-jnp.abs(raw)))
            decays = -rate_ref[...] * steps
            cum = jnp.dot(tri, decays, precision=HIGH, preferred_element_type=F32)
            cum_t = jnp.transpose(cum)
            grown = jnp.exp(cum)
            tail = jnp.exp(cum[QB - 1 : QB, :] - cum)
            x = conv[sub, :, 0:inner]
            b = conv[sub, :, inner : inner + N].astype(BF16)
            c = conv[sub, :, inner + N : width].astype(BF16)
            scaled = x * spread_heads(steps, expand)
            grown_e = spread_heads(grown, expand)
            tailed = (scaled * spread_heads(tail, expand)).astype(BF16)
            scaled_low = scaled.astype(BF16)
            held = state[...]
            carried = grown_e * jnp.dot(c, held.astype(BF16), preferred_element_type=F32)
            fresh = lax.dot_general(b, tailed, (((0,), (0,)), ((), ())), preferred_element_type=F32)
            state[...] = grown_e[QB - 1 : QB, :] * held + fresh
            affinity = lax.dot_general(c, b, (((1,), (1,)), ((), ())), preferred_element_type=F32)
            affinity = jnp.where(causal, affinity, 0.0)
            full = carried + skip_ref[...] * x
            squares = None
            for pair in range(inner // LANES):
                lanes = slice(pair * LANES, (pair + 1) * LANES)
                outs = []
                for k in range(2):
                    h = pair * 2 + k
                    spread_h = jnp.minimum(cum[:, h : h + 1] - cum_t[h : h + 1, :], 0.0)
                    mixing = (affinity * jnp.exp(spread_h)).astype(BF16)
                    outs.append(
                        jnp.dot(mixing, scaled_low[:, lanes], preferred_element_type=F32)
                    )
                inside = jnp.where(low_lanes, outs[0], outs[1])
                gated = (full[:, lanes] + inside) * silu(gate[here, lanes])
                out[i, here, lanes] = gated.astype(BF16)
                squares = gated * gated if squares is None else squares + gated * gated
            totals = jnp.broadcast_to(jnp.sum(squares, axis=-1, keepdims=True), (QB, LANES))
            power[i, 0, :, here] = jnp.transpose(totals)[0:8, :]
        window[0:8, :] = window[rows : rows + 8, :]

        for k in range(1, per):
            tell(i, k).start()

        @pl.when(i < parts)
        def _():
            for d in range(1, chips):
                first_leg(d, i).start()

        @pl.when(i > 1)
        def _():
            forward(i - 2)

        @pl.when(i == n - 3)
        def _():
            keep_held().wait()
            for d in range(1, chips):
                for q in range(parts):
                    landed(
                        held_ref.at[lax.rem(z + d, chips), q * slim : (q + 1) * slim, :],
                        first_recv.at[q, chips - d],
                    )
            keep_rows().start()
            for d in range(1, m):
                second_leg(d).start()

        return carry_none

    lax.fori_loop(0, n, block, 0)
    finish(n - 1)
    forward(n - 2)
    keep_rows().wait()
    third_leg(0).start()
    for d in range(1, m):
        landed(second_place(lax.rem(member + d, m)), wout_recv.at[1, m - d])
        third_leg(d).start()
    forward(n - 1)
    for d in range(m):
        strips = pl.ds(pl.multiple_of((1 - c) * strip, strip), strip)
        of = lax.rem(member + d, m)
        landed(
            rows_ref.at[pl.ds(pl.multiple_of(of * quarter, quarter), quarter), strips],
            wout_recv.at[2, d],
        )
    for j in range(chips):
        at = member * 2 + 1 - c
        landed(spot(2 * j, at), plane_recv.at[j, at, 0])
        for half in range(2):
            for core in range(2):
                at = far * 2 + core
                landed(spot(2 * j, at, half), plane_recv.at[j, at, half])
                relay(2 * j, half, core).wait_send()

    def flush(i, carry_none):
        for k in range(1, per):
            tell(i, k).wait_send()
        for k in range(2):
            to_plane(i, k).wait_send()

        @pl.when(lax.rem(i, 2) == c)
        def _():
            to_self(i).wait()

        @pl.when(lax.rem(i, 2) != c)
        def _():
            to_partner(i).wait_send()

        return carry_none

    lax.fori_loop(0, n, flush, 0)
    for d in range(1, chips):
        for q in range(parts):
            first_leg(d, q).wait_send()
    for d in range(1, m):
        second_leg(d).wait_send()
    for d in range(m):
        third_leg(d).wait_send()


def mix_heads(hidden, w_out, weights, w_dt, taps, bias, rate, skip, gain, groups):
    n, m = lax.axis_size("seq"), lax.axis_size("mp")
    rows = hidden.shape[0] // n
    features = hidden.shape[1]
    inner = skip.shape[1]
    width = inner + 2 * N
    quarter, strip = 2 * inner, w_out.shape[1]
    per = n // groups
    vmem = pl.BlockSpec(memory_space=pltpu.VMEM)
    anywhere = pl.BlockSpec(memory_space=pl.ANY)
    return pl.pallas_call(
        functools.partial(heads_kernel, n, groups),
        out_shape=(
            jax.ShapeDtypeStruct((n // 2, 2 * m, rows, inner), BF16),
            jax.ShapeDtypeStruct((m * quarter, 2 * strip), BF16),
        ),
        in_specs=[anywhere] + [vmem] * 9 + [anywhere],
        out_specs=(anywhere, vmem),
        scratch_shapes=[
            pltpu.VMEM((n // 2, quarter, strip), BF16),
            pltpu.VMEM((taps[0].shape[0], width), F32),
            pltpu.VMEM((2, rows, features), BF16),
            pltpu.VMEM((LANES, features), BF16),
            pltpu.VMEM((8 + rows, width), F32),
            pltpu.VMEM((rows, inner), F32),
            pltpu.VMEM((rows, LANES), F32),
            pltpu.VMEM((rows // QB, QB, width), F32),
            pltpu.VMEM((N, inner), F32),
            pltpu.VMEM((n, rows, inner), BF16),
            pltpu.VMEM((n, rows, inner), BF16),
            pltpu.VMEM((n, per, 8, rows), F32),
            pltpu.SemaphoreType.DMA((2,)),
            pltpu.SemaphoreType.DMA((2,)),
            pltpu.SemaphoreType.DMA((n, per)),
            pltpu.SemaphoreType.DMA((n, per)),
            pltpu.SemaphoreType.DMA((n, 3)),
            pltpu.SemaphoreType.DMA((n // 2, 2 * m, 2)),
            pltpu.SemaphoreType.DMA((n // 2, 2, 2)),
            pltpu.SemaphoreType.DMA((n // 2, n // 2)),
            pltpu.SemaphoreType.DMA((n // 2, n // 2)),
            pltpu.SemaphoreType.DMA((3, m)),
            pltpu.SemaphoreType.DMA((3, m)),
        ],
        compiler_params=pltpu.CompilerParams(
            collective_id=4, has_side_effects=True, vmem_limit_bytes=48 * 1024 * 1024
        ),
        cost_estimate=pl.CostEstimate(
            flops=40_000_000_000, bytes_accessed=50_000_000, transcendentals=8_000_000
        ),
    )(hidden, weights, w_dt, *taps, bias, rate, skip, gain, w_out)


def combine_kernel(
    n,
    y_ref,
    w_ref,
    hidden_ref,
    gain_ref,
    mixed_ref,
    normed_ref,
    part,
    outgoing,
    incoming,
    low,
    send_sem,
    recv_sem,
    own_sem,
    mp_send,
    mp_recv,
):
    me = lax.axis_index("seq")
    member = lax.axis_index("mp")
    chips = n // 2
    z = me // 2
    across = member + 1 - 2 * lax.rem(member, 2)
    along = lax.rem(member + 2, 4)
    far = 3 - member
    rows, wide = hidden_ref.shape
    tall = part.shape[0]
    chunks = rows // tall
    has_up, has_down = z + 1 <= chips - 1, z >= 1

    barrier = pltpu.get_barrier_semaphore()
    signal_mp(barrier, across)
    signal_mp(barrier, along)

    @pl.when(has_up)
    def _():
        signal_seq(barrier, me + 2)

    @pl.when(has_down)
    def _():
        signal_seq(barrier, me - 2)

    ends = jnp.logical_and(has_up, has_down)

    @pl.when(ends)
    def _():
        pl.semaphore_wait(barrier, 4)

    @pl.when(jnp.logical_not(ends))
    def _():
        pl.semaphore_wait(barrier, 3)

    def span(r):
        return pl.ds(pl.multiple_of(r * tall, tall), tall)

    def hand_on(j, r, way):
        return pltpu.make_async_remote_copy(
            src_ref=outgoing.at[j, span(r), :],
            dst_ref=incoming.at[way, j, span(r), :],
            send_sem=send_sem.at[j, r],
            recv_sem=recv_sem.at[way, j, r],
            device_id={"seq": me + 2 if way == 0 else me - 2},
            device_id_type=pl.DeviceIdType.MESH,
        )

    def take(j, r, way):
        where = incoming.at[way, j, span(r), :]
        pltpu.make_async_copy(where, where, recv_sem.at[way, j, r]).wait()
        return incoming[way, j, span(r), :].astype(F32)

    def feature(owner, r, half=None):
        at = pl.ds(pl.multiple_of(owner * wide, wide), wide)
        if half is None:
            return normed_ref.at[span(r), at]
        size = tall // 2
        return normed_ref.at[pl.ds(pl.multiple_of(r * tall + half * size, size), size), at]

    def shares(r):
        return [
            pltpu.make_async_remote_copy(
                src_ref=source,
                dst_ref=place,
                send_sem=mp_send.at[r, index],
                recv_sem=mp_recv.at[r, index],
                device_id={"mp": target},
                device_id_type=pl.DeviceIdType.MESH,
            )
            for index, (source, place, target) in enumerate(
                (
                    (low.at[span(r), :], feature(member, r), across),
                    (low.at[span(r), :], feature(member, r), along),
                    (feature(across, r, 0), feature(across, r, 0), along),
                    (feature(along, r, 1), feature(along, r, 1), across),
                )
            )
        ]

    def own_copy(r):
        return pltpu.make_async_copy(low.at[span(r), :], feature(member, r), own_sem.at[r])

    def arrived(r, index, place):
        pltpu.make_async_copy(place, place, mp_recv.at[r, index]).wait()

    def relay(r):
        mine = shares(r)
        arrived(r, 0, feature(across, r))
        mine[2].start()
        arrived(r, 1, feature(along, r))
        mine[3].start()

    def settle(r):
        arrived(r, 2, feature(far, r, 0))
        arrived(r, 3, feature(far, r, 1))
        own_copy(r).wait()
        for copy in shares(r):
            copy.wait_send()
        step = min(64, tall)
        for at in range(0, tall, step):
            here = pl.ds(pl.multiple_of(r * tall + at, step), step)
            normed_ref[here, :] = rms_norm(
                normed_ref[here, :].astype(F32), gain_ref[...]
            ).astype(BF16)

    order = []
    for k in range((chips + 1) // 2):
        order += [chips - 1 - k] + ([k] if k != chips - 1 - k else [])

    def product(j, r):
        y = jnp.concatenate([y_ref[j, at, span(r), :] for at in range(y_ref.shape[1])], axis=1)
        return jnp.dot(y, w_ref[...], preferred_element_type=F32)

    def outward(r):
        for j in order:

            @pl.when(z != j)
            def _():
                part[...] = product(j, r)

            @pl.when(jnp.logical_and(z < j, z >= 1))
            def _():
                part[...] += take(j, r, 0)

            @pl.when(jnp.logical_and(z > j, z <= chips - 2))
            def _():
                part[...] += take(j, r, 1)

            @pl.when(z != j)
            def _():
                outgoing[j, span(r), :] = part[...].astype(BF16)

            @pl.when(z < j)
            def _():
                hand_on(j, r, 0).start()

            @pl.when(z > j)
            def _():
                hand_on(j, r, 1).start()

    def final(r):
        part[...] = hidden_ref[span(r), :].astype(F32) + product(z, r)

        @pl.when(has_down)
        def _():
            part[...] += take(z, r, 0)

        @pl.when(has_up)
        def _():
            part[...] += take(z, r, 1)

        mixed_ref[span(r), :] = part[...]
        low[span(r), :] = part[...].astype(BF16)
        mine = shares(r)
        mine[0].start()
        mine[1].start()
        own_copy(r).start()

    def chunk(r, carry_none):
        for lag, stage in enumerate((outward, final, relay, settle)):

            @pl.when(jnp.logical_and(r >= lag, r < chunks + lag))
            def _():
                stage(r - lag)

        return carry_none

    lax.fori_loop(0, chunks + 3, chunk, 0)

    def flush(r, carry_none):
        for j in range(chips):

            @pl.when(z < j)
            def _():
                hand_on(j, r, 0).wait_send()

            @pl.when(z > j)
            def _():
                hand_on(j, r, 1).wait_send()

        return carry_none

    lax.fori_loop(0, chunks, flush, 0)


def combine(y, weights, hidden, gain):
    n = lax.axis_size("seq")
    rows, wide = hidden.shape
    chips = n // 2
    tall = min(128, rows)
    chunks = rows // tall
    vmem = pl.BlockSpec(memory_space=pltpu.VMEM)
    return pl.pallas_call(
        functools.partial(combine_kernel, n),
        out_shape=(
            jax.ShapeDtypeStruct((rows, wide), F32),
            jax.ShapeDtypeStruct((rows, 4 * wide), BF16),
        ),
        in_specs=[vmem] * 4,
        out_specs=(vmem, vmem),
        scratch_shapes=[
            pltpu.VMEM((tall, wide), F32),
            pltpu.VMEM((chips, rows, wide), BF16),
            pltpu.VMEM((2, chips, rows, wide), BF16),
            pltpu.VMEM((rows, wide), BF16),
            pltpu.SemaphoreType.DMA((chips, chunks)),
            pltpu.SemaphoreType.DMA((2, chips, chunks)),
            pltpu.SemaphoreType.DMA((chunks,)),
            pltpu.SemaphoreType.DMA((chunks, 4)),
            pltpu.SemaphoreType.DMA((chunks, 4)),
        ],
        compiler_params=pltpu.CompilerParams(
            collective_id=6, has_side_effects=True, vmem_limit_bytes=56 * 1024 * 1024
        ),
        cost_estimate=pl.CostEstimate(
            flops=2 * chips * rows * y.shape[2] * wide,
            bytes_accessed=60_000_000,
            transcendentals=0,
        ),
    )(y, weights, hidden, gain)


def own_slice(values, index, size):
    return lax.dynamic_slice_in_dim(values, index * size, size, values.ndim - 1)


def mixer_by_heads(
    hidden_in, norm_gain, w_z, w_x, w_b, w_c, w_dt, conv_x, conv_b, conv_c, dt_bias, a_rate,
    skip_gain, group_gain,
):
    n = lax.axis_size("seq")
    me = lax.axis_index("seq")
    groups = conv_b.shape[1] // N
    inner = conv_x.shape[1] // n
    heads = dt_bias.shape[0] // n
    pieces = []
    for g in range(groups):
        pieces += [w_b[:, g * N : (g + 1) * N], w_c[:, g * N : (g + 1) * N]]
    hidden, weights, steps = spread(
        hidden_in, norm_gain[None, :], w_x, w_z, jnp.concatenate(pieces, axis=1), jnp.transpose(w_dt), groups
    )
    return hidden, functools.partial(
        mix_heads,
        weights=weights,
        w_dt=steps,
        taps=(conv_x, conv_b, conv_c),
        bias=pad_lanes(own_slice(dt_bias[None, :], me, heads)),
        rate=pad_lanes(own_slice(a_rate[None, :], me, heads)),
        skip=jnp.repeat(own_slice(skip_gain[None, :], me, heads), P_SIZE, axis=1),
        gain=group_gain[None, :],
        groups=groups,
    )


def splits_by_heads(conv_x, conv_b):
    n, m = lax.axis_size("seq"), lax.axis_size("mp")
    groups = conv_b.shape[1] // N
    whole = conv_x.shape[1] % (n * LANES) == 0 and n % groups == 0
    return m == 4 and n == 2 * m and whole


def on_device(
    hidden_in,
    norm_gain,
    w_z,
    w_x,
    w_b,
    w_c,
    w_dt,
    conv_x,
    conv_b,
    conv_c,
    dt_bias,
    a_rate,
    skip_gain,
    group_gain,
    w_out,
    attn_gain,
    w_q,
    w_k,
    w_v,
):
    if splits_by_heads(conv_x, conv_b):
        hidden, mix = mixer_by_heads(
            hidden_in, norm_gain, w_z, w_x, w_b, w_c, w_dt, conv_x, conv_b, conv_c, dt_bias,
            a_rate, skip_gain, group_gain,
        )
        y_normed, out_rows = mix(hidden, w_out)
        mixed, normed_two = combine(y_normed, out_rows, hidden_in, attn_gain[None, :])
    else:
        proj = gather_dot(
            hidden_in,
            norm_gain[None, :],
            jnp.concatenate([w_x, w_b, w_c, pad_lanes(w_dt), w_z], axis=1),
        )
        proj, w_out = lax.optimization_barrier((proj, w_out))
        out_columns = lax.all_gather(w_out, "seq", axis=1, tiled=True)
        heads = dt_bias.shape[0]
        groups = conv_b.shape[1] // N
        width = conv_x.shape[1] + conv_b.shape[1] + conv_c.shape[1]
        rim = from_behind(proj[proj.shape[0] - 8 :, :width], "seq", 1)
        y_normed = mixer(
            proj,
            rim,
            jnp.concatenate([conv_x, conv_b, conv_c], axis=1),
            pad_lanes(dt_bias[None, :]),
            pad_lanes(a_rate[None, :]),
            jnp.repeat(skip_gain, P_SIZE)[None, :],
            group_gain[None, :],
            heads,
            groups,
        )
        mixed, normed_two = output_stage(
            y_normed, out_columns, hidden_in, attn_gain[None, :]
        )
    n = lax.axis_size("seq")
    if n % 2 == 0 and n >= 4 and WINDOW >= n * hidden_in.shape[0]:
        context = line_attention(normed_two, w_q, w_k, w_v)
    else:
        own_keys = jnp.dot(normed_two, w_k, preferred_element_type=F32).astype(BF16)
        own_values = jnp.dot(normed_two, w_v, preferred_element_type=F32).astype(BF16)
        pairs = lax.all_gather(
            jnp.concatenate([own_keys, own_values], axis=1), "seq", axis=0, tiled=True
        )
        queries = jnp.dot(normed_two, w_q, preferred_element_type=F32).astype(BF16)
        context = attention(queries, pairs, own_keys.shape[1] // HD)
    return (mixed, context)


def solution(mesh):
    placed = (
        P("seq", "mp"),
        P(),
        P("seq", "mp"),
        P("seq", "mp"),
        P("seq", "mp"),
        P("seq", "mp"),
        P("seq", "mp"),
        P(None, "mp"),
        P(None, "mp"),
        P(None, "mp"),
        P("mp"),
        P("mp"),
        P("mp"),
        P("mp"),
        P("mp", "seq"),
        P(),
        P(None, "mp"),
        P(None, "mp"),
        P(None, "mp"),
    )
    return jax.shard_map(
        on_device,
        mesh=mesh,
        in_specs=placed,
        out_specs=(P("seq", "mp"), P("seq", "mp")),
        check_vma=False,
    )
```
